8 devices in a mesh: dp: 1 (over z), tp: 2 (over y), sp: 4 (over x, core).
Axes of the slice: x: 2, y: 2, z: 1, core: 2. Of those that a mesh axis runs over, the one named last changes fastest.
Arguments:
- x_in: bfloat16 [256, 4608], P('dp')
- cur_pos: int32 [256], P('dp')
- w_pre: float32 [4608], replicated
- w_q: bfloat16 [4608, 4096], P(None, 'tp')
- w_k: bfloat16 [4608, 2048], P(None, 'tp')
- w_v: bfloat16 [4608, 2048], P(None, 'tp')
- w_o: bfloat16 [4096, 4608], P('tp')
- w_post: float32 [4608], replicated
- k_cache: bfloat16 [256, 256, 16, 128], P('dp', 'sp', 'tp')
- v_cache: bfloat16 [256, 256, 16, 128], P('dp', 'sp', 'tp')
Outputs:
- output 1: bfloat16 [256, 4608], P('dp')
- output 2: bfloat16 [256, 256, 16, 128], P('dp', 'sp', 'tp')
- output 3: bfloat16 [256, 256, 16, 128], P('dp', 'sp', 'tp')
All inputs are finite; a program needn't handle non-finite values.
Results may differ from the reference program's by a relative error of at most 0.00626649.
Values sent between devices are 32-bit elements.
A program may use at most 1 GiB of HBM per device.

```python
import jax
import jax.numpy as jnp
from jax import lax

BATCH_SIZE = 256
SEQ_LEN = 256
D_MODEL = 4608
NUM_HEADS = 32
KV_HEADS = 16
HEAD_DIM = 128
HOT_KEYS = 48

SOFT_CAP = 50.0
ROPE_BASE = 10000.0
NORM_EPS = 1e-6


def rms_scale(tensor, gain_w):
    mean_sq = jnp.mean(tensor * tensor, axis=-1, keepdims=True)
    return tensor * lax.rsqrt(mean_sq + NORM_EPS) * (1.0 + gain_w)


def rotary(tensor, positions):
    half_dim = tensor.shape[-1] // 2
    inv_freq = ROPE_BASE ** (-2.0 * jnp.arange(half_dim, dtype=jnp.float32) / (2 * half_dim))
    angles = positions.astype(jnp.float32)[:, None] * inv_freq[None, :]
    angles = angles.reshape((angles.shape[0],) + (1,) * (tensor.ndim - 2) + (half_dim,))
    cos_tab = jnp.cos(angles)
    sin_tab = jnp.sin(angles)
    lo_half = tensor[..., :half_dim]
    hi_half = tensor[..., half_dim:]
    return jnp.concatenate([lo_half * cos_tab - hi_half * sin_tab, hi_half * cos_tab + lo_half * sin_tab], axis=-1)


def setup_inputs(seed: int = 0, part: int = 0) -> dict:
    part_keys = jax.random.split(jax.random.fold_in(jax.random.key(seed), part), 6)
    shared_keys = jax.random.split(jax.random.key(seed + 1), 7)
    q_cols = NUM_HEADS * HEAD_DIM
    kv_cols = KV_HEADS * HEAD_DIM
    cache_shape = (BATCH_SIZE, SEQ_LEN, KV_HEADS, HEAD_DIM)
    x_in = jax.random.normal(part_keys[0], (BATCH_SIZE, D_MODEL), jnp.float32).astype(jnp.bfloat16)
    drawn_pos = jax.random.randint(part_keys[1], (BATCH_SIZE,), 0, SEQ_LEN)
    long_row = jax.random.randint(part_keys[2], (), 0, BATCH_SIZE)
    cur_pos = jnp.where(jnp.arange(BATCH_SIZE) == long_row, SEQ_LEN - 1, drawn_pos).astype(jnp.int32)
    hot_mark = jax.random.randint(part_keys[3], (BATCH_SIZE, SEQ_LEN, KV_HEADS, 1), 0, SEQ_LEN) < HOT_KEYS
    key_scale = jnp.where(hot_mark, 2.5, 0.03)
    k_cache = (jax.random.normal(part_keys[4], cache_shape, jnp.float32) * key_scale).astype(jnp.bfloat16)
    v_cache = jax.random.normal(part_keys[5], cache_shape, jnp.float32).astype(jnp.bfloat16)
    w_pre = 0.5 * jax.random.normal(shared_keys[0], (D_MODEL,), jnp.float32)
    w_q = (jax.random.normal(shared_keys[1], (D_MODEL, q_cols), jnp.float32) * (36.0 * D_MODEL ** -0.5)).astype(jnp.bfloat16)
    w_k = (jax.random.normal(shared_keys[2], (D_MODEL, kv_cols), jnp.float32) * (2.2 * D_MODEL ** -0.5)).astype(jnp.bfloat16)
    w_v = (jax.random.normal(shared_keys[3], (D_MODEL, kv_cols), jnp.float32) * D_MODEL ** -0.5).astype(jnp.bfloat16)
    w_o = (jax.random.normal(shared_keys[4], (q_cols, D_MODEL), jnp.float32) * q_cols ** -0.5).astype(jnp.bfloat16)
    w_post = 0.5 * jax.random.normal(shared_keys[5], (D_MODEL,), jnp.float32)
    return {'x_in': x_in, 'cur_pos': cur_pos, 'w_pre': w_pre, 'w_q': w_q, 'w_k': w_k, 'w_v': w_v, 'w_o': w_o, 'w_post': w_post, 'k_cache': k_cache, 'v_cache': v_cache}


def reference(x_in, cur_pos, w_pre, w_q, w_k, w_v, w_o, w_post, k_cache, v_cache):
    group_size = NUM_HEADS // KV_HEADS
    seq_ids = jnp.arange(SEQ_LEN)
    normed = rms_scale(x_in.astype(jnp.float32), w_pre).astype(jnp.bfloat16)
    q_proj = jnp.dot(normed, w_q, preferred_element_type=jnp.float32).reshape(BATCH_SIZE, NUM_HEADS, HEAD_DIM)
    k_proj = jnp.dot(normed, w_k, preferred_element_type=jnp.float32).reshape(BATCH_SIZE, KV_HEADS, HEAD_DIM)
    q_rot = rotary(q_proj, cur_pos).astype(jnp.bfloat16)
    k_new = rotary(k_proj, cur_pos).astype(jnp.bfloat16)
    v_new = jnp.dot(normed, w_v, preferred_element_type=jnp.float32).reshape(BATCH_SIZE, KV_HEADS, HEAD_DIM).astype(jnp.bfloat16)
    slot_hit = (seq_ids[None, :] == cur_pos[:, None])[:, :, None, None]
    k_out = jnp.where(slot_hit, k_new[:, None], k_cache)
    v_out = jnp.where(slot_hit, v_new[:, None], v_cache)

    def one_row(row_data):
        q_row, k_row, v_row, pos_row = row_data
        q_grp = q_row.astype(jnp.float32).reshape(KV_HEADS, group_size, HEAD_DIM)
        raw_score = jnp.einsum('grd,tgd->grt', q_grp, k_row.astype(jnp.float32)) * HEAD_DIM ** -0.5
        capped = SOFT_CAP * jnp.tanh(raw_score / SOFT_CAP)
        capped = jnp.where(seq_ids <= pos_row, capped, -jnp.inf)
        prob_w = jax.nn.softmax(capped, axis=-1)
        attn_row = jnp.einsum('grt,tgd->grd', prob_w, v_row.astype(jnp.float32))
        return attn_row.reshape(NUM_HEADS * HEAD_DIM)

    attn_out = lax.map(one_row, (q_rot, k_out, v_out, cur_pos))
    proj_sum = jnp.dot(attn_out.astype(jnp.bfloat16), w_o, preferred_element_type=jnp.float32)
    x_out = (x_in.astype(jnp.float32) + rms_scale(proj_sum, w_post)).astype(jnp.bfloat16)
    return (x_out, k_out, v_out)
```

```python
import functools

import jax
import jax.numpy as jnp
from jax import lax
from jax.experimental import pallas as pl
from jax.experimental.pallas import tpu as pltpu
from jax.sharding import PartitionSpec as P

SOFT_CAP = 50.0
ROPE_BASE = 10000.0
NORM_EPS = 1e-6
LOG2E = 1.4426950408889634

ROWS_STEP = 8
SLOTS = 6
AHEAD = 4


def rms_scale(tensor, gain_w):
    mean_sq = jnp.mean(tensor * tensor, axis=-1, keepdims=True)
    return tensor * lax.rsqrt(mean_sq + NORM_EPS) * (1.0 + gain_w)


def rotary(tensor, positions):
    half_dim = tensor.shape[-1] // 2
    inv_freq = ROPE_BASE ** (-2.0 * jnp.arange(half_dim, dtype=jnp.float32) / (2 * half_dim))
    angles = positions.astype(jnp.float32)[:, None] * inv_freq[None, :]
    angles = angles.reshape((angles.shape[0],) + (1,) * (tensor.ndim - 2) + (half_dim,))
    cos_tab = jnp.cos(angles)
    sin_tab = jnp.sin(angles)
    lo_half = tensor[..., :half_dim]
    hi_half = tensor[..., half_dim:]
    return jnp.concatenate([lo_half * cos_tab - hi_half * sin_tab, hi_half * cos_tab + lo_half * sin_tab], axis=-1)


def attend_kernel(n_steps, first_row, kv_heads, seq_block, pos_ref, base_ref, q_hbm, kn_hbm, vn_hbm, k_hbm, v_hbm,
                  *rest):
    (ko_hbm, vo_hbm, o_hbm, m_ref, l_ref, kbuf, vbuf, qbuf, knbuf, vnbuf, obuf, key_ref, in_sem, out_sem, o_sem) = rest[-15:]
    step_rows = ROWS_STEP
    heads, head_dim = qbuf.shape[2], qbuf.shape[3]
    cols = seq_block * kv_heads
    base = base_ref[0]

    row_id = lax.broadcasted_iota(jnp.int32, (heads, cols), 0)
    col_id = lax.broadcasted_iota(jnp.int32, (heads, cols), 1)
    mine = lax.rem(col_id, kv_heads) == row_id // (heads // kv_heads)
    key_ref[...] = jnp.where(mine, col_id, cols * 4)
    lane_id = lax.broadcasted_iota(jnp.int32, m_ref.shape, 1)
    half_id = lax.broadcasted_iota(jnp.int32, (2 * kv_heads, head_dim), 0) // kv_heads

    def loads(step, slot):
        rows = pl.ds(first_row + step * step_rows, step_rows)
        return (pltpu.make_async_copy(k_hbm.at[rows], kbuf.at[slot], in_sem.at[slot, 0]),
                pltpu.make_async_copy(v_hbm.at[rows], vbuf.at[slot], in_sem.at[slot, 1]),
                pltpu.make_async_copy(q_hbm.at[rows], qbuf.at[slot], in_sem.at[slot, 2]),
                pltpu.make_async_copy(kn_hbm.at[rows], knbuf.at[slot], in_sem.at[slot, 3]),
                pltpu.make_async_copy(vn_hbm.at[rows], vnbuf.at[slot], in_sem.at[slot, 4]))

    def stores(step, slot):
        rows = pl.ds(first_row + step * step_rows, step_rows)
        return (pltpu.make_async_copy(kbuf.at[slot], ko_hbm.at[rows], out_sem.at[slot, 0]),
                pltpu.make_async_copy(vbuf.at[slot], vo_hbm.at[rows], out_sem.at[slot, 1]))

    def o_store(step, slot):
        rows = pl.ds(step * step_rows, step_rows)
        return pltpu.make_async_copy(obuf.at[slot], o_hbm.at[rows], o_sem.at[slot])

    for step in range(min(AHEAD, n_steps)):
        for copy in loads(step, step):
            copy.start()
    m_ref[...] = jnp.zeros_like(m_ref)
    l_ref[...] = jnp.zeros_like(l_ref)
    scale = head_dim ** -0.5 / SOFT_CAP

    def body(step, carry):
        slot = lax.rem(step, SLOTS)
        oslot = lax.rem(step, 2)
        for copy in loads(step, slot):
            copy.wait()

        for r in range(step_rows):
            local = pos_ref[first_row + step * step_rows + r] - base

            @pl.when((local >= 0) & (local < seq_block))
            def _():
                pair = pl.ds(pl.multiple_of((local // 2) * (2 * kv_heads), 2 * kv_heads), 2 * kv_heads)
                hit = half_id == lax.rem(local, 2)
                kbuf[slot, r, pair, :] = jnp.where(hit, knbuf[slot, r], kbuf[slot, r, pair, :])
                vbuf[slot, r, pair, :] = jnp.where(hit, vnbuf[slot, r], vbuf[slot, r, pair, :])

        @pl.when(step >= 2)
        def _():
            o_store(step - 2, oslot).wait()

        m_all = m_ref[...]
        l_all = l_ref[...]
        for r in range(step_rows):
            local = pos_ref[first_row + step * step_rows + r] - base
            raw = lax.dot_general(qbuf[slot, r], kbuf[slot, r], (((1,), (1,)), ((), ())),
                                  preferred_element_type=jnp.float32)
            seen = key_ref[...] < (local + 1) * kv_heads
            soft = jnp.where(seen, jnp.tanh(raw * scale), -4.0)
            top = jnp.maximum(jnp.max(soft, axis=-1, keepdims=True), -1.0)
            weight = jnp.exp2((soft - top) * (SOFT_CAP * LOG2E))
            total = jnp.sum(weight, axis=-1, keepdims=True)
            weight = weight.astype(jnp.bfloat16)
            half = cols // 2
            left = jnp.concatenate([weight[:, :half], weight[:, half:]], axis=0)
            right = jnp.concatenate([vbuf[slot, r, :half, :], vbuf[slot, r, half:, :]], axis=1)
            both = jnp.dot(left, right, preferred_element_type=jnp.float32)
            obuf[oslot, r] = both[:heads, :head_dim] + both[heads:, head_dim:]
            here = lane_id == step * step_rows + r
            m_all = jnp.where(here, top * SOFT_CAP, m_all)
            l_all = jnp.where(here, total, l_all)
        m_ref[...] = m_all
        l_ref[...] = l_all
        o_store(step, oslot).start()
        for copy in stores(step, slot):
            copy.start()

        @pl.when(step + AHEAD < n_steps)
        def _():
            nxt = step + AHEAD
            nslot = lax.rem(nxt, SLOTS)

            @pl.when(nxt >= SLOTS)
            def _():
                for copy in stores(nxt - SLOTS, nslot):
                    copy.wait()
            for copy in loads(nxt, nslot):
                copy.start()
        return carry

    lax.fori_loop(0, n_steps, body, 0)
    for step in range(max(0, n_steps - SLOTS), n_steps):
        for copy in stores(step, step % SLOTS):
            copy.wait()
    for step in range(max(0, n_steps - 2), n_steps):
        o_store(step, step % 2).wait()


def attend(pos, base, q, kn, vn, k_cache, v_cache, prev, first_row, n_rows):
    rows, cols, head_dim = k_cache.shape
    heads = q.shape[1]
    kv_heads = kn.shape[1] // 2
    seq_block = cols // kv_heads
    n_steps = n_rows // ROWS_STEP
    hbm = pl.BlockSpec(memory_space=pl.ANY)
    vmem = pl.BlockSpec(memory_space=pltpu.VMEM)
    smem = pl.BlockSpec(memory_space=pltpu.SMEM)
    bf = jnp.bfloat16
    aliases = {} if prev is None else {7: 0, 8: 1}
    extra = () if prev is None else tuple(prev)
    return pl.pallas_call(
        functools.partial(attend_kernel, n_steps, first_row, kv_heads, seq_block),
        out_shape=(jax.ShapeDtypeStruct(k_cache.shape, bf), jax.ShapeDtypeStruct(v_cache.shape, bf),
                   jax.ShapeDtypeStruct((n_rows, heads, head_dim), jnp.float32),
                   jax.ShapeDtypeStruct((heads, n_rows), jnp.float32),
                   jax.ShapeDtypeStruct((heads, n_rows), jnp.float32)),
        in_specs=[smem, smem, hbm, hbm, hbm, hbm, hbm] + [hbm] * len(extra),
        out_specs=(hbm, hbm, hbm, vmem, vmem),
        scratch_shapes=[
            pltpu.VMEM((SLOTS, ROWS_STEP, cols, head_dim), bf),
            pltpu.VMEM((SLOTS, ROWS_STEP, cols, head_dim), bf),
            pltpu.VMEM((SLOTS, ROWS_STEP, heads, head_dim), bf),
            pltpu.VMEM((SLOTS, ROWS_STEP, 2 * kv_heads, head_dim), bf),
            pltpu.VMEM((SLOTS, ROWS_STEP, 2 * kv_heads, head_dim), bf),
            pltpu.VMEM((2, ROWS_STEP, heads, head_dim), jnp.float32),
            pltpu.VMEM((heads, cols), jnp.int32),
            pltpu.SemaphoreType.DMA((SLOTS, 5)),
            pltpu.SemaphoreType.DMA((SLOTS, 2)),
            pltpu.SemaphoreType.DMA((2,)),
        ],
        input_output_aliases=aliases,
        compiler_params=pltpu.CompilerParams(vmem_limit_bytes=40 * 1024 * 1024),
        cost_estimate=pl.CostEstimate(flops=n_rows * heads * cols * head_dim * 4,
                                      bytes_accessed=n_rows * cols * head_dim * 8, transcendentals=0),
        name='attend',
    )(pos, base, q, kn, vn, k_cache, v_cache, *extra)


def solution(mesh):
    cache_spec = P('dp', 'sp', 'tp', None)
    sp_size = mesh.shape['sp']
    tp_size = mesh.shape['tp']

    def swap(value, axis, size, bit):
        return lax.ppermute(value, axis, [(i, i ^ bit) for i in range(size)])

    def local_step(x_in, cur_pos, w_pre, w_q, w_k, w_v, w_o, w_post, k_cache, v_cache):
        row_count, seq_block, kv_local, head_dim = k_cache.shape
        heads_local = w_q.shape[1] // head_dim
        sp_index = lax.axis_index('sp')
        x_f = x_in.astype(jnp.float32)
        normed = rms_scale(x_f, w_pre).astype(jnp.bfloat16)
        q_proj = jnp.dot(normed, w_q, preferred_element_type=jnp.float32)
        q_rot = rotary(q_proj.reshape(row_count, heads_local, head_dim), cur_pos).astype(jnp.bfloat16)
        k_proj = jnp.dot(normed, w_k, preferred_element_type=jnp.float32)
        k_new = rotary(k_proj.reshape(row_count, kv_local, head_dim), cur_pos).astype(jnp.bfloat16)
        v_new = jnp.dot(normed, w_v, preferred_element_type=jnp.float32).reshape(row_count, kv_local, head_dim).astype(jnp.bfloat16)
        kn2 = jnp.concatenate([k_new, k_new], axis=1)
        vn2 = jnp.concatenate([v_new, v_new], axis=1)
        base = (sp_index * seq_block).astype(jnp.int32).reshape(1)
        kc = k_cache.reshape(row_count, seq_block * kv_local, head_dim)
        vc = v_cache.reshape(row_count, seq_block * kv_local, head_dim)
        k_out, v_out, o, m, l = attend(cur_pos, base, q_rot, kn2, vn2, kc, vc, None, 0, row_count)

        stat = jnp.concatenate([m, l], axis=0).T[:, :, None]
        stat = jnp.broadcast_to(stat, stat.shape[:2] + (4,)).reshape(row_count, 1, head_dim)
        pack = jnp.concatenate([o, stat], axis=1)

        def unpack(p):
            s = p[:, heads_local:].reshape(p.shape[0], 2 * heads_local, 4)[:, :, :1]
            return p[:, :heads_local], s[:, :heads_local], s[:, heads_local:]

        def merge(a, b):
            oa, ma, la = unpack(a)
            ob, mb, lb = unpack(b)
            mm = jnp.maximum(ma, mb)
            fa, fb = jnp.exp(ma - mm), jnp.exp(mb - mm)
            return oa * fa + ob * fb, mm, la * fa + lb * fb

        def repack(om, mm, lm):
            s = jnp.concatenate([mm, lm], axis=1)
            s = jnp.broadcast_to(s, s.shape[:2] + (4,)).reshape(om.shape[0], 1, head_dim)
            return jnp.concatenate([om, s], axis=1)

        half = row_count // 2
        core = sp_index % 2
        xpos = sp_index // 2
        keep = lax.dynamic_slice_in_dim(pack, core * half, half, 0)
        give = lax.dynamic_slice_in_dim(pack, (1 - core) * half, half, 0)
        got = swap(give, 'sp', sp_size, 1)
        pack = repack(*merge(keep, got))
        quarter = half // 2
        keep = lax.dynamic_slice_in_dim(pack, xpos * quarter, quarter, 0)
        give = lax.dynamic_slice_in_dim(pack, (1 - xpos) * quarter, quarter, 0)
        got = swap(give, 'sp', sp_size, 2)
        om, mm, lm = merge(keep, got)
        attn = (om / lm).reshape(quarter, heads_local * head_dim).astype(jnp.bfloat16)
        part = jnp.dot(attn, w_o, preferred_element_type=jnp.float32)
        proj_sum = part + swap(part, 'tp', tp_size, 1)
        y = rms_scale(proj_sum, w_post)
        other = swap(y, 'sp', sp_size, 2)
        y2 = jnp.where(xpos == 0, jnp.concatenate([y, other], 0), jnp.concatenate([other, y], 0))
        other = swap(y2, 'sp', sp_size, 1)
        y4 = jnp.where(core == 0, jnp.concatenate([y2, other], 0), jnp.concatenate([other, y2], 0))
        x_out = (x_f + y4).astype(jnp.bfloat16)
        return x_out, k_out.reshape(k_cache.shape), v_out.reshape(v_cache.shape)

    return jax.shard_map(local_step, mesh=mesh,
                         in_specs=(P('dp', None), P('dp'), P(None), P(None, 'tp'), P(None, 'tp'), P(None, 'tp'), P('tp', None), P(None), cache_spec, cache_spec),
                         out_specs=(P('dp', None), cache_spec, cache_spec), check_vma=False)
```

```python
import functools

import jax
import jax.numpy as jnp
from jax import lax
from jax.experimental import pallas as pl
from jax.experimental.pallas import tpu as pltpu
from jax.sharding import PartitionSpec as P

SOFT_CAP = 50.0
ROPE_BASE = 10000.0
NORM_EPS = 1e-6
LOG2E = 1.4426950408889634

ROWS_STEP = 16
SLOTS = 5
AHEAD = 3
LAG_SOFT = 2
LAG_OUT = 4


def rms_scale(tensor, gain_w):
    mean_sq = jnp.mean(tensor * tensor, axis=-1, keepdims=True)
    return tensor * lax.rsqrt(mean_sq + NORM_EPS) * (1.0 + gain_w)


def rotary(tensor, positions):
    half_dim = tensor.shape[-1] // 2
    inv_freq = ROPE_BASE ** (-2.0 * jnp.arange(half_dim, dtype=jnp.float32) / (2 * half_dim))
    angles = positions.astype(jnp.float32)[:, None] * inv_freq[None, :]
    angles = angles.reshape((angles.shape[0],) + (1,) * (tensor.ndim - 2) + (half_dim,))
    cos_tab = jnp.cos(angles)
    sin_tab = jnp.sin(angles)
    lo_half = tensor[..., :half_dim]
    hi_half = tensor[..., half_dim:]
    return jnp.concatenate([lo_half * cos_tab - hi_half * sin_tab, hi_half * cos_tab + lo_half * sin_tab], axis=-1)


def attend_kernel(n_steps, first_row, kv_heads, seq_block, pos_ref, base_ref, q_hbm, kn_hbm, vn_hbm, k_hbm, v_hbm,
                  *rest):
    (ko_hbm, vo_hbm, o_hbm, m_ref, l_ref, kbuf, vbuf, qbuf, knbuf, vnbuf, obuf, key_ref, s_ref, p_ref, in_sem, out_sem, o_sem) = rest[-17:]
    step_rows = ROWS_STEP
    heads, head_dim = qbuf.shape[2], qbuf.shape[3]
    cols = seq_block * kv_heads
    base = base_ref[0]

    row_id = lax.broadcasted_iota(jnp.int32, (heads, cols), 0)
    col_id = lax.broadcasted_iota(jnp.int32, (heads, cols), 1)
    mine = lax.rem(col_id, kv_heads) == row_id // (heads // kv_heads)
    key_ref[...] = jnp.where(mine, col_id, cols * 4)
    lane_id = lax.broadcasted_iota(jnp.int32, m_ref.shape, 1)
    half_id = lax.broadcasted_iota(jnp.int32, (2 * kv_heads, head_dim), 0) // kv_heads

    def loads(step, slot):
        rows = pl.ds(first_row + step * step_rows, step_rows)
        return (pltpu.make_async_copy(k_hbm.at[rows], kbuf.at[slot], in_sem.at[slot, 0]),
                pltpu.make_async_copy(v_hbm.at[rows], vbuf.at[slot], in_sem.at[slot, 1]),
                pltpu.make_async_copy(q_hbm.at[rows], qbuf.at[slot], in_sem.at[slot, 2]),
                pltpu.make_async_copy(kn_hbm.at[rows], knbuf.at[slot], in_sem.at[slot, 3]),
                pltpu.make_async_copy(vn_hbm.at[rows], vnbuf.at[slot], in_sem.at[slot, 4]))

    def stores(step, slot):
        rows = pl.ds(first_row + step * step_rows, step_rows)
        return (pltpu.make_async_copy(kbuf.at[slot], ko_hbm.at[rows], out_sem.at[slot, 0]),
                pltpu.make_async_copy(vbuf.at[slot], vo_hbm.at[rows], out_sem.at[slot, 1]))

    def o_store(step, slot):
        rows = pl.ds(step * step_rows, step_rows)
        return pltpu.make_async_copy(obuf.at[slot], o_hbm.at[rows], o_sem.at[slot])

    for step in range(min(AHEAD, n_steps)):
        for copy in loads(step, step):
            copy.start()
    m_ref[...] = jnp.zeros_like(m_ref)
    l_ref[...] = jnp.zeros_like(l_ref)
    scale = head_dim ** -0.5 / SOFT_CAP

    def body(step, carry):
        slot = lax.rem(step, SLOTS)
        oslot = lax.rem(step, 2)
        for copy in loads(step, slot):
            copy.wait()

        for r in range(step_rows):
            local = pos_ref[first_row + step * step_rows + r] - base
            inside = (local >= 0) & (local < seq_block)
            at = jnp.clip(local, 0, seq_block - 1)
            pair = pl.ds(pl.multiple_of((at // 2) * (2 * kv_heads), 2 * kv_heads), 2 * kv_heads)
            hit = half_id == jnp.where(inside, lax.rem(at, 2), 2)
            kbuf[slot, r, pair, :] = jnp.where(hit, knbuf[slot, r], kbuf[slot, r, pair, :])
            vbuf[slot, r, pair, :] = jnp.where(hit, vnbuf[slot, r], vbuf[slot, r, pair, :])

        @pl.when(step >= 2)
        def _():
            o_store(step - 2, oslot).wait()

        m_all = m_ref[...]
        l_all = l_ref[...]
        half = cols // 2
        for tick in range(step_rows + LAG_OUT):
            r = tick
            if r < step_rows:
                raw = lax.dot_general(qbuf[slot, r], kbuf[slot, r], (((1,), (1,)), ((), ())),
                                      preferred_element_type=jnp.float32)
                s_ref[r] = raw
            r = tick - LAG_SOFT
            if 0 <= r < step_rows:
                local = pos_ref[first_row + step * step_rows + r] - base
                seen = key_ref[...] < (local + 1) * kv_heads
                soft = jnp.where(seen, jnp.tanh(s_ref[r] * scale), -4.0)
                top = jnp.maximum(jnp.max(soft, axis=-1, keepdims=True), -1.0)
                weight = jnp.exp2((soft - top) * (SOFT_CAP * LOG2E))
                total = jnp.sum(weight, axis=-1, keepdims=True)
                weight = weight.astype(jnp.bfloat16)
                p_ref[r, :heads] = weight[:, :half]
                p_ref[r, heads:] = weight[:, half:]
                here = lane_id == step * step_rows + r
                m_all = jnp.where(here, top * SOFT_CAP, m_all)
                l_all = jnp.where(here, total, l_all)
            r = tick - LAG_OUT
            if 0 <= r < step_rows:
                right = jnp.concatenate([vbuf[slot, r, :half, :], vbuf[slot, r, half:, :]], axis=1)
                both = jnp.dot(p_ref[r], right, preferred_element_type=jnp.float32)
                obuf[oslot, r] = both[:heads, :head_dim] + both[heads:, head_dim:]
        m_ref[...] = m_all
        l_ref[...] = l_all
        o_store(step, oslot).start()
        for copy in stores(step, slot):
            copy.start()

        @pl.when(step + AHEAD < n_steps)
        def _():
            nxt = step + AHEAD
            nslot = lax.rem(nxt, SLOTS)

            @pl.when(nxt >= SLOTS)
            def _():
                for copy in stores(nxt - SLOTS, nslot):
                    copy.wait()
            for copy in loads(nxt, nslot):
                copy.start()
        return carry

    lax.fori_loop(0, n_steps, body, 0)
    for step in range(max(0, n_steps - SLOTS), n_steps):
        for copy in stores(step, step % SLOTS):
            copy.wait()
    for step in range(max(0, n_steps - 2), n_steps):
        o_store(step, step % 2).wait()


def attend(pos, base, q, kn, vn, k_cache, v_cache, prev, first_row, n_rows):
    rows, cols, head_dim = k_cache.shape
    heads = q.shape[1]
    kv_heads = kn.shape[1] // 2
    seq_block = cols // kv_heads
    n_steps = n_rows // ROWS_STEP
    hbm = pl.BlockSpec(memory_space=pl.ANY)
    vmem = pl.BlockSpec(memory_space=pltpu.VMEM)
    smem = pl.BlockSpec(memory_space=pltpu.SMEM)
    bf = jnp.bfloat16
    aliases = {} if prev is None else {7: 0, 8: 1}
    extra = () if prev is None else tuple(prev)
    return pl.pallas_call(
        functools.partial(attend_kernel, n_steps, first_row, kv_heads, seq_block),
        out_shape=(jax.ShapeDtypeStruct(k_cache.shape, bf), jax.ShapeDtypeStruct(v_cache.shape, bf),
                   jax.ShapeDtypeStruct((n_rows, heads, head_dim), jnp.float32),
                   jax.ShapeDtypeStruct((heads, n_rows), jnp.float32),
                   jax.ShapeDtypeStruct((heads, n_rows), jnp.float32)),
        in_specs=[smem, smem, hbm, hbm, hbm, hbm, hbm] + [hbm] * len(extra),
        out_specs=(hbm, hbm, hbm, vmem, vmem),
        scratch_shapes=[
            pltpu.VMEM((SLOTS, ROWS_STEP, cols, head_dim), bf),
            pltpu.VMEM((SLOTS, ROWS_STEP, cols, head_dim), bf),
            pltpu.VMEM((SLOTS, ROWS_STEP, heads, head_dim), bf),
            pltpu.VMEM((SLOTS, ROWS_STEP, 2 * kv_heads, head_dim), bf),
            pltpu.VMEM((SLOTS, ROWS_STEP, 2 * kv_heads, head_dim), bf),
            pltpu.VMEM((2, ROWS_STEP, heads, head_dim), jnp.float32),
            pltpu.VMEM((heads, cols), jnp.int32),
            pltpu.VMEM((ROWS_STEP, heads, cols), jnp.float32),
            pltpu.VMEM((ROWS_STEP, 2 * heads, cols // 2), bf),
            pltpu.SemaphoreType.DMA((SLOTS, 5)),
            pltpu.SemaphoreType.DMA((SLOTS, 2)),
            pltpu.SemaphoreType.DMA((2,)),
        ],
        input_output_aliases=aliases,
        compiler_params=pltpu.CompilerParams(vmem_limit_bytes=40 * 1024 * 1024),
        cost_estimate=pl.CostEstimate(flops=n_rows * heads * cols * head_dim * 4,
                                      bytes_accessed=n_rows * cols * head_dim * 8, transcendentals=0),
        name='attend',
    )(pos, base, q, kn, vn, k_cache, v_cache, *extra)


def solution(mesh):
    cache_spec = P('dp', 'sp', 'tp', None)
    sp_size = mesh.shape['sp']
    tp_size = mesh.shape['tp']

    def swap(value, axis, size, bit):
        return lax.ppermute(value, axis, [(i, i ^ bit) for i in range(size)])

    def local_step(x_in, cur_pos, w_pre, w_q, w_k, w_v, w_o, w_post, k_cache, v_cache):
        row_count, seq_block, kv_local, head_dim = k_cache.shape
        heads_local = w_q.shape[1] // head_dim
        sp_index = lax.axis_index('sp')
        x_f = x_in.astype(jnp.float32)
        normed = rms_scale(x_f, w_pre).astype(jnp.bfloat16)
        q_proj = jnp.dot(normed, w_q, preferred_element_type=jnp.float32)
        q_rot = rotary(q_proj.reshape(row_count, heads_local, head_dim), cur_pos).astype(jnp.bfloat16)
        k_proj = jnp.dot(normed, w_k, preferred_element_type=jnp.float32)
        k_new = rotary(k_proj.reshape(row_count, kv_local, head_dim), cur_pos).astype(jnp.bfloat16)
        v_new = jnp.dot(normed, w_v, preferred_element_type=jnp.float32).reshape(row_count, kv_local, head_dim).astype(jnp.bfloat16)
        kn2 = jnp.concatenate([k_new, k_new], axis=1)
        vn2 = jnp.concatenate([v_new, v_new], axis=1)
        base = (sp_index * seq_block).astype(jnp.int32).reshape(1)
        kc = k_cache.reshape(row_count, seq_block * kv_local, head_dim)
        vc = v_cache.reshape(row_count, seq_block * kv_local, head_dim)
        k_out, v_out, o, m, l = attend(cur_pos, base, q_rot, kn2, vn2, kc, vc, None, 0, row_count)

        stat = jnp.concatenate([m, l], axis=0).T[:, :, None]
        stat = jnp.broadcast_to(stat, stat.shape[:2] + (4,)).reshape(row_count, 1, head_dim)
        pack = jnp.concatenate([o, stat], axis=1)

        def unpack(p):
            s = p[:, heads_local:].reshape(p.shape[0], 2 * heads_local, 4)[:, :, :1]
            return p[:, :heads_local], s[:, :heads_local], s[:, heads_local:]

        def merge(a, b):
            oa, ma, la = unpack(a)
            ob, mb, lb = unpack(b)
            mm = jnp.maximum(ma, mb)
            fa, fb = jnp.exp(ma - mm), jnp.exp(mb - mm)
            return oa * fa + ob * fb, mm, la * fa + lb * fb

        def repack(om, mm, lm):
            s = jnp.concatenate([mm, lm], axis=1)
            s = jnp.broadcast_to(s, s.shape[:2] + (4,)).reshape(om.shape[0], 1, head_dim)
            return jnp.concatenate([om, s], axis=1)

        half = row_count // 2
        core = sp_index % 2
        xpos = sp_index // 2
        keep = lax.dynamic_slice_in_dim(pack, core * half, half, 0)
        give = lax.dynamic_slice_in_dim(pack, (1 - core) * half, half, 0)
        got = swap(give, 'sp', sp_size, 1)
        pack = repack(*merge(keep, got))
        quarter = half // 2
        keep = lax.dynamic_slice_in_dim(pack, xpos * quarter, quarter, 0)
        give = lax.dynamic_slice_in_dim(pack, (1 - xpos) * quarter, quarter, 0)
        got = swap(give, 'sp', sp_size, 2)
        om, mm, lm = merge(keep, got)
        attn = (om / lm).reshape(quarter, heads_local * head_dim).astype(jnp.bfloat16)
        part = jnp.dot(attn, w_o, preferred_element_type=jnp.float32)
        proj_sum = part + swap(part, 'tp', tp_size, 1)
        y = rms_scale(proj_sum, w_post)
        other = swap(y, 'sp', sp_size, 2)
        y2 = jnp.where(xpos == 0, jnp.concatenate([y, other], 0), jnp.concatenate([other, y], 0))
        other = swap(y2, 'sp', sp_size, 1)
        y4 = jnp.where(core == 0, jnp.concatenate([y2, other], 0), jnp.concatenate([other, y2], 0))
        x_out = (x_f + y4).astype(jnp.bfloat16)
        return x_out, k_out.reshape(k_cache.shape), v_out.reshape(v_cache.shape)

    return jax.shard_map(local_step, mesh=mesh,
                         in_specs=(P('dp', None), P('dp'), P(None), P(None, 'tp'), P(None, 'tp'), P(None, 'tp'), P('tp', None), P(None), cache_spec, cache_spec),
                         out_specs=(P('dp', None), cache_spec, cache_spec), check_vma=False)
```

```python
import functools

import jax
import jax.numpy as jnp
from jax import lax
from jax.experimental import pallas as pl
from jax.experimental.pallas import tpu as pltpu
from jax.sharding import PartitionSpec as P

SOFT_CAP = 50.0
ROPE_BASE = 10000.0
NORM_EPS = 1e-6
LOG2E = 1.4426950408889634

ROWS_STEP = 16
SLOTS = 5
AHEAD = 3
LAG_SOFT = 2
LAG_OUT = 4


def rms_scale(tensor, gain_w):
    mean_sq = jnp.mean(tensor * tensor, axis=-1, keepdims=True)
    return tensor * lax.rsqrt(mean_sq + NORM_EPS) * (1.0 + gain_w)


def rotary(tensor, positions):
    half_dim = tensor.shape[-1] // 2
    inv_freq = ROPE_BASE ** (-2.0 * jnp.arange(half_dim, dtype=jnp.float32) / (2 * half_dim))
    angles = positions.astype(jnp.float32)[:, None] * inv_freq[None, :]
    angles = angles.reshape((angles.shape[0],) + (1,) * (tensor.ndim - 2) + (half_dim,))
    cos_tab = jnp.cos(angles)
    sin_tab = jnp.sin(angles)
    lo_half = tensor[..., :half_dim]
    hi_half = tensor[..., half_dim:]
    return jnp.concatenate([lo_half * cos_tab - hi_half * sin_tab, hi_half * cos_tab + lo_half * sin_tab], axis=-1)


def attend_kernel(n_steps, first_row, kv_heads, seq_block, pos_ref, base_ref, q_hbm, kn_hbm, vn_hbm, k_hbm, v_hbm,
                  *rest):
    (ko_hbm, vo_hbm, o_hbm, m_ref, l_ref, kbuf, vbuf, qbuf, knbuf, vnbuf, obuf, key_ref, s_ref, p_ref, in_sem, out_sem, o_sem) = rest[-17:]
    step_rows = ROWS_STEP
    heads, head_dim = qbuf.shape[2], qbuf.shape[3]
    cols = seq_block * kv_heads
    base = base_ref[0]

    row_id = lax.broadcasted_iota(jnp.int32, (heads, cols), 0)
    col_id = lax.broadcasted_iota(jnp.int32, (heads, cols), 1)
    mine = lax.rem(col_id, kv_heads) == row_id // (heads // kv_heads)
    key_ref[...] = jnp.where(mine, col_id, cols * 4)
    lane_id = lax.broadcasted_iota(jnp.int32, m_ref.shape, 1)
    half_id = lax.broadcasted_iota(jnp.int32, (2 * kv_heads, head_dim), 0) // kv_heads

    def loads(step, slot):
        rows = pl.ds(first_row + step * step_rows, step_rows)
        return (pltpu.make_async_copy(k_hbm.at[rows], kbuf.at[slot], in_sem.at[slot, 0]),
                pltpu.make_async_copy(v_hbm.at[rows], vbuf.at[slot], in_sem.at[slot, 1]),
                pltpu.make_async_copy(q_hbm.at[rows], qbuf.at[slot], in_sem.at[slot, 2]),
                pltpu.make_async_copy(kn_hbm.at[rows], knbuf.at[slot], in_sem.at[slot, 3]),
                pltpu.make_async_copy(vn_hbm.at[rows], vnbuf.at[slot], in_sem.at[slot, 4]))

    def stores(step, slot):
        rows = pl.ds(first_row + step * step_rows, step_rows)
        return (pltpu.make_async_copy(kbuf.at[slot], ko_hbm.at[rows], out_sem.at[slot, 0]),
                pltpu.make_async_copy(vbuf.at[slot], vo_hbm.at[rows], out_sem.at[slot, 1]))

    def o_store(step, slot):
        rows = pl.ds(step * step_rows, step_rows)
        return pltpu.make_async_copy(obuf.at[slot], o_hbm.at[rows], o_sem.at[slot])

    for step in range(min(AHEAD, n_steps)):
        for copy in loads(step, step):
            copy.start()
    m_ref[...] = jnp.zeros_like(m_ref)
    l_ref[...] = jnp.zeros_like(l_ref)
    scale = head_dim ** -0.5 / SOFT_CAP

    def body(step, carry):
        slot = lax.rem(step, SLOTS)
        oslot = lax.rem(step, 2)
        for copy in loads(step, slot):
            copy.wait()

        for r in range(step_rows):
            local = pos_ref[first_row + step * step_rows + r] - base
            inside = (local >= 0) & (local < seq_block)
            at = jnp.clip(local, 0, seq_block - 1)
            pair = pl.ds(pl.multiple_of((at // 2) * (2 * kv_heads), 2 * kv_heads), 2 * kv_heads)
            hit = half_id == jnp.where(inside, lax.rem(at, 2), 2)
            kbuf[slot, r, pair, :] = jnp.where(hit, knbuf[slot, r], kbuf[slot, r, pair, :])
            vbuf[slot, r, pair, :] = jnp.where(hit, vnbuf[slot, r], vbuf[slot, r, pair, :])

        @pl.when(step >= 2)
        def _():
            o_store(step - 2, oslot).wait()

        m_all = m_ref[...]
        l_all = l_ref[...]
        half = cols // 2
        for tick in range(step_rows + LAG_OUT):
            r = tick
            if r < step_rows:
                raw = lax.dot_general(qbuf[slot, r], kbuf[slot, r], (((1,), (1,)), ((), ())),
                                      preferred_element_type=jnp.float32)
                s_ref[r] = raw
            r = tick - LAG_SOFT
            if 0 <= r < step_rows:
                local = pos_ref[first_row + step * step_rows + r] - base
                seen = key_ref[...] < (local + 1) * kv_heads
                soft = jnp.where(seen, jnp.tanh(s_ref[r] * scale), -4.0)
                top = jnp.maximum(jnp.max(soft, axis=-1, keepdims=True), -1.0)
                weight = jnp.exp2((soft - top) * (SOFT_CAP * LOG2E))
                total = jnp.sum(weight, axis=-1, keepdims=True)
                weight = weight.astype(jnp.bfloat16)
                p_ref[r, :heads] = weight[:, :half]
                p_ref[r, heads:] = weight[:, half:]
                here = lane_id == step * step_rows + r
                m_all = jnp.where(here, top * SOFT_CAP, m_all)
                l_all = jnp.where(here, total, l_all)
            r = tick - LAG_OUT
            if 0 <= r < step_rows:
                right = jnp.concatenate([vbuf[slot, r, :half, :], vbuf[slot, r, half:, :]], axis=1)
                both = jnp.dot(p_ref[r], right, preferred_element_type=jnp.float32)
                obuf[oslot, r] = both[:heads, :head_dim] + both[heads:, head_dim:]
        m_ref[...] = m_all
        l_ref[...] = l_all
        o_store(step, oslot).start()
        for copy in stores(step, slot):
            copy.start()

        @pl.when(step + AHEAD < n_steps)
        def _():
            nxt = step + AHEAD
            nslot = lax.rem(nxt, SLOTS)

            @pl.when(nxt >= SLOTS)
            def _():
                for copy in stores(nxt - SLOTS, nslot):
                    copy.wait()
            for copy in loads(nxt, nslot):
                copy.start()
        return carry

    lax.fori_loop(0, n_steps, body, 0)
    for step in range(max(0, n_steps - SLOTS), n_steps):
        for copy in stores(step, step % SLOTS):
            copy.wait()
    for step in range(max(0, n_steps - 2), n_steps):
        o_store(step, step % 2).wait()


def attend(pos, base, q, kn, vn, k_cache, v_cache, prev, first_row, n_rows):
    rows, cols, head_dim = k_cache.shape
    heads = q.shape[1]
    kv_heads = kn.shape[1] // 2
    seq_block = cols // kv_heads
    n_steps = n_rows // ROWS_STEP
    hbm = pl.BlockSpec(memory_space=pl.ANY)
    vmem = pl.BlockSpec(memory_space=pltpu.VMEM)
    smem = pl.BlockSpec(memory_space=pltpu.SMEM)
    bf = jnp.bfloat16
    aliases = {} if prev is None else {7: 0, 8: 1}
    extra = () if prev is None else tuple(prev)
    return pl.pallas_call(
        functools.partial(attend_kernel, n_steps, first_row, kv_heads, seq_block),
        out_shape=(jax.ShapeDtypeStruct(k_cache.shape, bf), jax.ShapeDtypeStruct(v_cache.shape, bf),
                   jax.ShapeDtypeStruct((n_rows, heads, head_dim), jnp.float32),
                   jax.ShapeDtypeStruct((heads, n_rows), jnp.float32),
                   jax.ShapeDtypeStruct((heads, n_rows), jnp.float32)),
        in_specs=[smem, smem, hbm, hbm, hbm, hbm, hbm] + [hbm] * len(extra),
        out_specs=(hbm, hbm, hbm, vmem, vmem),
        scratch_shapes=[
            pltpu.VMEM((SLOTS, ROWS_STEP, cols, head_dim), bf),
            pltpu.VMEM((SLOTS, ROWS_STEP, cols, head_dim), bf),
            pltpu.VMEM((SLOTS, ROWS_STEP, heads, head_dim), bf),
            pltpu.VMEM((SLOTS, ROWS_STEP, 2 * kv_heads, head_dim), bf),
            pltpu.VMEM((SLOTS, ROWS_STEP, 2 * kv_heads, head_dim), bf),
            pltpu.VMEM((2, ROWS_STEP, heads, head_dim), jnp.float32),
            pltpu.VMEM((heads, cols), jnp.int32),
            pltpu.VMEM((ROWS_STEP, heads, cols), jnp.float32),
            pltpu.VMEM((ROWS_STEP, 2 * heads, cols // 2), bf),
            pltpu.SemaphoreType.DMA((SLOTS, 5)),
            pltpu.SemaphoreType.DMA((SLOTS, 2)),
            pltpu.SemaphoreType.DMA((2,)),
        ],
        input_output_aliases=aliases,
        compiler_params=pltpu.CompilerParams(vmem_limit_bytes=40 * 1024 * 1024),
        cost_estimate=pl.CostEstimate(flops=n_rows * heads * cols * head_dim * 4,
                                      bytes_accessed=n_rows * cols * head_dim * 8, transcendentals=0),
        name='attend',
    )(pos, base, q, kn, vn, k_cache, v_cache, *extra)


def merge_kernel(halves, sp_axis, tp_axis, o_ref, m_ref, l_ref, x_ref, wpost_ref, wo_hbm, out_ref,
                 wo, scaled, stats, core_in, x_in, lhs, y_out, y_in, sums, far_sum,
                 w_sem, st_send, st_recv, c_send, c_recv, r_send, r_recv, y_send, y_recv, g_send, g_recv,
                 d_send, d_recv, f_send, f_recv):
    sp = lax.axis_index(sp_axis)
    tp = lax.axis_index(tp_axis)
    core = lax.rem(sp, 2)
    xpos = sp // 2
    heads = m_ref.shape[0]
    rows, width = x_ref.shape
    quarter = rows // 4
    part = quarter // halves
    q_rows = quarter * heads
    h_rows = part * heads
    n_chunks = wo.shape[0]
    chunk = width // n_chunks
    core_peer = {sp_axis: 2 * xpos + (1 - core)}
    x_peer = {sp_axis: 2 * (1 - xpos) + core}
    far_peer = {sp_axis: 2 * (1 - xpos) + (1 - core)}
    y_peer = {tp_axis: 1 - tp}
    mesh_id = pl.DeviceIdType.MESH

    def remote(src, dst, send, recv, peer):
        return pltpu.make_async_remote_copy(src_ref=src, dst_ref=dst, send_sem=send, recv_sem=recv,
                                            device_id=peer, device_id_type=mesh_id)

    def w_load(n):
        return pltpu.make_async_copy(wo_hbm.at[:, pl.ds(n * chunk, chunk)], wo.at[n], w_sem.at[n])

    for n in range(n_chunks):
        w_load(n).start()
    barrier = pltpu.get_barrier_semaphore()
    for peer in (core_peer, x_peer, far_peer, y_peer):
        pl.semaphore_signal(barrier, inc=1, device_id=peer, device_id_type=mesh_id)
    pl.semaphore_wait(barrier, 4)

    stats[sp, :heads] = m_ref[...]
    stats[sp, heads:] = l_ref[...]
    st = [remote(stats.at[sp], stats.at[sp], st_send.at[i], st_recv.at[i], peer)
          for i, peer in enumerate((core_peer, x_peer, far_peer))]
    for copy in st:
        copy.start()
    for copy in st:
        copy.wait()
    tops = [stats[j, :heads] for j in range(4)]
    top = jnp.maximum(jnp.maximum(tops[0], tops[1]), jnp.maximum(tops[2], tops[3]))
    total = sum(stats[j, heads:] * jnp.exp(tops[j] - top) for j in range(4))
    factor = jnp.exp(m_ref[...] - top) / total
    for b in range(rows):
        at = pl.ds((b % quarter) * heads, heads)
        scaled[b // quarter, at, :] = o_ref[b * heads:(b + 1) * heads, :] * factor[:, b:b + 1]

    q_own = 2 * xpos + core
    q_far = 2 * (1 - xpos) + core
    p_own = 2 * xpos + (1 - core)
    p_far = 2 * (1 - xpos) + (1 - core)
    to_core = [remote(scaled.at[p_far], core_in.at[0], c_send.at[0], c_recv.at[0], core_peer),
               remote(scaled.at[p_own], core_in.at[1], c_send.at[1], c_recv.at[1], core_peer)]
    for copy in to_core:
        copy.start()
    to_core[0].wait_recv()
    to_x = []
    for i in range(halves):
        at = pl.ds(i * h_rows, h_rows)
        far_sum[at, :] = scaled[q_far, at, :] + core_in[0, at, :]
        copy = remote(far_sum.at[at], x_in.at[at], r_send.at[i], r_recv.at[i], x_peer)
        copy.start()
        to_x.append(copy)
    to_core[1].wait_recv()
    for copy in to_core:
        copy.wait_send()

    to_y = []
    for i in range(halves):
        to_x[i].wait_recv()
        for h in range(heads):
            at = pl.ds(i * h_rows + h, part, stride=heads)
            value = (scaled[q_own, at, :] + core_in[1, at, :]) + x_in[at, :]
            lhs[pl.ds(i * part, part), h * 128:(h + 1) * 128] = value.astype(jnp.bfloat16)
        at = pl.ds(i * part, part)

        def project(n, carry):
            if i == 0:
                w_load(n).wait()
            y_out[n, at, :] = jnp.dot(lhs[at, :], wo[n], preferred_element_type=jnp.float32)
            remote(y_out.at[n, at], y_in.at[n, at], y_send.at[i, n], y_recv.at[i, n], y_peer).start()
            return carry

        lax.fori_loop(0, n_chunks, project, 0)

    own = sums.at[sp]

    def piece(i, n):
        return pl.ds(i * part, part), pl.ds(n * chunk, chunk)

    def to_x_gather(i, n):
        r, c = piece(i, n)
        return remote(sums.at[sp, n, r], sums.at[sp, n, r], g_send.at[i, n], g_recv.at[i, n], x_peer)

    def to_core_gather(i, n):
        r, c = piece(i, n)
        return remote(sums.at[sp, n, r], sums.at[sp, n, r], d_send.at[i, n], d_recv.at[i, n], core_peer)

    def relay(i, n):
        r, c = piece(i, n)
        other = 2 * (1 - xpos) + core
        return remote(sums.at[other, n, r], sums.at[other, n, r], f_send.at[i, n], f_recv.at[i, n], core_peer)

    order = [(i, n) for i in range(halves) for n in range(n_chunks)]
    for t in range(len(order) + 1):
        if t < len(order):
            i, n = order[t]
            r, c = piece(i, n)
            remote(y_out.at[n, r], y_in.at[n, r], y_send.at[i, n], y_recv.at[i, n], y_peer).wait()
            sums[sp, n, r, :] = y_out[n, r, :] + y_in[n, r, :]
            to_x_gather(i, n).start()
            to_core_gather(i, n).start()
        if t >= 1:
            i, n = order[t - 1]
            to_x_gather(i, n).wait_recv()
            relay(i, n).start()
    for i, n in order:
        to_x_gather(i, n).wait_send()
        to_core_gather(i, n).wait()
        relay(i, n).wait()
    for copy in to_x:
        copy.wait_send()

    block = 16
    for q in range(4):
        def finish(k, carry):
            at = pl.ds(pl.multiple_of(k * block, block), block)
            out_at = pl.ds(pl.multiple_of(q * quarter + k * block, block), block)
            square = jnp.zeros((block, 1), jnp.float32)
            for n in range(n_chunks):
                u = sums[q, n, at, :]
                square = square + jnp.sum(u * u, axis=-1, keepdims=True)
            inv = lax.rsqrt(square * (1.0 / width) + NORM_EPS)
            for n in range(n_chunks):
                col = slice(n * chunk, (n + 1) * chunk)
                u = sums[q, n, at, :]
                y = x_ref[out_at, col].astype(jnp.float32) + u * inv * (1.0 + wpost_ref[:, col])
                out_ref[out_at, col] = y.astype(jnp.bfloat16)
            return carry
        lax.fori_loop(0, quarter // block, finish, 0)


def merge(o, m, l, x_in, w_post, w_o, halves, n_chunks):
    rows, width = x_in.shape
    inner = w_o.shape[0]
    heads = m.shape[0]
    head_dim = inner // heads
    quarter = rows // 4
    chunk = width // n_chunks
    vmem = pl.BlockSpec(memory_space=pltpu.VMEM)
    hbm = pl.BlockSpec(memory_space=pl.ANY)
    f32 = jnp.float32
    dma = pltpu.SemaphoreType.DMA
    pieces = dma((halves, n_chunks))
    return pl.pallas_call(
        functools.partial(merge_kernel, halves, 'sp', 'tp'),
        out_shape=jax.ShapeDtypeStruct(x_in.shape, x_in.dtype),
        in_specs=[vmem, vmem, vmem, vmem, vmem, hbm],
        out_specs=vmem,
        scratch_shapes=[
            pltpu.VMEM((n_chunks, inner, chunk), jnp.bfloat16),
            pltpu.VMEM((4, quarter * heads, head_dim), f32),
            pltpu.VMEM((4, 2 * heads, rows), f32),
            pltpu.VMEM((2, quarter * heads, head_dim), f32),
            pltpu.VMEM((quarter * heads, head_dim), f32),
            pltpu.VMEM((quarter, inner), jnp.bfloat16),
            pltpu.VMEM((n_chunks, quarter, chunk), f32),
            pltpu.VMEM((n_chunks, quarter, chunk), f32),
            pltpu.VMEM((4, n_chunks, quarter, chunk), f32),
            pltpu.VMEM((quarter * heads, head_dim), f32),
            dma((n_chunks,)), dma((3,)), dma((3,)), dma((2,)), dma((2,)), dma((halves,)), dma((halves,)),
            pieces, pieces, pieces, pieces, pieces, pieces, pieces, pieces,
        ],
        compiler_params=pltpu.CompilerParams(vmem_limit_bytes=56 * 1024 * 1024, collective_id=0, has_side_effects=True),
        cost_estimate=pl.CostEstimate(flops=2 * quarter * inner * width, bytes_accessed=2 * inner * width, transcendentals=0),
        name='merge',
    )(o, m, l, x_in, w_post, w_o)


def solution(mesh):
    cache_spec = P('dp', 'sp', 'tp', None)

    def local_step(x_in, cur_pos, w_pre, w_q, w_k, w_v, w_o, w_post, k_cache, v_cache):
        row_count, seq_block, kv_local, head_dim = k_cache.shape
        heads_local = w_q.shape[1] // head_dim
        sp_index = lax.axis_index('sp')
        x_f = x_in.astype(jnp.float32)
        normed = rms_scale(x_f, w_pre).astype(jnp.bfloat16)
        q_proj = jnp.dot(normed, w_q, preferred_element_type=jnp.float32)
        q_rot = rotary(q_proj.reshape(row_count, heads_local, head_dim), cur_pos).astype(jnp.bfloat16)
        k_proj = jnp.dot(normed, w_k, preferred_element_type=jnp.float32)
        k_new = rotary(k_proj.reshape(row_count, kv_local, head_dim), cur_pos).astype(jnp.bfloat16)
        v_new = jnp.dot(normed, w_v, preferred_element_type=jnp.float32).reshape(row_count, kv_local, head_dim).astype(jnp.bfloat16)
        kn2 = jnp.concatenate([k_new, k_new], axis=1)
        vn2 = jnp.concatenate([v_new, v_new], axis=1)
        base = (sp_index * seq_block).astype(jnp.int32).reshape(1)
        kc = k_cache.reshape(row_count, seq_block * kv_local, head_dim)
        vc = v_cache.reshape(row_count, seq_block * kv_local, head_dim)
        k_out, v_out, o, m, l = attend(cur_pos, base, q_rot, kn2, vn2, kc, vc, None, 0, row_count)

        x_out = merge(o.reshape(row_count * heads_local, head_dim), m, l, x_in, w_post.reshape(1, -1), w_o, 2, 9)
        return x_out, k_out.reshape(k_cache.shape), v_out.reshape(v_cache.shape)

    return jax.shard_map(local_step, mesh=mesh,
                         in_specs=(P('dp', None), P('dp'), P(None), P(None, 'tp'), P(None, 'tp'), P(None, 'tp'), P('tp', None), P(None), cache_spec, cache_spec),
                         out_specs=(P('dp', None), cache_spec, cache_spec), check_vma=False)
```

```python
import functools

import jax
import jax.numpy as jnp
from jax import lax
from jax.experimental import pallas as pl
from jax.experimental.pallas import tpu as pltpu
from jax.sharding import PartitionSpec as P


SOFT_CAP = 50.0
ROPE_BASE = 10000.0
NORM_EPS = 1e-6
LOG2E = 1.4426950408889634

ROWS_STEP = 16
SLOTS = 5
AHEAD = 3
LAG_SOFT = 2
LAG_OUT = 4


def rms_scale(tensor, gain_w):
    mean_sq = jnp.mean(tensor * tensor, axis=-1, keepdims=True)
    return tensor * lax.rsqrt(mean_sq + NORM_EPS) * (1.0 + gain_w)


def rotary(tensor, positions):
    half_dim = tensor.shape[-1] // 2
    inv_freq = ROPE_BASE ** (-2.0 * jnp.arange(half_dim, dtype=jnp.float32) / (2 * half_dim))
    angles = positions.astype(jnp.float32)[:, None] * inv_freq[None, :]
    angles = angles.reshape((angles.shape[0],) + (1,) * (tensor.ndim - 2) + (half_dim,))
    cos_tab = jnp.cos(angles)
    sin_tab = jnp.sin(angles)
    lo_half = tensor[..., :half_dim]
    hi_half = tensor[..., half_dim:]
    return jnp.concatenate([lo_half * cos_tab - hi_half * sin_tab, hi_half * cos_tab + lo_half * sin_tab], axis=-1)


def attend_kernel(n_steps, first_row, kv_heads, seq_block, pos_ref, base_ref, q_hbm, kn_hbm, vn_hbm, k_hbm, v_hbm,
                  *rest):
    (ko_hbm, vo_hbm, o0_hbm, o1_hbm, o2_hbm, o3_hbm, m_ref, l_ref, kbuf, vbuf, qbuf, knbuf, vnbuf, obuf, key_ref, s_ref, p_ref, in_sem, out_sem, o_sem, st_sem) = rest[-21:]
    step_rows = ROWS_STEP
    piece_steps = n_steps // 4
    heads, head_dim = qbuf.shape[2], qbuf.shape[3]
    cols = seq_block * kv_heads
    base = base_ref[0]

    row_id = lax.broadcasted_iota(jnp.int32, (heads, cols), 0)
    col_id = lax.broadcasted_iota(jnp.int32, (heads, cols), 1)
    mine = lax.rem(col_id, kv_heads) == row_id // (heads // kv_heads)
    key_ref[...] = jnp.where(mine, col_id, cols * 4)
    lane_id = lax.broadcasted_iota(jnp.int32, m_ref.shape, 1)
    half_id = lax.broadcasted_iota(jnp.int32, (2 * kv_heads, head_dim), 0) // kv_heads

    def loads(step, slot):
        rows = pl.ds(first_row + step * step_rows, step_rows)
        return (pltpu.make_async_copy(k_hbm.at[rows], kbuf.at[slot], in_sem.at[slot, 0]),
                pltpu.make_async_copy(v_hbm.at[rows], vbuf.at[slot], in_sem.at[slot, 1]),
                pltpu.make_async_copy(q_hbm.at[rows], qbuf.at[slot], in_sem.at[slot, 2]),
                pltpu.make_async_copy(kn_hbm.at[rows], knbuf.at[slot], in_sem.at[slot, 3]),
                pltpu.make_async_copy(vn_hbm.at[rows], vnbuf.at[slot], in_sem.at[slot, 4]))

    def stores(step, slot):
        rows = pl.ds(first_row + step * step_rows, step_rows)
        return (pltpu.make_async_copy(kbuf.at[slot], ko_hbm.at[rows], out_sem.at[slot, 0]),
                pltpu.make_async_copy(vbuf.at[slot], vo_hbm.at[rows], out_sem.at[slot, 1]))

    def o_store(step, slot, d=0):
        at = pl.ds(lax.rem(step, piece_steps) * step_rows * heads, step_rows * heads)
        o_hbm = (o0_hbm, o1_hbm, o2_hbm, o3_hbm)[d]
        return pltpu.make_async_copy(obuf.at[slot], o_hbm.at[at], o_sem.at[slot])

    def o_start(step, slot):
        turn = jnp.bitwise_xor(step // piece_steps, base // seq_block)
        for d in range(4):
            @pl.when(turn == d)
            def _():
                o_store(step, slot, d).start()

    for step in range(min(AHEAD, n_steps)):
        for copy in loads(step, step):
            copy.start()
    m_ref[...] = jnp.zeros_like(m_ref)
    l_ref[...] = jnp.zeros_like(l_ref)
    scale = head_dim ** -0.5 / SOFT_CAP

    def body(step, carry):
        slot = lax.rem(step, SLOTS)
        oslot = lax.rem(step, 2)
        for copy in loads(step, slot):
            copy.wait()

        for r in range(step_rows):
            local = pos_ref[first_row + step * step_rows + r] - base
            inside = (local >= 0) & (local < seq_block)
            at = jnp.clip(local, 0, seq_block - 1)
            pair = pl.ds(pl.multiple_of((at // 2) * (2 * kv_heads), 2 * kv_heads), 2 * kv_heads)
            hit = half_id == jnp.where(inside, lax.rem(at, 2), 2)
            kbuf[slot, r, pair, :] = jnp.where(hit, knbuf[slot, r], kbuf[slot, r, pair, :])
            vbuf[slot, r, pair, :] = jnp.where(hit, vnbuf[slot, r], vbuf[slot, r, pair, :])

        @pl.when(step >= 2)
        def _():
            o_store(step - 2, oslot).wait()

        m_all = m_ref[...]
        l_all = l_ref[...]
        half = cols // 2
        for tick in range(step_rows + LAG_OUT):
            r = tick
            if r < step_rows:
                raw = lax.dot_general(qbuf[slot, r], kbuf[slot, r], (((1,), (1,)), ((), ())),
                                      preferred_element_type=jnp.float32)
                s_ref[r] = raw
            r = tick - LAG_SOFT
            if 0 <= r < step_rows:
                local = pos_ref[first_row + step * step_rows + r] - base
                seen = key_ref[...] < (local + 1) * kv_heads
                soft = jnp.where(seen, jnp.tanh(s_ref[r] * scale), -4.0)
                top = jnp.maximum(jnp.max(soft, axis=-1, keepdims=True), -1.0)
                weight = jnp.exp2((soft - top) * (SOFT_CAP * LOG2E))
                total = jnp.sum(weight, axis=-1, keepdims=True)
                weight = weight.astype(jnp.bfloat16)
                p_ref[r, :heads] = weight[:, :half]
                p_ref[r, heads:] = weight[:, half:]
                here = lane_id == step * step_rows + r
                m_all = jnp.where(here, top * SOFT_CAP, m_all)
                l_all = jnp.where(here, total, l_all)
            r = tick - LAG_OUT
            if 0 <= r < step_rows:
                right = jnp.concatenate([vbuf[slot, r, :half, :], vbuf[slot, r, half:, :]], axis=1)
                both = jnp.dot(p_ref[r], right, preferred_element_type=jnp.float32)
                obuf[oslot, r * heads:(r + 1) * heads, :] = both[:heads, :head_dim] + both[heads:, head_dim:]
        m_ref[...] = m_all
        l_ref[...] = l_all
        o_start(step, oslot)
        for copy in stores(step, slot):
            copy.start()

        @pl.when(step + AHEAD < n_steps)
        def _():
            nxt = step + AHEAD
            nslot = lax.rem(nxt, SLOTS)

            @pl.when(nxt >= SLOTS)
            def _():
                for copy in stores(nxt - SLOTS, nslot):
                    copy.wait()

            for copy in loads(nxt, nslot):
                copy.start()

        return carry

    lax.fori_loop(0, n_steps, body, 0)
    tail = piece_steps * step_rows * heads
    stat_copies = []
    for d, o_hbm in enumerate((o0_hbm, o1_hbm, o2_hbm, o3_hbm)):
        stat_copies.append(pltpu.make_async_copy(m_ref, o_hbm.at[pl.ds(tail, heads)], st_sem.at[d, 0]))
        stat_copies.append(pltpu.make_async_copy(l_ref, o_hbm.at[pl.ds(tail + heads, heads)], st_sem.at[d, 1]))
    for copy in stat_copies:
        copy.start()
    for copy in stat_copies:
        copy.wait()
    for step in range(max(0, n_steps - SLOTS), n_steps):
        for copy in stores(step, step % SLOTS):
            copy.wait()
    for step in range(max(0, n_steps - 2), n_steps):
        o_store(step, step % 2).wait()


def attend(pos, base, q, kn, vn, k_cache, v_cache, prev, first_row, n_rows):
    _, cols, head_dim = k_cache.shape
    heads = q.shape[1]
    kv_heads = kn.shape[1] // 2
    seq_block = cols // kv_heads
    n_steps = n_rows // ROWS_STEP
    hbm = pl.BlockSpec(memory_space=pl.ANY)
    piece = jax.ShapeDtypeStruct((n_rows // 4 * heads + 2 * heads, head_dim), jnp.float32)
    smem = pl.BlockSpec(memory_space=pltpu.SMEM)
    bf = jnp.bfloat16
    aliases = {} if prev is None else {7: 0, 8: 1}
    extra = () if prev is None else tuple(prev)
    return pl.pallas_call(
        functools.partial(attend_kernel, n_steps, first_row, kv_heads, seq_block),
        out_shape=(jax.ShapeDtypeStruct(k_cache.shape, bf), jax.ShapeDtypeStruct(v_cache.shape, bf)) + (piece,) * 4,
        in_specs=[smem, smem, hbm, hbm, hbm, hbm, hbm] + [hbm] * len(extra),
        out_specs=(hbm,) * 6,
        scratch_shapes=[
            pltpu.VMEM((heads, 128), jnp.float32),
            pltpu.VMEM((heads, 128), jnp.float32),
            pltpu.VMEM((SLOTS, ROWS_STEP, cols, head_dim), bf),
            pltpu.VMEM((SLOTS, ROWS_STEP, cols, head_dim), bf),
            pltpu.VMEM((SLOTS, ROWS_STEP, heads, head_dim), bf),
            pltpu.VMEM((SLOTS, ROWS_STEP, 2 * kv_heads, head_dim), bf),
            pltpu.VMEM((SLOTS, ROWS_STEP, 2 * kv_heads, head_dim), bf),
            pltpu.VMEM((2, ROWS_STEP * heads, head_dim), jnp.float32),
            pltpu.VMEM((heads, cols), jnp.int32),
            pltpu.VMEM((ROWS_STEP, heads, cols), jnp.float32),
            pltpu.VMEM((ROWS_STEP, 2 * heads, cols // 2), bf),
            pltpu.SemaphoreType.DMA((SLOTS, 5)),
            pltpu.SemaphoreType.DMA((SLOTS, 2)),
            pltpu.SemaphoreType.DMA((2,)),
            pltpu.SemaphoreType.DMA((4, 2)),
        ],
        input_output_aliases=aliases,
        compiler_params=pltpu.CompilerParams(vmem_limit_bytes=40 * 1024 * 1024),
        cost_estimate=pl.CostEstimate(flops=n_rows * heads * cols * head_dim * 4,
                                      bytes_accessed=n_rows * cols * head_dim * 8, transcendentals=0),
        name='attend',
    )(pos, base, q, kn, vn, k_cache, v_cache, *extra)


def merge_kernel(chunks, *refs):
    n_in = 4 * len(chunks)
    source = [refs[4 * c:4 * c + 4] for c in range(len(chunks))]
    pieces = [[b.at[d] for d in range(4)] for b in refs[-len(chunks):]]
    refs = refs[:-len(chunks)]
    (x_hbm, wpost_hbm, wo_hbm, out_ref, wo, xbuf, wpost_ref, last_in, osum, lhs, y_out, y_in, sums,
     in_sem, p_sem, w_sem, o_send, o_recv, y_send, y_recv, g_send, g_recv, d_send, d_recv, f_send, f_recv) = refs[n_in:]
    sp = lax.axis_index('sp')
    tp = lax.axis_index('tp')
    core = lax.rem(sp, 2)
    xpos = sp // 2
    _, width = xbuf.shape
    n_chunks, quarter, chunk = y_out.shape
    heads = lhs.shape[1] // 128
    parts = [c // 4 for c in chunks]
    core_peer = {'sp': 2 * xpos + (1 - core)}
    x_peer = {'sp': 2 * (1 - xpos) + core}
    far_peer = {'sp': 2 * (1 - xpos) + (1 - core)}
    y_peer = {'tp': 1 - tp}
    mesh_id = pl.DeviceIdType.MESH

    def remote(src, dst, send, recv, peer):
        return pltpu.make_async_remote_copy(src_ref=src, dst_ref=dst, send_sem=send, recv_sem=recv,
                                            device_id=peer, device_id_type=mesh_id)

    def w_load(n):
        return pltpu.make_async_copy(wo_hbm.at[:, pl.ds(n * chunk, chunk)], wo.at[n], w_sem.at[n])

    small = [pltpu.make_async_copy(x_hbm, xbuf, in_sem.at[0]), pltpu.make_async_copy(wpost_hbm, wpost_ref, in_sem.at[1])]
    local = [[pltpu.make_async_copy(source[c][d], pieces[c][d], p_sem.at[c, d]) for d in range(4)] for c in range(len(chunks))]
    for group in local:
        for copy in group:
            copy.start()
    for n in range(n_chunks):
        w_load(n).start()
    for copy in small:
        copy.start()
    barrier = pltpu.get_barrier_semaphore()
    for peer in (core_peer, x_peer, far_peer, y_peer):
        pl.semaphore_signal(barrier, inc=1, device_id=peer, device_id_type=mesh_id)
    pl.semaphore_wait(barrier, 4)

    for copy in local[-1]:
        copy.wait()
    last = [remote(pieces[-1][d], last_in.at[d - 1], o_send.at[d - 1], o_recv.at[d - 1], peer)
            for d, peer in ((2, x_peer), (3, far_peer), (1, core_peer))]
    for copy in last:
        copy.start()

    def combine(blocks, part, row0):
        count = part * heads
        stats = [block[count:count + 2 * heads, :] for block in blocks]
        top = functools.reduce(jnp.maximum, [st[:heads] for st in stats])
        grown = [jnp.exp(st[:heads] - top) for st in stats]
        total = sum(st[heads:] * g for st, g in zip(stats, grown))
        shift = lax.rem(128 - sp * part, 128)
        factors = [pltpu.roll(g / total, shift, 1) for g in grown]
        for b in range(part):
            at = slice(b * heads, (b + 1) * heads)
            osum[at, :] = sum(block[at, :] * f[:, b:b + 1] for block, f in zip(blocks, factors))
        for h in range(heads):
            lhs[row0:row0 + part, h * 128:(h + 1) * 128] = osum[pl.ds(h, part, stride=heads), :].astype(jnp.bfloat16)

    first = sum(parts[:-1])
    row0 = 0
    for c in range(len(chunks) - 1):
        for copy in local[c]:
            copy.wait()
        combine(pieces[c], parts[c], row0)
        row0 += parts[c]

    wide = 3
    first_at, last_at = pl.ds(0, first), pl.ds(first, quarter - first)
    order = [(pl.ds(n, 1), first_at) for n in range(n_chunks)] + [(pl.ds(n, wide), last_at) for n in range(0, n_chunks, wide)]

    def to_y(t):
        ns, r = order[t]
        return remote(y_out.at[ns, r], y_in.at[ns, r], y_send.at[t], y_recv.at[t], y_peer)

    def to_x(t):
        ns, r = order[t]
        return remote(sums.at[sp, ns, r], sums.at[sp, ns, r], g_send.at[t], g_recv.at[t], x_peer)

    def to_core(t):
        ns, r = order[t]
        return remote(sums.at[sp, ns, r], sums.at[sp, ns, r], d_send.at[t], d_recv.at[t], core_peer)

    def relay(t):
        ns, r = order[t]
        other = 2 * (1 - xpos) + core
        return remote(sums.at[other, ns, r], sums.at[other, ns, r], f_send.at[t], f_recv.at[t], core_peer)

    def project(n, r0, count):
        y_out[n, r0:r0 + count, :] = jnp.dot(lhs[r0:r0 + count, :], wo[n], preferred_element_type=jnp.float32)

    for n in range(n_chunks):
        w_load(n).wait()
        project(n, 0, first)
        to_y(n).start()

    for t in range(len(order) + 1):
        if t == 2:
            for copy in last:
                copy.wait()
            combine([pieces[-1][0]] + [last_in.at[d] for d in range(3)], parts[-1], first)
        if 2 <= t < 2 + n_chunks // wide:
            for n in range((t - 2) * wide, (t - 1) * wide):
                project(n, first, quarter - first)
            to_y(n_chunks + t - 2).start()
        if t < len(order):
            ns, r = order[t]
            to_y(t).wait()
            sums[sp, ns, r, :] = y_out[ns, r, :] + y_in[ns, r, :]
            to_x(t).start()
            to_core(t).start()
        if t >= 1:
            to_x(t - 1).wait_recv()
            relay(t - 1).start()
    for copy in small:
        copy.wait()
    for t in range(len(order)):
        to_x(t).wait_send()
        to_core(t).wait()
        relay(t).wait()

    starts = []
    base = 0
    for c, part in zip(chunks, parts):
        starts += [(base, part, k) for k in range(0, part, 16)]
        base += c
    for q in range(4):
        for k, (base, part, off) in enumerate(starts):
            at = slice(k * 16, (k + 1) * 16)
            out_at = slice(base + q * part + off, base + q * part + off + 16)
            square = jnp.zeros((16, chunk), jnp.float32)
            for n in range(n_chunks):
                u = sums[q, n, at, :]
                square = square + u * u
            inv = lax.rsqrt(jnp.sum(square, axis=-1, keepdims=True) * (1.0 / width) + NORM_EPS)
            for n in range(n_chunks):
                col = slice(n * chunk, (n + 1) * chunk)
                y = xbuf[out_at, col].astype(jnp.float32) + sums[q, n, at, :] * inv * (1.0 + wpost_ref[:, col])
                out_ref[out_at, col] = y.astype(jnp.bfloat16)


def merge(chunks, pieces, x_in, w_post, w_o, n_chunks):
    rows, width = x_in.shape
    inner = w_o.shape[0]
    heads = inner // 128
    quarter = rows // 4
    chunk = width // n_chunks
    vmem = pl.BlockSpec(memory_space=pltpu.VMEM)
    hbm = pl.BlockSpec(memory_space=pl.ANY)
    f32 = jnp.float32
    dma = pltpu.SemaphoreType.DMA
    per_piece = dma((n_chunks + 3,))
    flat = [p for piece in pieces for p in piece]
    big = max(chunks) // 4 * heads
    return pl.pallas_call(
        functools.partial(merge_kernel, chunks),
        out_shape=jax.ShapeDtypeStruct(x_in.shape, x_in.dtype),
        in_specs=[hbm] * (len(flat) + 3),
        out_specs=vmem,
        scratch_shapes=[
            pltpu.VMEM((n_chunks, inner, chunk), jnp.bfloat16),
            pltpu.VMEM(x_in.shape, x_in.dtype),
            pltpu.VMEM(w_post.shape, f32),
            pltpu.VMEM((3,) + pieces[-1][0].shape, f32),
            pltpu.VMEM((big, 128), f32),
            pltpu.VMEM((quarter, inner), jnp.bfloat16),
            pltpu.VMEM((n_chunks, quarter, chunk), f32),
            pltpu.VMEM((n_chunks, quarter, chunk), f32),
            pltpu.VMEM((4, n_chunks, quarter, chunk), f32),
            dma((2,)), dma((len(chunks), 4)), dma((n_chunks,)), dma((3,)), dma((3,)),
        ] + [per_piece] * 8 + [pltpu.VMEM((4,) + piece[0].shape, f32) for piece in pieces],
        compiler_params=pltpu.CompilerParams(vmem_limit_bytes=56 * 1024 * 1024, collective_id=0, has_side_effects=True),
        cost_estimate=pl.CostEstimate(flops=2 * quarter * inner * width, bytes_accessed=2 * inner * width, transcendentals=0),
        name='merge',
    )(*flat, x_in, w_post, w_o)


def solution(mesh):
    cache_spec = P('dp', 'sp', 'tp', None)
    sp_size = mesh.shape['sp']

    def local_step(x_in, cur_pos, w_pre, w_q, w_k, w_v, w_o, w_post, k_cache, v_cache):
        row_count, seq_block, kv_local, head_dim = k_cache.shape
        heads_local = w_q.shape[1] // head_dim
        sp_index = lax.axis_index('sp')
        x_f = x_in.astype(jnp.float32)
        normed = rms_scale(x_f, w_pre).astype(jnp.bfloat16)
        q_proj = jnp.dot(normed, w_q, preferred_element_type=jnp.float32)
        q_rot = rotary(q_proj.reshape(row_count, heads_local, head_dim), cur_pos).astype(jnp.bfloat16)
        k_proj = jnp.dot(normed, w_k, preferred_element_type=jnp.float32)
        k_new = rotary(k_proj.reshape(row_count, kv_local, head_dim), cur_pos).astype(jnp.bfloat16)
        v_new = jnp.dot(normed, w_v, preferred_element_type=jnp.float32).reshape(row_count, kv_local, head_dim).astype(jnp.bfloat16)
        kn2 = jnp.concatenate([k_new, k_new], axis=1)
        vn2 = jnp.concatenate([v_new, v_new], axis=1)
        base = (sp_index * seq_block).astype(jnp.int32).reshape(1)
        kc = k_cache.reshape(row_count, seq_block * kv_local, head_dim)
        vc = v_cache.reshape(row_count, seq_block * kv_local, head_dim)
        chunks = (row_count // 2, row_count // 4, row_count // 4)
        prev, first_row, pieces = None, 0, []
        for index, n_rows in enumerate(chunks):
            *prev, p0, p1, p2, p3 = attend(cur_pos, base, q_rot, kn2, vn2, kc, vc, prev, first_row, n_rows)
            first_row += n_rows
            if index < len(chunks) - 1:
                moved = []
                for d, p in ((1, p1), (2, p2), (3, p3)):
                    moved.append(lax.ppermute(p, 'sp', [(i, i ^ d) for i in range(sp_size)]))
                p1, p2, p3 = moved
            pieces.append((p0, p1, p2, p3))
        k_out, v_out = prev
        x_out = merge(chunks, pieces, x_in, w_post.reshape(1, -1), w_o, 9)
        return x_out, k_out.reshape(k_cache.shape), v_out.reshape(v_cache.shape)

    return jax.shard_map(local_step, mesh=mesh,
                         in_specs=(P('dp', None), P('dp'), P(None), P(None, 'tp'), P(None, 'tp'), P(None, 'tp'), P('tp', None), P(None), cache_spec, cache_spec),
                         out_specs=(P('dp', None), cache_spec, cache_spec), check_vma=False)
```

```python
import functools

import jax
import jax.numpy as jnp
from jax import lax
from jax.experimental import pallas as pl
from jax.experimental.pallas import tpu as pltpu
from jax.sharding import PartitionSpec as P


SOFT_CAP = 50.0
ROPE_BASE = 10000.0
NORM_EPS = 1e-6
LOG2E = 1.4426950408889634

ROWS_STEP = 16
SLOTS = 5
AHEAD = 3
LAG_SOFT = 2
LAG_OUT = 4


def rotary_tables(positions, head_dim):
    half_dim = head_dim // 2
    inv_freq = ROPE_BASE ** (-2.0 * jnp.arange(half_dim, dtype=jnp.float32) / (2 * half_dim))
    angles = positions.astype(jnp.float32)[:, None] * inv_freq[None, :]
    cos_tab = jnp.cos(angles)
    sin_tab = jnp.sin(angles)
    return jnp.concatenate([cos_tab, cos_tab], axis=-1), jnp.concatenate([-sin_tab, sin_tab], axis=-1)


def project_kernel(x_ref, wpre_ref, cos_ref, sin_ref, wq_hbm, wk_hbm, wv_hbm, q_ref, k_ref, v_ref,
                   weight, normed, q_part, k_part, v_part, w_sem, send_sem, recv_sem):
    sp = lax.axis_index('sp')
    core = lax.rem(sp, 2)
    peer = {'sp': sp + 1 - 2 * core}
    mesh_id = pl.DeviceIdType.MESH
    rows = x_ref.shape[0]
    block = weight.shape[2]
    per = block // 128
    plan = []
    for w_hbm, part, turn in ((wq_hbm, q_part, True), (wk_hbm, k_part, True), (wv_hbm, v_part, False)):
        mine = w_hbm.shape[1] // 2
        for j in range(mine // block):
            plan.append((w_hbm, part, turn, mine, j, j == mine // block - 1))

    def load(i):
        w_hbm, _, _, mine, j, _ = plan[i]
        col = pl.multiple_of(core * mine + j * block, block)
        return pltpu.make_async_copy(w_hbm.at[:, pl.ds(col, block)], weight.at[i], w_sem.at[i])

    for i in range(len(plan)):
        load(i).start()
    barrier = pltpu.get_barrier_semaphore()
    pl.semaphore_signal(barrier, inc=1, device_id=peer, device_id_type=mesh_id)
    pl.semaphore_wait(barrier, 1)

    gain = 1.0 + wpre_ref[...]

    def norm(k, carry):
        at = pl.ds(pl.multiple_of(k * 16, 16), 16)
        x = x_ref[at, :].astype(jnp.float32)
        inv = lax.rsqrt(jnp.mean(x * x, axis=-1, keepdims=True) + NORM_EPS)
        normed[at, :] = (x * inv * gain).astype(jnp.bfloat16)
        return carry

    lax.fori_loop(0, rows // 16, norm, 0)

    sends = []
    for i, (_, part, turn, mine, j, done) in enumerate(plan):
        load(i).wait()
        heads = mine // 128
        acc = jnp.dot(normed[...], weight[i], preferred_element_type=jnp.float32)
        for t in range(per):
            value = acc[:, t * 128:(t + 1) * 128]
            if turn:
                value = value * cos_ref[...] + pltpu.roll(value, 64, 1) * sin_ref[...]
            part[core, pl.ds(j * per + t, rows, stride=heads), :] = value
        if done:
            n = len(sends)
            copy = pltpu.make_async_remote_copy(src_ref=part.at[core], dst_ref=part.at[core], send_sem=send_sem.at[n],
                                                recv_sem=recv_sem.at[n], device_id=peer, device_id_type=mesh_id)
            copy.start()
            sends.append(copy)
    for copy in sends:
        copy.wait()

    q_heads = q_part.shape[1] // rows
    kv = k_part.shape[1] // rows

    def pack(k, carry):
        for r in range(8):
            b = k * 8 + r
            at = pl.ds(pl.multiple_of(b * q_heads, q_heads), q_heads)
            q_ref[b] = jnp.concatenate([q_part[0, at, :], q_part[1, at, :]], axis=0).astype(jnp.bfloat16)
        for part, out in ((k_part, k_ref), (v_part, v_ref)):
            group = pl.ds(pl.multiple_of(k * 8 * kv, 8), 8 * kv)
            low, high = part[0, group, :], part[1, group, :]
            for r in range(8):
                both = [low[r * kv:(r + 1) * kv], high[r * kv:(r + 1) * kv]]
                out[k * 8 + r] = jnp.concatenate(both + both, axis=0).astype(jnp.bfloat16)
        return carry

    lax.fori_loop(0, rows // 8, pack, 0)


def project(x_in, w_pre, cos_tab, sin_tab, w_q, w_k, w_v):
    rows, width = x_in.shape
    block = 256
    q_cols, kv_cols = w_q.shape[1], w_k.shape[1]
    n_blocks = (q_cols + 2 * kv_cols) // 2 // block
    vmem = pl.BlockSpec(memory_space=pltpu.VMEM)
    hbm = pl.BlockSpec(memory_space=pltpu.HBM)
    f32, bf = jnp.float32, jnp.bfloat16
    dma = pltpu.SemaphoreType.DMA
    return pl.pallas_call(
        project_kernel,
        out_shape=(jax.ShapeDtypeStruct((rows, q_cols // 128, 128), bf),
                   jax.ShapeDtypeStruct((rows, kv_cols // 64, 128), bf),
                   jax.ShapeDtypeStruct((rows, kv_cols // 64, 128), bf)),
        in_specs=[vmem] * 4 + [hbm] * 3,
        out_specs=(vmem,) * 3,
        scratch_shapes=[
            pltpu.VMEM((n_blocks, width, block), bf),
            pltpu.VMEM((rows, width), bf),
            pltpu.VMEM((2, rows * q_cols // 256, 128), f32),
            pltpu.VMEM((2, rows * kv_cols // 256, 128), f32),
            pltpu.VMEM((2, rows * kv_cols // 256, 128), f32),
            dma((n_blocks,)), dma((3,)), dma((3,)),
        ],
        compiler_params=pltpu.CompilerParams(vmem_limit_bytes=44 * 1024 * 1024, collective_id=1, has_side_effects=True),
        cost_estimate=pl.CostEstimate(flops=rows * width * (q_cols + 2 * kv_cols), bytes_accessed=width * (q_cols + 2 * kv_cols), transcendentals=0),
        name='project',
    )(x_in, w_pre, cos_tab, sin_tab, w_q, w_k, w_v)


def attend_kernel(n_steps, first_row, kv_heads, seq_block, pos_ref, base_ref, q_hbm, kn_hbm, vn_hbm, k_hbm, v_hbm,
                  *rest):
    (ko_hbm, vo_hbm, o0_hbm, o1_hbm, o2_hbm, o3_hbm, m_ref, l_ref, kbuf, vbuf, qbuf, knbuf, vnbuf, obuf, key_ref, s_ref, p_ref, in_sem, out_sem, o_sem, st_sem) = rest[-21:]
    step_rows = ROWS_STEP
    piece_steps = n_steps // 4
    heads, head_dim = qbuf.shape[2], qbuf.shape[3]
    cols = seq_block * kv_heads
    base = base_ref[0]

    row_id = lax.broadcasted_iota(jnp.int32, (heads, cols), 0)
    col_id = lax.broadcasted_iota(jnp.int32, (heads, cols), 1)
    mine = lax.rem(col_id, kv_heads) == row_id // (heads // kv_heads)
    key_ref[...] = jnp.where(mine, col_id, cols * 4)
    lane_id = lax.broadcasted_iota(jnp.int32, m_ref.shape, 1)
    half_id = lax.broadcasted_iota(jnp.int32, (2 * kv_heads, head_dim), 0) // kv_heads

    def loads(step, slot):
        rows = pl.ds(first_row + step * step_rows, step_rows)
        return (pltpu.make_async_copy(k_hbm.at[rows], kbuf.at[slot], in_sem.at[slot, 0]),
                pltpu.make_async_copy(v_hbm.at[rows], vbuf.at[slot], in_sem.at[slot, 1]),
                pltpu.make_async_copy(q_hbm.at[rows], qbuf.at[slot], in_sem.at[slot, 2]),
                pltpu.make_async_copy(kn_hbm.at[rows], knbuf.at[slot], in_sem.at[slot, 3]),
                pltpu.make_async_copy(vn_hbm.at[rows], vnbuf.at[slot], in_sem.at[slot, 4]))

    def stores(step, slot):
        rows = pl.ds(first_row + step * step_rows, step_rows)
        return (pltpu.make_async_copy(kbuf.at[slot], ko_hbm.at[rows], out_sem.at[slot, 0]),
                pltpu.make_async_copy(vbuf.at[slot], vo_hbm.at[rows], out_sem.at[slot, 1]))

    def o_store(step, slot, d=0):
        at = pl.ds(lax.rem(step, piece_steps) * step_rows * heads, step_rows * heads)
        o_hbm = (o0_hbm, o1_hbm, o2_hbm, o3_hbm)[d]
        return pltpu.make_async_copy(obuf.at[slot], o_hbm.at[at], o_sem.at[slot])

    def o_start(step, slot):
        turn = jnp.bitwise_xor(step // piece_steps, base // seq_block)
        for d in range(4):
            @pl.when(turn == d)
            def _():
                o_store(step, slot, d).start()

    for step in range(min(AHEAD, n_steps)):
        for copy in loads(step, step):
            copy.start()
    m_ref[...] = jnp.zeros_like(m_ref)
    l_ref[...] = jnp.zeros_like(l_ref)
    scale = head_dim ** -0.5 / SOFT_CAP

    def body(step, carry):
        slot = lax.rem(step, SLOTS)
        oslot = lax.rem(step, 2)
        for copy in loads(step, slot):
            copy.wait()

        for r in range(step_rows):
            local = pos_ref[first_row + step * step_rows + r] - base
            inside = (local >= 0) & (local < seq_block)
            at = jnp.clip(local, 0, seq_block - 1)
            pair = pl.ds(pl.multiple_of((at // 2) * (2 * kv_heads), 2 * kv_heads), 2 * kv_heads)
            hit = half_id == jnp.where(inside, lax.rem(at, 2), 2)
            kbuf[slot, r, pair, :] = jnp.where(hit, knbuf[slot, r], kbuf[slot, r, pair, :])
            vbuf[slot, r, pair, :] = jnp.where(hit, vnbuf[slot, r], vbuf[slot, r, pair, :])

        @pl.when(step >= 2)
        def _():
            o_store(step - 2, oslot).wait()

        m_all = m_ref[...]
        l_all = l_ref[...]
        half = cols // 2
        for tick in range(step_rows + LAG_OUT):
            r = tick
            if r < step_rows:
                raw = lax.dot_general(qbuf[slot, r], kbuf[slot, r], (((1,), (1,)), ((), ())),
                                      preferred_element_type=jnp.float32)
                s_ref[r] = raw
            r = tick - LAG_SOFT
            if 0 <= r < step_rows:
                local = pos_ref[first_row + step * step_rows + r] - base
                seen = key_ref[...] < (local + 1) * kv_heads
                soft = jnp.where(seen, jnp.tanh(s_ref[r] * scale), -4.0)
                top = jnp.maximum(jnp.max(soft, axis=-1, keepdims=True), -1.0)
                weight = jnp.exp2((soft - top) * (SOFT_CAP * LOG2E))
                total = jnp.sum(weight, axis=-1, keepdims=True)
                weight = weight.astype(jnp.bfloat16)
                p_ref[r, :heads] = weight[:, :half]
                p_ref[r, heads:] = weight[:, half:]
                here = lane_id == step * step_rows + r
                m_all = jnp.where(here, top * SOFT_CAP, m_all)
                l_all = jnp.where(here, total, l_all)
            r = tick - LAG_OUT
            if 0 <= r < step_rows:
                right = jnp.concatenate([vbuf[slot, r, :half, :], vbuf[slot, r, half:, :]], axis=1)
                both = jnp.dot(p_ref[r], right, preferred_element_type=jnp.float32)
                obuf[oslot, r * heads:(r + 1) * heads, :] = both[:heads, :head_dim] + both[heads:, head_dim:]
        m_ref[...] = m_all
        l_ref[...] = l_all
        o_start(step, oslot)
        for copy in stores(step, slot):
            copy.start()

        @pl.when(step + AHEAD < n_steps)
        def _():
            nxt = step + AHEAD
            nslot = lax.rem(nxt, SLOTS)

            @pl.when(nxt >= SLOTS)
            def _():
                for copy in stores(nxt - SLOTS, nslot):
                    copy.wait()

            for copy in loads(nxt, nslot):
                copy.start()

        return carry

    lax.fori_loop(0, n_steps, body, 0)
    tail = piece_steps * step_rows * heads
    stat_copies = []
    for d, o_hbm in enumerate((o0_hbm, o1_hbm, o2_hbm, o3_hbm)):
        stat_copies.append(pltpu.make_async_copy(m_ref, o_hbm.at[pl.ds(tail, heads)], st_sem.at[d, 0]))
        stat_copies.append(pltpu.make_async_copy(l_ref, o_hbm.at[pl.ds(tail + heads, heads)], st_sem.at[d, 1]))
    for copy in stat_copies:
        copy.start()
    for copy in stat_copies:
        copy.wait()
    for step in range(max(0, n_steps - SLOTS), n_steps):
        for copy in stores(step, step % SLOTS):
            copy.wait()
    for step in range(max(0, n_steps - 2), n_steps):
        o_store(step, step % 2).wait()


def attend(pos, base, q, kn, vn, k_cache, v_cache, prev, first_row, n_rows):
    _, cols, head_dim = k_cache.shape
    heads = q.shape[1]
    kv_heads = kn.shape[1] // 2
    seq_block = cols // kv_heads
    n_steps = n_rows // ROWS_STEP
    hbm = pl.BlockSpec(memory_space=pl.ANY)
    piece = pltpu.HBM((n_rows // 4 * heads + 2 * heads, head_dim), jnp.float32)
    smem = pl.BlockSpec(memory_space=pltpu.SMEM)
    bf = jnp.bfloat16
    aliases = {} if prev is None else {7: 0, 8: 1}
    extra = () if prev is None else tuple(prev)
    return pl.pallas_call(
        functools.partial(attend_kernel, n_steps, first_row, kv_heads, seq_block),
        out_shape=(jax.ShapeDtypeStruct(k_cache.shape, bf), jax.ShapeDtypeStruct(v_cache.shape, bf)) + (piece,) * 4,
        in_specs=[smem, smem, hbm, hbm, hbm, hbm, hbm] + [hbm] * len(extra),
        out_specs=(hbm, hbm) + (pl.BlockSpec(memory_space=pltpu.HBM),) * 4,
        scratch_shapes=[
            pltpu.VMEM((heads, 128), jnp.float32),
            pltpu.VMEM((heads, 128), jnp.float32),
            pltpu.VMEM((SLOTS, ROWS_STEP, cols, head_dim), bf),
            pltpu.VMEM((SLOTS, ROWS_STEP, cols, head_dim), bf),
            pltpu.VMEM((SLOTS, ROWS_STEP, heads, head_dim), bf),
            pltpu.VMEM((SLOTS, ROWS_STEP, 2 * kv_heads, head_dim), bf),
            pltpu.VMEM((SLOTS, ROWS_STEP, 2 * kv_heads, head_dim), bf),
            pltpu.VMEM((2, ROWS_STEP * heads, head_dim), jnp.float32),
            pltpu.VMEM((heads, cols), jnp.int32),
            pltpu.VMEM((ROWS_STEP, heads, cols), jnp.float32),
            pltpu.VMEM((ROWS_STEP, 2 * heads, cols // 2), bf),
            pltpu.SemaphoreType.DMA((SLOTS, 5)),
            pltpu.SemaphoreType.DMA((SLOTS, 2)),
            pltpu.SemaphoreType.DMA((2,)),
            pltpu.SemaphoreType.DMA((4, 2)),
        ],
        input_output_aliases=aliases,
        compiler_params=pltpu.CompilerParams(vmem_limit_bytes=40 * 1024 * 1024),
        cost_estimate=pl.CostEstimate(flops=n_rows * heads * cols * head_dim * 4,
                                      bytes_accessed=n_rows * cols * head_dim * 8, transcendentals=0),
        name='attend',
    )(pos, base, q, kn, vn, k_cache, v_cache, *extra)


def merge_kernel(chunks, *refs):
    n_in = 4 * len(chunks)
    source = [refs[4 * c:4 * c + 4] for c in range(len(chunks))]
    pieces = [[b.at[d] for d in range(4)] for b in refs[-len(chunks):]]
    refs = refs[:-len(chunks)]
    (x_hbm, wpost_hbm, wo_hbm, out_ref, wo, xbuf, wpost_ref, last_in, osum, lhs, y_out, y_in, sums,
     in_sem, p_sem, w_sem, o_send, o_recv, y_send, y_recv, g_send, g_recv, d_send, d_recv, f_send, f_recv) = refs[n_in:]
    sp = lax.axis_index('sp')
    tp = lax.axis_index('tp')
    core = lax.rem(sp, 2)
    xpos = sp // 2
    _, width = xbuf.shape
    n_chunks, quarter, chunk = y_out.shape
    heads = lhs.shape[1] // 128
    parts = [c // 4 for c in chunks]
    core_peer = {'sp': 2 * xpos + (1 - core)}
    x_peer = {'sp': 2 * (1 - xpos) + core}
    far_peer = {'sp': 2 * (1 - xpos) + (1 - core)}
    y_peer = {'tp': 1 - tp}
    mesh_id = pl.DeviceIdType.MESH

    def remote(src, dst, send, recv, peer):
        return pltpu.make_async_remote_copy(src_ref=src, dst_ref=dst, send_sem=send, recv_sem=recv,
                                            device_id=peer, device_id_type=mesh_id)

    def w_load(n):
        return pltpu.make_async_copy(wo_hbm.at[:, pl.ds(n * chunk, chunk)], wo.at[n], w_sem.at[n])

    small = [pltpu.make_async_copy(x_hbm, xbuf, in_sem.at[0]), pltpu.make_async_copy(wpost_hbm, wpost_ref, in_sem.at[1])]
    local = [[pltpu.make_async_copy(source[c][d], pieces[c][d], p_sem.at[c, d]) for d in range(4)] for c in range(len(chunks))]
    for group in local:
        for copy in group:
            copy.start()
    for n in range(n_chunks):
        w_load(n).start()
    for copy in small:
        copy.start()
    barrier = pltpu.get_barrier_semaphore()
    for peer in (core_peer, x_peer, far_peer, y_peer):
        pl.semaphore_signal(barrier, inc=1, device_id=peer, device_id_type=mesh_id)
    pl.semaphore_wait(barrier, 4)

    for copy in local[-1]:
        copy.wait()
    last = [remote(pieces[-1][d], last_in.at[d - 1], o_send.at[d - 1], o_recv.at[d - 1], peer)
            for d, peer in ((2, x_peer), (3, far_peer), (1, core_peer))]
    for copy in last:
        copy.start()

    def combine(blocks, part, row0):
        count = part * heads
        stats = [block[count:count + 2 * heads, :] for block in blocks]
        top = functools.reduce(jnp.maximum, [st[:heads] for st in stats])
        grown = [jnp.exp(st[:heads] - top) for st in stats]
        total = sum(st[heads:] * g for st, g in zip(stats, grown))
        shift = lax.rem(128 - sp * part, 128)
        factors = [pltpu.roll(g / total, shift, 1) for g in grown]
        for b in range(part):
            at = slice(b * heads, (b + 1) * heads)
            osum[at, :] = sum(block[at, :] * f[:, b:b + 1] for block, f in zip(blocks, factors))
        for h in range(heads):
            lhs[row0:row0 + part, h * 128:(h + 1) * 128] = osum[pl.ds(h, part, stride=heads), :].astype(jnp.bfloat16)

    first = sum(parts[:-1])
    row0 = 0
    for c in range(len(chunks) - 1):
        for copy in local[c]:
            copy.wait()
        combine(pieces[c], parts[c], row0)
        row0 += parts[c]

    wide = 3
    first_at, last_at = pl.ds(0, first), pl.ds(first, quarter - first)
    order = [(pl.ds(n, 1), first_at) for n in range(n_chunks)] + [(pl.ds(n, wide), last_at) for n in range(0, n_chunks, wide)]

    def to_y(t):
        ns, r = order[t]
        return remote(y_out.at[ns, r], y_in.at[ns, r], y_send.at[t], y_recv.at[t], y_peer)

    def to_x(t):
        ns, r = order[t]
        return remote(sums.at[sp, ns, r], sums.at[sp, ns, r], g_send.at[t], g_recv.at[t], x_peer)

    def to_core(t):
        ns, r = order[t]
        return remote(sums.at[sp, ns, r], sums.at[sp, ns, r], d_send.at[t], d_recv.at[t], core_peer)

    def relay(t):
        ns, r = order[t]
        other = 2 * (1 - xpos) + core
        return remote(sums.at[other, ns, r], sums.at[other, ns, r], f_send.at[t], f_recv.at[t], core_peer)

    def project(n, r0, count):
        y_out[n, r0:r0 + count, :] = jnp.dot(lhs[r0:r0 + count, :], wo[n], preferred_element_type=jnp.float32)

    for n in range(n_chunks):
        w_load(n).wait()
        project(n, 0, first)
        to_y(n).start()

    for t in range(len(order) + 1):
        if t == 2:
            for copy in last:
                copy.wait()
            combine([pieces[-1][0]] + [last_in.at[d] for d in range(3)], parts[-1], first)
        if 2 <= t < 2 + n_chunks // wide:
            for n in range((t - 2) * wide, (t - 1) * wide):
                project(n, first, quarter - first)
            to_y(n_chunks + t - 2).start()
        if t < len(order):
            ns, r = order[t]
            to_y(t).wait()
            sums[sp, ns, r, :] = y_out[ns, r, :] + y_in[ns, r, :]
            to_x(t).start()
            to_core(t).start()
        if t >= 1:
            to_x(t - 1).wait_recv()
            relay(t - 1).start()
    for copy in small:
        copy.wait()
    for t in range(len(order)):
        to_x(t).wait_send()
        to_core(t).wait()
        relay(t).wait()

    starts = []
    base = 0
    for c, part in zip(chunks, parts):
        starts += [(base, part, k) for k in range(0, part, 16)]
        base += c
    for q in range(4):
        for k, (base, part, off) in enumerate(starts):
            at = slice(k * 16, (k + 1) * 16)
            out_at = slice(base + q * part + off, base + q * part + off + 16)
            square = jnp.zeros((16, chunk), jnp.float32)
            for n in range(n_chunks):
                u = sums[q, n, at, :]
                square = square + u * u
            inv = lax.rsqrt(jnp.sum(square, axis=-1, keepdims=True) * (1.0 / width) + NORM_EPS)
            for n in range(n_chunks):
                col = slice(n * chunk, (n + 1) * chunk)
                y = xbuf[out_at, col].astype(jnp.float32) + sums[q, n, at, :] * inv * (1.0 + wpost_ref[:, col])
                out_ref[out_at, col] = y.astype(jnp.bfloat16)


def merge(chunks, pieces, x_in, w_post, w_o, n_chunks):
    rows, width = x_in.shape
    inner = w_o.shape[0]
    heads = inner // 128
    quarter = rows // 4
    chunk = width // n_chunks
    vmem = pl.BlockSpec(memory_space=pltpu.VMEM)
    hbm = pl.BlockSpec(memory_space=pl.ANY)
    f32 = jnp.float32
    dma = pltpu.SemaphoreType.DMA
    per_piece = dma((n_chunks + 3,))
    flat = [p for piece in pieces for p in piece]
    big = max(chunks) // 4 * heads
    return pl.pallas_call(
        functools.partial(merge_kernel, chunks),
        out_shape=jax.ShapeDtypeStruct(x_in.shape, x_in.dtype),
        in_specs=[pl.BlockSpec(memory_space=pltpu.HBM)] * (len(flat) + 3),
        out_specs=vmem,
        scratch_shapes=[
            pltpu.VMEM((n_chunks, inner, chunk), jnp.bfloat16),
            pltpu.VMEM(x_in.shape, x_in.dtype),
            pltpu.VMEM(w_post.shape, f32),
            pltpu.VMEM((3,) + pieces[-1][0].shape, f32),
            pltpu.VMEM((big, 128), f32),
            pltpu.VMEM((quarter, inner), jnp.bfloat16),
            pltpu.VMEM((n_chunks, quarter, chunk), f32),
            pltpu.VMEM((n_chunks, quarter, chunk), f32),
            pltpu.VMEM((4, n_chunks, quarter, chunk), f32),
            dma((2,)), dma((len(chunks), 4)), dma((n_chunks,)), dma((3,)), dma((3,)),
        ] + [per_piece] * 8 + [pltpu.VMEM((4,) + piece[0].shape, f32) for piece in pieces],
        compiler_params=pltpu.CompilerParams(vmem_limit_bytes=56 * 1024 * 1024, collective_id=0, has_side_effects=True),
        cost_estimate=pl.CostEstimate(flops=2 * quarter * inner * width, bytes_accessed=2 * inner * width, transcendentals=0),
        name='merge',
    )(*flat, x_in, w_post, w_o)


def solution(mesh):
    cache_spec = P('dp', 'sp', 'tp', None)
    sp_size = mesh.shape['sp']

    def local_step(x_in, cur_pos, w_pre, w_q, w_k, w_v, w_o, w_post, k_cache, v_cache):
        row_count, seq_block, kv_local, head_dim = k_cache.shape
        sp_index = lax.axis_index('sp')
        cos_tab, sin_tab = rotary_tables(cur_pos, head_dim)
        q_rot, kn2, vn2 = project(x_in, w_pre.reshape(1, -1), cos_tab, sin_tab, w_q, w_k, w_v)
        base = (sp_index * seq_block).astype(jnp.int32).reshape(1)
        kc = k_cache.reshape(row_count, seq_block * kv_local, head_dim)
        vc = v_cache.reshape(row_count, seq_block * kv_local, head_dim)
        chunks = (row_count // 2, row_count // 4, row_count // 4)
        prev, first_row, pieces = None, 0, []
        for index, n_rows in enumerate(chunks):
            *prev, p0, p1, p2, p3 = attend(cur_pos, base, q_rot, kn2, vn2, kc, vc, prev, first_row, n_rows)
            first_row += n_rows
            if index < len(chunks) - 1:
                moved = []
                for d, p in ((1, p1), (2, p2), (3, p3)):
                    moved.append(lax.ppermute(p, 'sp', [(i, i ^ d) for i in range(sp_size)]))
                p1, p2, p3 = moved
            pieces.append((p0, p1, p2, p3))
        k_out, v_out = prev
        x_out = merge(chunks, pieces, x_in, w_post.reshape(1, -1), w_o, 9)
        return x_out, k_out.reshape(k_cache.shape), v_out.reshape(v_cache.shape)

    return jax.shard_map(local_step, mesh=mesh,
                         in_specs=(P('dp', None), P('dp'), P(None), P(None, 'tp'), P(None, 'tp'), P(None, 'tp'), P('tp', None), P(None), cache_spec, cache_spec),
                         out_specs=(P('dp', None), cache_spec, cache_spec), check_vma=False)
```

```python
import functools

import jax
import jax.numpy as jnp
import numpy as np
from jax import lax
from jax.experimental import pallas as pl
from jax.experimental.pallas import tpu as pltpu
from jax.sharding import PartitionSpec as P


SOFT_CAP = 50.0
ROPE_BASE = 10000.0
NORM_EPS = 1e-6
LOG2E = 1.4426950408889634

ROWS_STEP = 8
SLOTS = 8
AHEAD = 5
LAG_SOFT = 2
LAG_OUT = 4


def rotary_table(length, head_dim):
    half_dim = head_dim // 2
    inv_freq = np.power(np.float32(ROPE_BASE), -2.0 * np.arange(half_dim, dtype=np.float32) / np.float32(2 * half_dim)).astype(np.float32)
    angles = np.arange(length, dtype=np.float32)[:, None] * inv_freq[None, :]
    cos_tab = np.cos(angles.astype(np.float64))
    sin_tab = np.sin(angles.astype(np.float64))
    return np.concatenate([cos_tab, cos_tab, -sin_tab, sin_tab], axis=-1).astype(np.float32)


def project_kernel(pos_ref, x_hbm, wpre_ref, table_ref, wq_hbm, wk_hbm, wv_hbm, q_ref, k_ref, v_ref,
                   x_ref, gain_ref, cos_ref, sin_ref, weight, normed, q_part, k_part, v_part, x_sem, w_sem, send_sem, recv_sem):
    sp = lax.axis_index('sp')
    core = lax.rem(sp, 2)
    peer = {'sp': sp + 1 - 2 * core}
    mesh_id = pl.DeviceIdType.MESH
    rows = x_ref.shape[0]
    block = weight.shape[2]
    per = block // 128
    plan = []
    for w_hbm, part, turn in ((wq_hbm, q_part, True), (wk_hbm, k_part, True), (wv_hbm, v_part, False)):
        mine = w_hbm.shape[1] // 2
        for j in range(mine // block):
            plan.append((w_hbm, part, turn, mine, j, j == mine // block - 1))

    def load(i):
        w_hbm, _, _, mine, j, _ = plan[i]
        col = pl.multiple_of(core * mine + j * block, block)
        return pltpu.make_async_copy(w_hbm.at[:, pl.ds(col, block)], weight.at[i], w_sem.at[i])

    x_loads = [pltpu.make_async_copy(x_hbm.at[pl.ds(k * (rows // 4), rows // 4)], x_ref.at[pl.ds(k * (rows // 4), rows // 4)],
                                     x_sem.at[k]) for k in range(4)]
    for copy in x_loads:
        copy.start()
    for i in range(len(plan)):
        load(i).start()
    barrier = pltpu.get_barrier_semaphore()
    pl.semaphore_signal(barrier, inc=1, device_id=peer, device_id_type=mesh_id)
    pl.semaphore_wait(barrier, 1)

    for j in range(wpre_ref.shape[0]):
        gain_ref[:, j * 128:(j + 1) * 128] = 1.0 + wpre_ref[j:j + 1, :]
    gain = gain_ref[...]

    def look_up(k, carry):
        for r in range(8):
            b = k * 8 + r
            row = table_ref[pl.ds(pos_ref[b], 1), :]
            cos_ref[pl.ds(b, 1), :] = row[:, :128]
            sin_ref[pl.ds(b, 1), :] = row[:, 128:]
        return carry

    lax.fori_loop(0, rows // 8, look_up, 0)

    def norm(k, carry):
        at = pl.ds(pl.multiple_of(k * 16, 16), 16)
        x = x_ref[at, :].astype(jnp.float32)
        inv = lax.rsqrt(jnp.mean(x * x, axis=-1, keepdims=True) + NORM_EPS)
        normed[at, :] = (x * inv * gain).astype(jnp.bfloat16)
        return carry

    for k in range(4):
        x_loads[k].wait()
        lax.fori_loop(k * rows // 64, (k + 1) * rows // 64, norm, 0)

    sends = []
    for i, (_, part, turn, mine, j, done) in enumerate(plan):
        load(i).wait()
        heads = mine // 128
        acc = jnp.dot(normed[...], weight[i], preferred_element_type=jnp.float32)
        for t in range(per):
            value = acc[:, t * 128:(t + 1) * 128]
            if turn:
                value = value * cos_ref[...] + pltpu.roll(value, 64, 1) * sin_ref[...]
            part[core, pl.ds(j * per + t, rows, stride=heads), :] = value
        if done:
            n = len(sends)
            copy = pltpu.make_async_remote_copy(src_ref=part.at[core], dst_ref=part.at[core], send_sem=send_sem.at[n],
                                                recv_sem=recv_sem.at[n], device_id=peer, device_id_type=mesh_id)
            copy.start()
            sends.append(copy)
    for copy in sends:
        copy.wait()

    q_heads = q_part.shape[1] // rows
    kv = k_part.shape[1] // rows

    def pack(k, carry):
        for r in range(8):
            b = k * 8 + r
            at = pl.ds(pl.multiple_of(b * q_heads, q_heads), q_heads)
            q_ref[b] = jnp.concatenate([q_part[0, at, :], q_part[1, at, :]], axis=0).astype(jnp.bfloat16)
        for part, out in ((k_part, k_ref), (v_part, v_ref)):
            group = pl.ds(pl.multiple_of(k * 8 * kv, 8), 8 * kv)
            low, high = part[0, group, :], part[1, group, :]
            for r in range(8):
                both = [low[r * kv:(r + 1) * kv], high[r * kv:(r + 1) * kv]]
                out[k * 8 + r] = jnp.concatenate(both + both, axis=0).astype(jnp.bfloat16)
        return carry

    lax.fori_loop(0, rows // 8, pack, 0)


def project(cur_pos, x_in, w_pre, table, w_q, w_k, w_v):
    rows, width = x_in.shape
    block = 512
    q_cols, kv_cols = w_q.shape[1], w_k.shape[1]
    n_blocks = (q_cols + 2 * kv_cols) // 2 // block
    vmem = pl.BlockSpec(memory_space=pltpu.VMEM)
    hbm = pl.BlockSpec(memory_space=pltpu.HBM)
    f32, bf = jnp.float32, jnp.bfloat16
    dma = pltpu.SemaphoreType.DMA
    return pl.pallas_call(
        project_kernel,
        out_shape=(jax.ShapeDtypeStruct((rows, q_cols // 128, 128), bf),
                   jax.ShapeDtypeStruct((rows, kv_cols // 64, 128), bf),
                   jax.ShapeDtypeStruct((rows, kv_cols // 64, 128), bf)),
        in_specs=[pl.BlockSpec(memory_space=pltpu.SMEM), hbm, vmem, vmem] + [hbm] * 3,
        out_specs=(vmem,) * 3,
        scratch_shapes=[
            pltpu.VMEM((rows, width), bf),
            pltpu.VMEM((1, width), f32),
            pltpu.VMEM((rows, 128), f32),
            pltpu.VMEM((rows, 128), f32),
            pltpu.VMEM((n_blocks, width, block), bf),
            pltpu.VMEM((rows, width), bf),
            pltpu.VMEM((2, rows * q_cols // 256, 128), f32),
            pltpu.VMEM((2, rows * kv_cols // 256, 128), f32),
            pltpu.VMEM((2, rows * kv_cols // 256, 128), f32),
            dma((4,)), dma((n_blocks,)), dma((3,)), dma((3,)),
        ],
        compiler_params=pltpu.CompilerParams(vmem_limit_bytes=62 * 1024 * 1024, collective_id=1, has_side_effects=True),
        cost_estimate=pl.CostEstimate(flops=rows * width * (q_cols + 2 * kv_cols), bytes_accessed=width * (q_cols + 2 * kv_cols), transcendentals=0),
        name='project',
    )(cur_pos, x_in, w_pre, table, w_q, w_k, w_v)


def attend_kernel(n_steps, first_row, kv_heads, seq_block, pos_ref, base_ref, q_hbm, kn_hbm, vn_hbm, k_hbm, v_hbm,
                  *rest):
    (ko_hbm, vo_hbm, o0_hbm, o1_hbm, o2_hbm, o3_hbm, m_ref, l_ref, kbuf, vbuf, qbuf, knbuf, vnbuf, obuf, key_ref, s_ref, p_ref, in_sem, out_sem, o_sem, st_sem) = rest[-21:]
    step_rows = ROWS_STEP
    piece_steps = n_steps // 4
    heads, head_dim = qbuf.shape[2], qbuf.shape[3]
    cols = seq_block * kv_heads
    base = base_ref[0]

    row_id = lax.broadcasted_iota(jnp.int32, (heads, cols), 0)
    col_id = lax.broadcasted_iota(jnp.int32, (heads, cols), 1)
    mine = lax.rem(col_id, kv_heads) == row_id // (heads // kv_heads)
    key_ref[...] = jnp.where(mine, col_id, cols * 4)
    lane_id = lax.broadcasted_iota(jnp.int32, m_ref.shape, 1)
    half_id = lax.broadcasted_iota(jnp.int32, (2 * kv_heads, head_dim), 0) // kv_heads

    def loads(step, slot):
        rows = pl.ds(first_row + step * step_rows, step_rows)
        return (pltpu.make_async_copy(k_hbm.at[rows], kbuf.at[slot], in_sem.at[slot, 0]),
                pltpu.make_async_copy(v_hbm.at[rows], vbuf.at[slot], in_sem.at[slot, 1]),
                pltpu.make_async_copy(q_hbm.at[rows], qbuf.at[slot], in_sem.at[slot, 2]),
                pltpu.make_async_copy(kn_hbm.at[rows], knbuf.at[slot], in_sem.at[slot, 3]),
                pltpu.make_async_copy(vn_hbm.at[rows], vnbuf.at[slot], in_sem.at[slot, 4]))

    def stores(step, slot):
        rows = pl.ds(first_row + step * step_rows, step_rows)
        return (pltpu.make_async_copy(kbuf.at[slot], ko_hbm.at[rows], out_sem.at[slot, 0]),
                pltpu.make_async_copy(vbuf.at[slot], vo_hbm.at[rows], out_sem.at[slot, 1]))

    def o_store(step, slot, d=0):
        at = pl.ds(lax.rem(step, piece_steps) * step_rows * heads, step_rows * heads)
        o_hbm = (o0_hbm, o1_hbm, o2_hbm, o3_hbm)[d]
        return pltpu.make_async_copy(obuf.at[slot], o_hbm.at[at], o_sem.at[slot])

    def o_start(step, slot):
        turn = jnp.bitwise_xor(step // piece_steps, base // seq_block)
        for d in range(4):
            @pl.when(turn == d)
            def _():
                o_store(step, slot, d).start()

    for step in range(min(AHEAD, n_steps)):
        for copy in loads(step, step):
            copy.start()
    m_ref[...] = jnp.zeros_like(m_ref)
    l_ref[...] = jnp.zeros_like(l_ref)
    scale = head_dim ** -0.5 / SOFT_CAP

    def body(step, carry):
        slot = lax.rem(step, SLOTS)
        oslot = lax.rem(step, 2)
        for copy in loads(step, slot):
            copy.wait()

        for r in range(step_rows):
            local = pos_ref[first_row + step * step_rows + r] - base
            inside = (local >= 0) & (local < seq_block)
            at = jnp.clip(local, 0, seq_block - 1)
            pair = pl.ds(pl.multiple_of((at // 2) * (2 * kv_heads), 2 * kv_heads), 2 * kv_heads)
            hit = half_id == jnp.where(inside, lax.rem(at, 2), 2)
            kbuf[slot, r, pair, :] = jnp.where(hit, knbuf[slot, r], kbuf[slot, r, pair, :])
            vbuf[slot, r, pair, :] = jnp.where(hit, vnbuf[slot, r], vbuf[slot, r, pair, :])

        @pl.when(step >= 2)
        def _():
            o_store(step - 2, oslot).wait()

        m_all = m_ref[...]
        l_all = l_ref[...]
        half = cols // 2
        for tick in range(step_rows + LAG_OUT):
            r = tick
            if r < step_rows:
                raw = lax.dot_general(qbuf[slot, r], kbuf[slot, r], (((1,), (1,)), ((), ())),
                                      preferred_element_type=jnp.float32)
                s_ref[r] = raw
            r = tick - LAG_SOFT
            if 0 <= r < step_rows:
                local = pos_ref[first_row + step * step_rows + r] - base
                seen = key_ref[...] < (local + 1) * kv_heads
                soft = jnp.where(seen, jnp.tanh(s_ref[r] * scale), -4.0)
                top = jnp.maximum(jnp.max(soft, axis=-1, keepdims=True), -1.0)
                weight = jnp.exp2((soft - top) * (SOFT_CAP * LOG2E))
                total = jnp.sum(weight, axis=-1, keepdims=True)
                weight = weight.astype(jnp.bfloat16)
                p_ref[r, :heads] = weight[:, :half]
                p_ref[r, heads:] = weight[:, half:]
                here = lane_id == step * step_rows + r
                m_all = jnp.where(here, top * SOFT_CAP, m_all)
                l_all = jnp.where(here, total, l_all)
            r = tick - LAG_OUT
            if 0 <= r < step_rows:
                right = jnp.concatenate([vbuf[slot, r, :half, :], vbuf[slot, r, half:, :]], axis=1)
                both = jnp.dot(p_ref[r], right, preferred_element_type=jnp.float32)
                obuf[oslot, r * heads:(r + 1) * heads, :] = both[:heads, :head_dim] + both[heads:, head_dim:]
        m_ref[...] = m_all
        l_ref[...] = l_all
        o_start(step, oslot)
        for copy in stores(step, slot):
            copy.start()

        @pl.when(step + AHEAD < n_steps)
        def _():
            nxt = step + AHEAD
            nslot = lax.rem(nxt, SLOTS)

            @pl.when(nxt >= SLOTS)
            def _():
                for copy in stores(nxt - SLOTS, nslot):
                    copy.wait()

            for copy in loads(nxt, nslot):
                copy.start()

        return carry

    lax.fori_loop(0, n_steps, body, 0)
    tail = piece_steps * step_rows * heads
    stat_copies = []
    for d, o_hbm in enumerate((o0_hbm, o1_hbm, o2_hbm, o3_hbm)):
        stat_copies.append(pltpu.make_async_copy(m_ref, o_hbm.at[pl.ds(tail, heads)], st_sem.at[d, 0]))
        stat_copies.append(pltpu.make_async_copy(l_ref, o_hbm.at[pl.ds(tail + heads, heads)], st_sem.at[d, 1]))
    for copy in stat_copies:
        copy.start()
    for copy in stat_copies:
        copy.wait()
    for step in range(max(0, n_steps - SLOTS), n_steps):
        for copy in stores(step, step % SLOTS):
            copy.wait()
    for step in range(max(0, n_steps - 2), n_steps):
        o_store(step, step % 2).wait()


def attend(pos, base, q, kn, vn, k_cache, v_cache, prev, first_row, n_rows):
    _, cols, head_dim = k_cache.shape
    heads = q.shape[1]
    kv_heads = kn.shape[1] // 2
    seq_block = cols // kv_heads
    n_steps = n_rows // ROWS_STEP
    hbm = pl.BlockSpec(memory_space=pl.ANY)
    piece = pltpu.HBM((n_rows // 4 * heads + 2 * heads, head_dim), jnp.float32)
    smem = pl.BlockSpec(memory_space=pltpu.SMEM)
    bf = jnp.bfloat16
    aliases = {} if prev is None else {7: 0, 8: 1}
    extra = () if prev is None else tuple(prev)
    return pl.pallas_call(
        functools.partial(attend_kernel, n_steps, first_row, kv_heads, seq_block),
        out_shape=(jax.ShapeDtypeStruct(k_cache.shape, bf), jax.ShapeDtypeStruct(v_cache.shape, bf)) + (piece,) * 4,
        in_specs=[smem, smem, hbm, hbm, hbm, hbm, hbm] + [hbm] * len(extra),
        out_specs=(hbm, hbm) + (pl.BlockSpec(memory_space=pltpu.HBM),) * 4,
        scratch_shapes=[
            pltpu.VMEM((heads, 128), jnp.float32),
            pltpu.VMEM((heads, 128), jnp.float32),
            pltpu.VMEM((SLOTS, ROWS_STEP, cols, head_dim), bf),
            pltpu.VMEM((SLOTS, ROWS_STEP, cols, head_dim), bf),
            pltpu.VMEM((SLOTS, ROWS_STEP, heads, head_dim), bf),
            pltpu.VMEM((SLOTS, ROWS_STEP, 2 * kv_heads, head_dim), bf),
            pltpu.VMEM((SLOTS, ROWS_STEP, 2 * kv_heads, head_dim), bf),
            pltpu.VMEM((2, ROWS_STEP * heads, head_dim), jnp.float32),
            pltpu.VMEM((heads, cols), jnp.int32),
            pltpu.VMEM((ROWS_STEP, heads, cols), jnp.float32),
            pltpu.VMEM((ROWS_STEP, 2 * heads, cols // 2), bf),
            pltpu.SemaphoreType.DMA((SLOTS, 5)),
            pltpu.SemaphoreType.DMA((SLOTS, 2)),
            pltpu.SemaphoreType.DMA((2,)),
            pltpu.SemaphoreType.DMA((4, 2)),
        ],
        input_output_aliases=aliases,
        compiler_params=pltpu.CompilerParams(vmem_limit_bytes=40 * 1024 * 1024),
        cost_estimate=pl.CostEstimate(flops=n_rows * heads * cols * head_dim * 4,
                                      bytes_accessed=n_rows * cols * head_dim * 8, transcendentals=0),
        name='attend',
    )(pos, base, q, kn, vn, k_cache, v_cache, *extra)


def merge_kernel(chunks, *refs):
    n_in = 4 * len(chunks)
    source = [refs[4 * c:4 * c + 4] for c in range(len(chunks))]
    pieces = [[b.at[d] for d in range(4)] for b in refs[-len(chunks):]]
    refs = refs[:-len(chunks)]
    (x_hbm, wpost_hbm, wo_hbm, out_ref, wo, xbuf, wpost_ref, last_in, osum, lhs, y_out, y_in, sums,
     in_sem, p_sem, w_sem, o_send, o_recv, y_send, y_recv, g_send, g_recv, d_send, d_recv, f_send, f_recv) = refs[n_in:]
    sp = lax.axis_index('sp')
    tp = lax.axis_index('tp')
    core = lax.rem(sp, 2)
    xpos = sp // 2
    _, width = xbuf.shape
    n_chunks, quarter, chunk = y_out.shape
    heads = lhs.shape[1] // 128
    parts = [c // 4 for c in chunks]
    core_peer = {'sp': 2 * xpos + (1 - core)}
    x_peer = {'sp': 2 * (1 - xpos) + core}
    far_peer = {'sp': 2 * (1 - xpos) + (1 - core)}
    y_peer = {'tp': 1 - tp}
    mesh_id = pl.DeviceIdType.MESH

    def remote(src, dst, send, recv, peer):
        return pltpu.make_async_remote_copy(src_ref=src, dst_ref=dst, send_sem=send, recv_sem=recv,
                                            device_id=peer, device_id_type=mesh_id)

    def w_load(n):
        return pltpu.make_async_copy(wo_hbm.at[:, pl.ds(n * chunk, chunk)], wo.at[n], w_sem.at[n])

    small = [pltpu.make_async_copy(x_hbm, xbuf, in_sem.at[0]), pltpu.make_async_copy(wpost_hbm, wpost_ref, in_sem.at[1])]
    local = [[pltpu.make_async_copy(source[c][d], pieces[c][d], p_sem.at[c, d]) for d in range(4)] for c in range(len(chunks))]
    for group in local:
        for copy in group:
            copy.start()
    for n in range(n_chunks):
        w_load(n).start()
    for copy in small:
        copy.start()
    barrier = pltpu.get_barrier_semaphore()
    for peer in (core_peer, x_peer, far_peer, y_peer):
        pl.semaphore_signal(barrier, inc=1, device_id=peer, device_id_type=mesh_id)
    pl.semaphore_wait(barrier, 4)

    for copy in local[-1]:
        copy.wait()
    last = [remote(pieces[-1][d], last_in.at[d - 1], o_send.at[d - 1], o_recv.at[d - 1], peer)
            for d, peer in ((2, x_peer), (3, far_peer), (1, core_peer))]
    for copy in last:
        copy.start()

    def combine(blocks, part, row0):
        count = part * heads
        stats = [block[count:count + 2 * heads, :] for block in blocks]
        top = functools.reduce(jnp.maximum, [st[:heads] for st in stats])
        grown = [jnp.exp(st[:heads] - top) for st in stats]
        total = sum(st[heads:] * g for st, g in zip(stats, grown))
        shift = lax.rem(128 - sp * part, 128)
        factors = [pltpu.roll(g / total, shift, 1) for g in grown]
        for b in range(part):
            at = slice(b * heads, (b + 1) * heads)
            osum[at, :] = sum(block[at, :] * f[:, b:b + 1] for block, f in zip(blocks, factors))
        for h in range(heads):
            lhs[row0:row0 + part, h * 128:(h + 1) * 128] = osum[pl.ds(h, part, stride=heads), :].astype(jnp.bfloat16)

    first = sum(parts[:-1])
    row0 = 0
    for c in range(len(chunks) - 1):
        for copy in local[c]:
            copy.wait()
        combine(pieces[c], parts[c], row0)
        row0 += parts[c]

    first_at, last_at = pl.ds(0, first), pl.ds(first, quarter - first)
    split = ((2, 2, 2, 2, 1), (1, 2, 2, 2, 2))
    wide = 3
    orders = []
    for sizes in split:
        begin, order = 0, []
        for size in sizes:
            order.append((begin, size, first_at))
            begin += size
        orders.append(order + [(n, wide, last_at) for n in range(0, n_chunks, wide)])
    n_first = len(split[0])
    n_pieces = len(orders[0])

    def to_y(v, t):
        n, size, r = orders[v][t]
        ns = pl.ds(n, size)
        return remote(y_out.at[ns, r], y_in.at[ns, r], y_send.at[t], y_recv.at[t], y_peer)

    def to_x(v, t):
        n, size, r = orders[v][t]
        ns = pl.ds(n, size)
        return remote(sums.at[sp, ns, r], sums.at[sp, ns, r], g_send.at[t], g_recv.at[t], x_peer)

    def to_core(v, t):
        n, size, r = orders[v][t]
        ns = pl.ds(n, size)
        return remote(sums.at[sp, ns, r], sums.at[sp, ns, r], d_send.at[t], d_recv.at[t], core_peer)

    def relay(v, t):
        n, size, r = orders[v][t]
        ns = pl.ds(n, size)
        other = 2 * (1 - xpos) + core
        return remote(sums.at[other, ns, r], sums.at[other, ns, r], f_send.at[t], f_recv.at[t], core_peer)

    def project_rows(n, r0, count):
        y_out[n, r0:r0 + count, :] = jnp.dot(lhs[r0:r0 + count, :], wo[n], preferred_element_type=jnp.float32)

    for n in range(n_chunks):
        w_load(n).wait()
        project_rows(n, 0, first)
        for v in range(2):
            for t in range(n_first):
                if sum(orders[v][t][:2]) == n + 1:
                    @pl.when(core == v)
                    def _():
                        to_y(v, t).start()

    def step(v, t):
        if t < n_pieces:
            n, size, r = orders[v][t]
            ns = pl.ds(n, size)
            to_y(v, t).wait()
            sums[sp, ns, r, :] = y_out[ns, r, :] + y_in[ns, r, :]
            to_x(v, t).start()
            to_core(v, t).start()
        if t >= 1:
            to_x(v, t - 1).wait_recv()
            relay(v, t - 1).start()

    for t in range(n_pieces + 1):
        if t == 1:
            for copy in last:
                copy.wait()
            combine([pieces[-1][0]] + [last_in.at[d] for d in range(3)], parts[-1], first)
        if 1 <= t < 1 + n_chunks // wide:
            for n in range((t - 1) * wide, t * wide):
                project_rows(n, first, quarter - first)
            to_y(0, n_first + t - 1).start()
        for v in range(2):
            @pl.when(core == v)
            def _():
                step(v, t)
    for copy in small:
        copy.wait()
    for v in range(2):
        @pl.when(core == v)
        def _():
            for t in range(n_pieces):
                to_x(v, t).wait_send()
                to_core(v, t).wait_send()
                relay(v, t).wait_send()
                to_core(1 - v, t).wait_recv()
                relay(1 - v, t).wait_recv()

    starts = []
    base = 0
    for c, part in zip(chunks, parts):
        starts += [(base, part, k) for k in range(0, part, 16)]
        base += c
    for q in range(4):
        for k, (base, part, off) in enumerate(starts):
            at = slice(k * 16, (k + 1) * 16)
            out_at = slice(base + q * part + off, base + q * part + off + 16)
            square = jnp.zeros((16, chunk), jnp.float32)
            for n in range(n_chunks):
                u = sums[q, n, at, :]
                square = square + u * u
            inv = lax.rsqrt(jnp.sum(square, axis=-1, keepdims=True) * (1.0 / width) + NORM_EPS)
            for n in range(n_chunks):
                col = slice(n * chunk, (n + 1) * chunk)
                y = xbuf[out_at, col].astype(jnp.float32) + sums[q, n, at, :] * inv * (1.0 + wpost_ref[:, col])
                out_ref[out_at, col] = y.astype(jnp.bfloat16)


def merge(chunks, pieces, x_in, w_post, w_o, n_chunks):
    rows, width = x_in.shape
    inner = w_o.shape[0]
    heads = inner // 128
    quarter = rows // 4
    chunk = width // n_chunks
    vmem = pl.BlockSpec(memory_space=pltpu.VMEM)
    hbm = pl.BlockSpec(memory_space=pl.ANY)
    f32 = jnp.float32
    dma = pltpu.SemaphoreType.DMA
    per_piece = dma((n_chunks + 3,))
    flat = [p for piece in pieces for p in piece]
    big = max(chunks) // 4 * heads
    return pl.pallas_call(
        functools.partial(merge_kernel, chunks),
        out_shape=jax.ShapeDtypeStruct(x_in.shape, x_in.dtype),
        in_specs=[pl.BlockSpec(memory_space=pltpu.HBM)] * (len(flat) + 3),
        out_specs=vmem,
        scratch_shapes=[
            pltpu.VMEM((n_chunks, inner, chunk), jnp.bfloat16),
            pltpu.VMEM(x_in.shape, x_in.dtype),
            pltpu.VMEM(w_post.shape, f32),
            pltpu.VMEM((3,) + pieces[-1][0].shape, f32),
            pltpu.VMEM((big, 128), f32),
            pltpu.VMEM((quarter, inner), jnp.bfloat16),
            pltpu.VMEM((n_chunks, quarter, chunk), f32),
            pltpu.VMEM((n_chunks, quarter, chunk), f32),
            pltpu.VMEM((4, n_chunks, quarter, chunk), f32),
            dma((2,)), dma((len(chunks), 4)), dma((n_chunks,)), dma((3,)), dma((3,)),
        ] + [per_piece] * 8 + [pltpu.VMEM((4,) + piece[0].shape, f32) for piece in pieces],
        compiler_params=pltpu.CompilerParams(vmem_limit_bytes=56 * 1024 * 1024, collective_id=0, has_side_effects=True),
        cost_estimate=pl.CostEstimate(flops=2 * quarter * inner * width, bytes_accessed=2 * inner * width, transcendentals=0),
        name='merge',
    )(*flat, x_in, w_post, w_o)


def solution(mesh):
    cache_spec = P('dp', 'sp', 'tp', None)
    sp_size = mesh.shape['sp']

    def local_step(x_in, cur_pos, w_pre, w_q, w_k, w_v, w_o, w_post, k_cache, v_cache):
        row_count, seq_block, kv_local, head_dim = k_cache.shape
        sp_index = lax.axis_index('sp')
        table = rotary_table(sp_size * seq_block, head_dim)
        q_rot, kn2, vn2 = project(cur_pos, x_in, w_pre.reshape(-1, 128), table, w_q, w_k, w_v)
        base = (sp_index * seq_block).astype(jnp.int32).reshape(1)
        kc = k_cache.reshape(row_count, seq_block * kv_local, head_dim)
        vc = v_cache.reshape(row_count, seq_block * kv_local, head_dim)
        chunks = (row_count // 2, row_count // 4, row_count // 4)
        prev, first_row, pieces = None, 0, []
        for index, n_rows in enumerate(chunks):
            *prev, p0, p1, p2, p3 = attend(cur_pos, base, q_rot, kn2, vn2, kc, vc, prev, first_row, n_rows)
            first_row += n_rows
            if index < len(chunks) - 1:
                moved = []
                for d, p in ((1, p1), (2, p2), (3, p3)):
                    moved.append(lax.ppermute(p, 'sp', [(i, i ^ d) for i in range(sp_size)]))
                p1, p2, p3 = moved
            pieces.append((p0, p1, p2, p3))
        k_out, v_out = prev
        x_out = merge(chunks, pieces, x_in, w_post.reshape(1, -1), w_o, 9)
        return x_out, k_out.reshape(k_cache.shape), v_out.reshape(v_cache.shape)

    return jax.shard_map(local_step, mesh=mesh,
                         in_specs=(P('dp', None), P('dp'), P(None), P(None, 'tp'), P(None, 'tp'), P(None, 'tp'), P('tp', None), P(None), cache_spec, cache_spec),
                         out_specs=(P('dp', None), cache_spec, cache_spec), check_vma=False)
```

```python
import functools

import jax
import jax.numpy as jnp
import numpy as np
from jax import lax
from jax.experimental import pallas as pl
from jax.experimental.pallas import tpu as pltpu
from jax.sharding import PartitionSpec as P


SOFT_CAP = 50.0
ROPE_BASE = 10000.0
NORM_EPS = 1e-6
LOG2E = 1.4426950408889634

ROWS_STEP = 8
SLOTS = 8
AHEAD = 5
LAG_SOFT = 2
LAG_OUT = 4


def rotary_table(length, head_dim):
    half_dim = head_dim // 2
    inv_freq = np.power(np.float32(ROPE_BASE), -2.0 * np.arange(half_dim, dtype=np.float32) / np.float32(2 * half_dim)).astype(np.float32)
    angles = np.arange(length, dtype=np.float32)[:, None] * inv_freq[None, :]
    cos_tab = np.cos(angles.astype(np.float64))
    sin_tab = np.sin(angles.astype(np.float64))
    return np.concatenate([cos_tab, cos_tab, -sin_tab, sin_tab], axis=-1).astype(np.float32)


def project_kernel(pos_ref, x_hbm, wpre_ref, table_ref, wq_hbm, wk_hbm, wv_hbm, q_ref, k_ref, v_ref,
                   x_ref, gain_ref, cos_ref, sin_ref, weight, normed, q_part, k_part, v_part, x_sem, w_sem, send_sem, recv_sem,
                   out_sem):
    sp = lax.axis_index('sp')
    core = lax.rem(sp, 2)
    peer = {'sp': sp + 1 - 2 * core}
    mesh_id = pl.DeviceIdType.MESH
    rows = x_ref.shape[0]
    block = weight.shape[2]
    per = block // 128
    plan = []
    for w_hbm, part, turn in ((wq_hbm, q_part, True), (wk_hbm, k_part, True), (wv_hbm, v_part, False)):
        mine = w_hbm.shape[1] // 2
        for j in range(mine // block):
            plan.append((w_hbm, part, turn, mine, j, j == mine // block - 1))

    def load(i):
        w_hbm, _, _, mine, j, _ = plan[i]
        col = pl.multiple_of(core * mine + j * block, block)
        return pltpu.make_async_copy(w_hbm.at[:, pl.ds(col, block)], weight.at[i], w_sem.at[i])

    x_loads = [pltpu.make_async_copy(x_hbm.at[pl.ds(k * (rows // 4), rows // 4)], x_ref.at[pl.ds(k * (rows // 4), rows // 4)],
                                     x_sem.at[k]) for k in range(4)]
    for copy in x_loads:
        copy.start()
    for i in range(len(plan)):
        load(i).start()
    barrier = pltpu.get_barrier_semaphore()
    pl.semaphore_signal(barrier, inc=1, device_id=peer, device_id_type=mesh_id)
    pl.semaphore_wait(barrier, 1)

    for j in range(wpre_ref.shape[0]):
        gain_ref[:, j * 128:(j + 1) * 128] = 1.0 + wpre_ref[j:j + 1, :]
    gain = gain_ref[...]

    def look_up(k, carry):
        for r in range(8):
            b = k * 8 + r
            row = table_ref[pl.ds(pos_ref[b], 1), :]
            cos_ref[pl.ds(b, 1), :] = row[:, :128]
            sin_ref[pl.ds(b, 1), :] = row[:, 128:]
        return carry

    lax.fori_loop(0, rows // 8, look_up, 0)

    def norm(k, carry):
        at = pl.ds(pl.multiple_of(k * 16, 16), 16)
        x = x_ref[at, :].astype(jnp.float32)
        inv = lax.rsqrt(jnp.mean(x * x, axis=-1, keepdims=True) + NORM_EPS)
        normed[at, :] = (x * inv * gain).astype(jnp.bfloat16)
        return carry

    for k in range(4):
        x_loads[k].wait()
        lax.fori_loop(k * rows // 64, (k + 1) * rows // 64, norm, 0)

    outs = ((q_part, q_ref), (k_part, k_ref), (v_part, v_ref))
    sends, writes = [], []
    for i, (_, part, turn, mine, j, done) in enumerate(plan):
        load(i).wait()
        heads = mine // 128
        acc = jnp.dot(normed[...], weight[i], preferred_element_type=jnp.float32)
        for t in range(per):
            value = acc[:, t * 128:(t + 1) * 128]
            if turn:
                value = value * cos_ref[...] + pltpu.roll(value, 64, 1) * sin_ref[...]
            part[core, pl.ds(j * per + t, rows, stride=heads), :] = value
        if done:
            n = len(sends)
            copy = pltpu.make_async_remote_copy(src_ref=part.at[core], dst_ref=part.at[core], send_sem=send_sem.at[n],
                                                recv_sem=recv_sem.at[n], device_id=peer, device_id_type=mesh_id)
            copy.start()
            sends.append(copy)
            out = pltpu.make_async_copy(part.at[core], outs[n][1].at[core], out_sem.at[0, n])
            out.start()
            writes.append(out)
    for n, copy in enumerate(sends):
        copy.wait_recv()
        out = pltpu.make_async_copy(outs[n][0].at[1 - core], outs[n][1].at[1 - core], out_sem.at[1, n])
        out.start()
        writes.append(out)
    for copy in sends:
        copy.wait_send()
    for copy in writes:
        copy.wait()


def project(cur_pos, x_in, w_pre, table, w_q, w_k, w_v):
    rows, width = x_in.shape
    block = 512
    q_cols, kv_cols = w_q.shape[1], w_k.shape[1]
    n_blocks = (q_cols + 2 * kv_cols) // 2 // block
    vmem = pl.BlockSpec(memory_space=pltpu.VMEM)
    hbm = pl.BlockSpec(memory_space=pltpu.HBM)
    f32, bf = jnp.float32, jnp.bfloat16
    dma = pltpu.SemaphoreType.DMA
    return pl.pallas_call(
        project_kernel,
        out_shape=(pltpu.HBM((2, rows * q_cols // 256, 128), f32), pltpu.HBM((2, rows * kv_cols // 256, 128), f32),
                   pltpu.HBM((2, rows * kv_cols // 256, 128), f32)),
        in_specs=[pl.BlockSpec(memory_space=pltpu.SMEM), hbm, vmem, vmem] + [hbm] * 3,
        out_specs=(hbm,) * 3,
        scratch_shapes=[
            pltpu.VMEM((rows, width), bf),
            pltpu.VMEM((1, width), f32),
            pltpu.VMEM((rows, 128), f32),
            pltpu.VMEM((rows, 128), f32),
            pltpu.VMEM((n_blocks, width, block), bf),
            pltpu.VMEM((rows, width), bf),
            pltpu.VMEM((2, rows * q_cols // 256, 128), f32),
            pltpu.VMEM((2, rows * kv_cols // 256, 128), f32),
            pltpu.VMEM((2, rows * kv_cols // 256, 128), f32),
            dma((4,)), dma((n_blocks,)), dma((3,)), dma((3,)), dma((2, 3)),
        ],
        compiler_params=pltpu.CompilerParams(vmem_limit_bytes=62 * 1024 * 1024, collective_id=1, has_side_effects=True),
        cost_estimate=pl.CostEstimate(flops=rows * width * (q_cols + 2 * kv_cols), bytes_accessed=width * (q_cols + 2 * kv_cols), transcendentals=0),
        name='project',
    )(cur_pos, x_in, w_pre, table, w_q, w_k, w_v)


def attend_kernel(n_steps, first_row, kv_heads, seq_block, pos_ref, base_ref, q_hbm, kn_hbm, vn_hbm, k_hbm, v_hbm,
                  *rest):
    (ko_hbm, vo_hbm, o0_hbm, o1_hbm, o2_hbm, o3_hbm, m_ref, l_ref, kbuf, vbuf, qbuf, knbuf, vnbuf, obuf, key_ref, s_ref, p_ref, in_sem, out_sem, o_sem, st_sem) = rest[-21:]
    step_rows = ROWS_STEP
    piece_steps = n_steps // 4
    heads, head_dim = m_ref.shape
    q_half, kv_half = heads // 2, kv_heads // 2
    cols = seq_block * kv_heads
    base = base_ref[0]

    row_id = lax.broadcasted_iota(jnp.int32, (heads, cols), 0)
    col_id = lax.broadcasted_iota(jnp.int32, (heads, cols), 1)
    mine = lax.rem(col_id, kv_heads) == row_id // (heads // kv_heads)
    key_ref[...] = jnp.where(mine, col_id, cols * 4)
    lane_id = lax.broadcasted_iota(jnp.int32, m_ref.shape, 1)
    half_id = lax.broadcasted_iota(jnp.int32, (2 * kv_heads, head_dim), 0) // kv_heads

    def heads_of(step, count):
        return pl.ds((first_row + step * step_rows) * count, step_rows * count)

    def both_halves(ref, slot, r, count):
        at = slice(r * count, (r + 1) * count)
        return [ref[slot, 0, at, :], ref[slot, 1, at, :]]

    def loads(step, slot):
        rows = pl.ds(first_row + step * step_rows, step_rows)
        return (pltpu.make_async_copy(k_hbm.at[rows], kbuf.at[slot], in_sem.at[slot, 0]),
                pltpu.make_async_copy(v_hbm.at[rows], vbuf.at[slot], in_sem.at[slot, 1]),
                pltpu.make_async_copy(q_hbm.at[:, heads_of(step, q_half)], qbuf.at[slot], in_sem.at[slot, 2]),
                pltpu.make_async_copy(kn_hbm.at[:, heads_of(step, kv_half)], knbuf.at[slot], in_sem.at[slot, 3]),
                pltpu.make_async_copy(vn_hbm.at[:, heads_of(step, kv_half)], vnbuf.at[slot], in_sem.at[slot, 4]))

    def stores(step, slot):
        rows = pl.ds(first_row + step * step_rows, step_rows)
        return (pltpu.make_async_copy(kbuf.at[slot], ko_hbm.at[rows], out_sem.at[slot, 0]),
                pltpu.make_async_copy(vbuf.at[slot], vo_hbm.at[rows], out_sem.at[slot, 1]))

    def o_store(step, slot, d=0):
        at = pl.ds(lax.rem(step, piece_steps) * step_rows * heads, step_rows * heads)
        o_hbm = (o0_hbm, o1_hbm, o2_hbm, o3_hbm)[d]
        return pltpu.make_async_copy(obuf.at[slot], o_hbm.at[at], o_sem.at[slot])

    def o_start(step, slot):
        turn = jnp.bitwise_xor(step // piece_steps, base // seq_block)
        for d in range(4):
            @pl.when(turn == d)
            def _():
                o_store(step, slot, d).start()

    for step in range(min(AHEAD, n_steps)):
        for copy in loads(step, step):
            copy.start()
    m_ref[...] = jnp.zeros_like(m_ref)
    l_ref[...] = jnp.zeros_like(l_ref)
    scale = head_dim ** -0.5 / SOFT_CAP

    def body(step, carry):
        slot = lax.rem(step, SLOTS)
        oslot = lax.rem(step, 2)
        for copy in loads(step, slot):
            copy.wait()

        for r in range(step_rows):
            local = pos_ref[first_row + step * step_rows + r] - base
            inside = (local >= 0) & (local < seq_block)
            at = jnp.clip(local, 0, seq_block - 1)
            pair = pl.ds(pl.multiple_of((at // 2) * (2 * kv_heads), 2 * kv_heads), 2 * kv_heads)
            hit = half_id == jnp.where(inside, lax.rem(at, 2), 2)
            k_row = jnp.concatenate(both_halves(knbuf, slot, r, kv_half) * 2, axis=0).astype(jnp.bfloat16)
            v_row = jnp.concatenate(both_halves(vnbuf, slot, r, kv_half) * 2, axis=0).astype(jnp.bfloat16)
            kbuf[slot, r, pair, :] = jnp.where(hit, k_row, kbuf[slot, r, pair, :])
            vbuf[slot, r, pair, :] = jnp.where(hit, v_row, vbuf[slot, r, pair, :])

        @pl.when(step >= 2)
        def _():
            o_store(step - 2, oslot).wait()

        m_all = m_ref[...]
        l_all = l_ref[...]
        half = cols // 2
        for tick in range(step_rows + LAG_OUT):
            r = tick
            if r < step_rows:
                q_row = jnp.concatenate(both_halves(qbuf, slot, r, q_half), axis=0).astype(jnp.bfloat16)
                raw = lax.dot_general(q_row, kbuf[slot, r], (((1,), (1,)), ((), ())),
                                      preferred_element_type=jnp.float32)
                s_ref[r] = raw
            r = tick - LAG_SOFT
            if 0 <= r < step_rows:
                local = pos_ref[first_row + step * step_rows + r] - base
                seen = key_ref[...] < (local + 1) * kv_heads
                soft = jnp.where(seen, jnp.tanh(s_ref[r] * scale), -4.0)
                top = jnp.maximum(jnp.max(soft, axis=-1, keepdims=True), -1.0)
                weight = jnp.exp2((soft - top) * (SOFT_CAP * LOG2E))
                total = jnp.sum(weight, axis=-1, keepdims=True)
                weight = weight.astype(jnp.bfloat16)
                p_ref[r, :heads] = weight[:, :half]
                p_ref[r, heads:] = weight[:, half:]
                here = lane_id == step * step_rows + r
                m_all = jnp.where(here, top * SOFT_CAP, m_all)
                l_all = jnp.where(here, total, l_all)
            r = tick - LAG_OUT
            if 0 <= r < step_rows:
                right = jnp.concatenate([vbuf[slot, r, :half, :], vbuf[slot, r, half:, :]], axis=1)
                both = jnp.dot(p_ref[r], right, preferred_element_type=jnp.float32)
                obuf[oslot, r * heads:(r + 1) * heads, :] = both[:heads, :head_dim] + both[heads:, head_dim:]
        m_ref[...] = m_all
        l_ref[...] = l_all
        o_start(step, oslot)
        for copy in stores(step, slot):
            copy.start()

        @pl.when(step + AHEAD < n_steps)
        def _():
            nxt = step + AHEAD
            nslot = lax.rem(nxt, SLOTS)

            @pl.when(nxt >= SLOTS)
            def _():
                for copy in stores(nxt - SLOTS, nslot):
                    copy.wait()

            for copy in loads(nxt, nslot):
                copy.start()

        return carry

    lax.fori_loop(0, n_steps, body, 0)
    tail = piece_steps * step_rows * heads
    stat_copies = []
    for d, o_hbm in enumerate((o0_hbm, o1_hbm, o2_hbm, o3_hbm)):
        stat_copies.append(pltpu.make_async_copy(m_ref, o_hbm.at[pl.ds(tail, heads)], st_sem.at[d, 0]))
        stat_copies.append(pltpu.make_async_copy(l_ref, o_hbm.at[pl.ds(tail + heads, heads)], st_sem.at[d, 1]))
    for copy in stat_copies:
        copy.start()
    for copy in stat_copies:
        copy.wait()
    for step in range(max(0, n_steps - SLOTS), n_steps):
        for copy in stores(step, step % SLOTS):
            copy.wait()
    for step in range(max(0, n_steps - 2), n_steps):
        o_store(step, step % 2).wait()


def attend(pos, base, q, kn, vn, k_cache, v_cache, prev, first_row, n_rows):
    rows, cols, head_dim = k_cache.shape
    heads = 2 * q.shape[1] // rows
    kv_heads = 2 * kn.shape[1] // rows
    seq_block = cols // kv_heads
    n_steps = n_rows // ROWS_STEP
    hbm = pl.BlockSpec(memory_space=pl.ANY)
    piece = pltpu.HBM((n_rows // 4 * heads + 2 * heads, head_dim), jnp.float32)
    smem = pl.BlockSpec(memory_space=pltpu.SMEM)
    bf = jnp.bfloat16
    aliases = {} if prev is None else {7: 0, 8: 1}
    extra = () if prev is None else tuple(prev)
    return pl.pallas_call(
        functools.partial(attend_kernel, n_steps, first_row, kv_heads, seq_block),
        out_shape=(jax.ShapeDtypeStruct(k_cache.shape, bf), jax.ShapeDtypeStruct(v_cache.shape, bf)) + (piece,) * 4,
        in_specs=[smem, smem, hbm, hbm, hbm, hbm, hbm] + [hbm] * len(extra),
        out_specs=(hbm, hbm) + (pl.BlockSpec(memory_space=pltpu.HBM),) * 4,
        scratch_shapes=[
            pltpu.VMEM((heads, 128), jnp.float32),
            pltpu.VMEM((heads, 128), jnp.float32),
            pltpu.VMEM((SLOTS, ROWS_STEP, cols, head_dim), bf),
            pltpu.VMEM((SLOTS, ROWS_STEP, cols, head_dim), bf),
            pltpu.VMEM((SLOTS, 2, ROWS_STEP * heads // 2, head_dim), jnp.float32),
            pltpu.VMEM((SLOTS, 2, ROWS_STEP * kv_heads // 2, head_dim), jnp.float32),
            pltpu.VMEM((SLOTS, 2, ROWS_STEP * kv_heads // 2, head_dim), jnp.float32),
            pltpu.VMEM((2, ROWS_STEP * heads, head_dim), jnp.float32),
            pltpu.VMEM((heads, cols), jnp.int32),
            pltpu.VMEM((ROWS_STEP, heads, cols), jnp.float32),
            pltpu.VMEM((ROWS_STEP, 2 * heads, cols // 2), bf),
            pltpu.SemaphoreType.DMA((SLOTS, 5)),
            pltpu.SemaphoreType.DMA((SLOTS, 2)),
            pltpu.SemaphoreType.DMA((2,)),
            pltpu.SemaphoreType.DMA((4, 2)),
        ],
        input_output_aliases=aliases,
        compiler_params=pltpu.CompilerParams(vmem_limit_bytes=62 * 1024 * 1024),
        cost_estimate=pl.CostEstimate(flops=n_rows * heads * cols * head_dim * 4,
                                      bytes_accessed=n_rows * cols * head_dim * 8, transcendentals=0),
        name='attend',
    )(pos, base, q, kn, vn, k_cache, v_cache, *extra)


def merge_kernel(chunks, *refs):
    n_in = 4 * len(chunks)
    source = [refs[4 * c:4 * c + 4] for c in range(len(chunks))]
    pieces = [[b.at[d] for d in range(4)] for b in refs[-len(chunks):]]
    refs = refs[:-len(chunks)]
    (x_hbm, wpost_hbm, wo_hbm, out_ref, wo, xbuf, wpost_ref, last_in, osum, lhs, y_out, y_in, sums,
     in_sem, p_sem, w_sem, o_send, o_recv, y_send, y_recv, g_send, g_recv, d_send, d_recv, f_send, f_recv) = refs[n_in:]
    sp = lax.axis_index('sp')
    tp = lax.axis_index('tp')
    core = lax.rem(sp, 2)
    xpos = sp // 2
    _, width = xbuf.shape
    n_chunks, quarter, chunk = y_out.shape
    heads = lhs.shape[1] // 128
    parts = [c // 4 for c in chunks]
    core_peer = {'sp': 2 * xpos + (1 - core)}
    x_peer = {'sp': 2 * (1 - xpos) + core}
    far_peer = {'sp': 2 * (1 - xpos) + (1 - core)}
    y_peer = {'tp': 1 - tp}
    mesh_id = pl.DeviceIdType.MESH

    def remote(src, dst, send, recv, peer):
        return pltpu.make_async_remote_copy(src_ref=src, dst_ref=dst, send_sem=send, recv_sem=recv,
                                            device_id=peer, device_id_type=mesh_id)

    def w_load(n):
        return pltpu.make_async_copy(wo_hbm.at[:, pl.ds(n * chunk, chunk)], wo.at[n], w_sem.at[n])

    small = [pltpu.make_async_copy(x_hbm, xbuf, in_sem.at[0]), pltpu.make_async_copy(wpost_hbm, wpost_ref, in_sem.at[1])]
    local = [[pltpu.make_async_copy(source[c][d], pieces[c][d], p_sem.at[c, d]) for d in range(4)] for c in range(len(chunks))]
    for group in local:
        for copy in group:
            copy.start()
    for n in range(n_chunks):
        w_load(n).start()
    for copy in small:
        copy.start()
    barrier = pltpu.get_barrier_semaphore()
    for peer in (core_peer, x_peer, far_peer, y_peer):
        pl.semaphore_signal(barrier, inc=1, device_id=peer, device_id_type=mesh_id)
    pl.semaphore_wait(barrier, 4)

    for copy in local[-1]:
        copy.wait()
    last = [remote(pieces[-1][d], last_in.at[d - 1], o_send.at[d - 1], o_recv.at[d - 1], peer)
            for d, peer in ((2, x_peer), (3, far_peer), (1, core_peer))]
    for copy in last:
        copy.start()

    def combine(blocks, part, row0):
        count = part * heads
        stats = [block[count:count + 2 * heads, :] for block in blocks]
        top = functools.reduce(jnp.maximum, [st[:heads] for st in stats])
        grown = [jnp.exp(st[:heads] - top) for st in stats]
        total = sum(st[heads:] * g for st, g in zip(stats, grown))
        shift = lax.rem(128 - sp * part, 128)
        factors = [pltpu.roll(g / total, shift, 1) for g in grown]
        for b in range(part):
            at = slice(b * heads, (b + 1) * heads)
            osum[at, :] = sum(block[at, :] * f[:, b:b + 1] for block, f in zip(blocks, factors))
        for h in range(heads):
            lhs[row0:row0 + part, h * 128:(h + 1) * 128] = osum[pl.ds(h, part, stride=heads), :].astype(jnp.bfloat16)

    first = sum(parts[:-1])
    row0 = 0
    for c in range(len(chunks) - 1):
        for copy in local[c]:
            copy.wait()
        combine(pieces[c], parts[c], row0)
        row0 += parts[c]

    first_at, last_at = pl.ds(0, first), pl.ds(first, quarter - first)
    split = ((2, 2, 2, 2, 1), (1, 2, 2, 2, 2))
    wide = 3
    orders = []
    for sizes in split:
        begin, order = 0, []
        for size in sizes:
            order.append((begin, size, first_at))
            begin += size
        orders.append(order + [(n, wide, last_at) for n in range(0, n_chunks, wide)])
    n_pieces = len(orders[0])

    def to_y(v, t):
        n, size, r = orders[v][t]
        ns = pl.ds(n, size)
        return remote(y_out.at[ns, r], y_in.at[ns, r], y_send.at[t], y_recv.at[t], y_peer)

    def to_x(v, t):
        n, size, r = orders[v][t]
        ns = pl.ds(n, size)
        return remote(sums.at[sp, ns, r], sums.at[sp, ns, r], g_send.at[t], g_recv.at[t], x_peer)

    def to_core(v, t):
        n, size, r = orders[v][t]
        ns = pl.ds(n, size)
        return remote(sums.at[sp, ns, r], sums.at[sp, ns, r], d_send.at[t], d_recv.at[t], core_peer)

    def relay(v, t):
        n, size, r = orders[v][t]
        ns = pl.ds(n, size)
        other = 2 * (1 - xpos) + core
        return remote(sums.at[other, ns, r], sums.at[other, ns, r], f_send.at[t], f_recv.at[t], core_peer)

    def project_rows(n, r0, count):
        y_out[n, r0:r0 + count, :] = jnp.dot(lhs[r0:r0 + count, :], wo[n], preferred_element_type=jnp.float32)

    for n in range(n_chunks):
        w_load(n).wait()
        project_rows(n, 0, first)
        for v in range(2):
            for t in range(2):
                if sum(orders[v][t][:2]) == n + 1:
                    @pl.when(core == v)
                    def _():
                        to_y(v, t).start()

    def step(v, t):
        if t < n_pieces:
            n, size, r = orders[v][t]
            ns = pl.ds(n, size)
            to_y(v, t).wait()
            if t + 2 < n_pieces:
                to_y(v, t + 2).start()
            sums[sp, ns, r, :] = y_out[ns, r, :] + y_in[ns, r, :]
            to_x(v, t).start()
            to_core(v, t).start()
        if t >= 1:
            to_x(v, t - 1).wait_recv()
            relay(v, t - 1).start()

    for t in range(n_pieces + 1):
        if t == 1:
            for copy in last:
                copy.wait()
            combine([pieces[-1][0]] + [last_in.at[d] for d in range(3)], parts[-1], first)
        if 1 <= t < 1 + n_chunks // wide:
            for n in range((t - 1) * wide, t * wide):
                project_rows(n, first, quarter - first)
        for v in range(2):
            @pl.when(core == v)
            def _():
                step(v, t)
    for copy in small:
        copy.wait()
    for v in range(2):
        @pl.when(core == v)
        def _():
            for t in range(n_pieces):
                to_x(v, t).wait_send()
                to_core(v, t).wait_send()
                relay(v, t).wait_send()
                to_core(1 - v, t).wait_recv()
                relay(1 - v, t).wait_recv()

    starts = []
    base = 0
    for c, part in zip(chunks, parts):
        starts += [(base, part, k) for k in range(0, part, 16)]
        base += c
    for q in range(4):
        for k, (base, part, off) in enumerate(starts):
            at = slice(k * 16, (k + 1) * 16)
            out_at = slice(base + q * part + off, base + q * part + off + 16)
            square = jnp.zeros((16, chunk), jnp.float32)
            for n in range(n_chunks):
                u = sums[q, n, at, :]
                square = square + u * u
            inv = lax.rsqrt(jnp.sum(square, axis=-1, keepdims=True) * (1.0 / width) + NORM_EPS)
            for n in range(n_chunks):
                col = slice(n * chunk, (n + 1) * chunk)
                y = xbuf[out_at, col].astype(jnp.float32) + sums[q, n, at, :] * inv * (1.0 + wpost_ref[:, col])
                out_ref[out_at, col] = y.astype(jnp.bfloat16)


def merge(chunks, pieces, x_in, w_post, w_o, n_chunks):
    rows, width = x_in.shape
    inner = w_o.shape[0]
    heads = inner // 128
    quarter = rows // 4
    chunk = width // n_chunks
    vmem = pl.BlockSpec(memory_space=pltpu.VMEM)
    hbm = pl.BlockSpec(memory_space=pl.ANY)
    f32 = jnp.float32
    dma = pltpu.SemaphoreType.DMA
    per_piece = dma((n_chunks + 3,))
    flat = [p for piece in pieces for p in piece]
    big = max(chunks) // 4 * heads
    return pl.pallas_call(
        functools.partial(merge_kernel, chunks),
        out_shape=jax.ShapeDtypeStruct(x_in.shape, x_in.dtype),
        in_specs=[pl.BlockSpec(memory_space=pltpu.HBM)] * (len(flat) + 3),
        out_specs=vmem,
        scratch_shapes=[
            pltpu.VMEM((n_chunks, inner, chunk), jnp.bfloat16),
            pltpu.VMEM(x_in.shape, x_in.dtype),
            pltpu.VMEM(w_post.shape, f32),
            pltpu.VMEM((3,) + pieces[-1][0].shape, f32),
            pltpu.VMEM((big, 128), f32),
            pltpu.VMEM((quarter, inner), jnp.bfloat16),
            pltpu.VMEM((n_chunks, quarter, chunk), f32),
            pltpu.VMEM((n_chunks, quarter, chunk), f32),
            pltpu.VMEM((4, n_chunks, quarter, chunk), f32),
            dma((2,)), dma((len(chunks), 4)), dma((n_chunks,)), dma((3,)), dma((3,)),
        ] + [per_piece] * 8 + [pltpu.VMEM((4,) + piece[0].shape, f32) for piece in pieces],
        compiler_params=pltpu.CompilerParams(vmem_limit_bytes=56 * 1024 * 1024, collective_id=0, has_side_effects=True),
        cost_estimate=pl.CostEstimate(flops=2 * quarter * inner * width, bytes_accessed=2 * inner * width, transcendentals=0),
        name='merge',
    )(*flat, x_in, w_post, pltpu.with_memory_space_constraint(w_o, pltpu.HBM))


def solution(mesh):
    cache_spec = P('dp', 'sp', 'tp', None)
    sp_size = mesh.shape['sp']

    def local_step(x_in, cur_pos, w_pre, w_q, w_k, w_v, w_o, w_post, k_cache, v_cache):
        row_count, seq_block, kv_local, head_dim = k_cache.shape
        sp_index = lax.axis_index('sp')
        table = rotary_table(sp_size * seq_block, head_dim)
        q_rot, kn2, vn2 = project(cur_pos, x_in, w_pre.reshape(-1, 128), table, w_q, w_k, w_v)
        base = (sp_index * seq_block).astype(jnp.int32).reshape(1)
        kc = k_cache.reshape(row_count, seq_block * kv_local, head_dim)
        vc = v_cache.reshape(row_count, seq_block * kv_local, head_dim)
        chunks = (row_count // 2, row_count // 4, row_count // 4)
        prev, first_row, pieces = None, 0, []
        for index, n_rows in enumerate(chunks):
            *prev, p0, p1, p2, p3 = attend(cur_pos, base, q_rot, kn2, vn2, kc, vc, prev, first_row, n_rows)
            first_row += n_rows
            if index < len(chunks) - 1:
                moved = []
                for d, p in ((1, p1), (2, p2), (3, p3)):
                    moved.append(lax.ppermute(p, 'sp', [(i, i ^ d) for i in range(sp_size)]))
                p1, p2, p3 = moved
            pieces.append((p0, p1, p2, p3))
        k_out, v_out = prev
        x_out = merge(chunks, pieces, x_in, w_post.reshape(1, -1), w_o, 9)
        return x_out, k_out.reshape(k_cache.shape), v_out.reshape(v_cache.shape)

    return jax.shard_map(local_step, mesh=mesh,
                         in_specs=(P('dp', None), P('dp'), P(None), P(None, 'tp'), P(None, 'tp'), P(None, 'tp'), P('tp', None), P(None), cache_spec, cache_spec),
                         out_specs=(P('dp', None), cache_spec, cache_spec), check_vma=False)
```

```python
import functools

import jax
import jax.numpy as jnp
import numpy as np
from jax import lax
from jax.experimental import pallas as pl
from jax.experimental.pallas import tpu as pltpu
from jax.sharding import PartitionSpec as P


SOFT_CAP = 50.0
ROPE_BASE = 10000.0
NORM_EPS = 1e-6
LOG2E = 1.4426950408889634

ROWS_STEP = 8
SLOTS = 12
AHEAD = 6
START = 2
LAG_SOFT = 2
LAG_OUT = 4


def rotary_table(length, head_dim):
    half_dim = head_dim // 2
    inv_freq = np.power(np.float32(ROPE_BASE), -2.0 * np.arange(half_dim, dtype=np.float32) / np.float32(2 * half_dim)).astype(np.float32)
    angles = np.arange(length, dtype=np.float32)[:, None] * inv_freq[None, :]
    cos_tab = np.cos(angles.astype(np.float64))
    sin_tab = np.sin(angles.astype(np.float64))
    return np.concatenate([cos_tab, cos_tab, -sin_tab, sin_tab], axis=-1).astype(np.float32)


def project_kernel(pos_ref, x_hbm, wpre_ref, table_ref, wq_hbm, wk_hbm, wv_hbm, q_ref, k_ref, v_ref,
                   x_ref, gain_ref, cos_ref, sin_ref, weight, normed, q_part, k_part, v_part, x_sem, w_sem, send_sem, recv_sem,
                   out_sem):
    sp = lax.axis_index('sp')
    core = lax.rem(sp, 2)
    peer = {'sp': sp + 1 - 2 * core}
    mesh_id = pl.DeviceIdType.MESH
    rows = x_ref.shape[0]
    block = weight.shape[2]
    per = block // 128
    plan = []
    for w_hbm, part, turn in ((wq_hbm, q_part, True), (wk_hbm, k_part, True), (wv_hbm, v_part, False)):
        mine = w_hbm.shape[1] // 2
        for j in range(mine // block):
            plan.append((w_hbm, part, turn, mine, j, j == mine // block - 1))

    def load(i):
        w_hbm, _, _, mine, j, _ = plan[i]
        col = pl.multiple_of(core * mine + j * block, block)
        return pltpu.make_async_copy(w_hbm.at[:, pl.ds(col, block)], weight.at[i], w_sem.at[i])

    x_loads = [pltpu.make_async_copy(x_hbm.at[pl.ds(k * (rows // 4), rows // 4)], x_ref.at[pl.ds(k * (rows // 4), rows // 4)],
                                     x_sem.at[k]) for k in range(4)]
    for copy in x_loads:
        copy.start()
    load(0).start()
    barrier = pltpu.get_barrier_semaphore()
    pl.semaphore_signal(barrier, inc=1, device_id=peer, device_id_type=mesh_id)
    pl.semaphore_wait(barrier, 1)

    for j in range(wpre_ref.shape[0]):
        gain_ref[:, j * 128:(j + 1) * 128] = 1.0 + wpre_ref[j:j + 1, :]
    gain = gain_ref[...]

    def look_up(k, carry):
        for r in range(8):
            b = k * 8 + r
            row = table_ref[pl.ds(pos_ref[b], 1), :]
            cos_ref[pl.ds(b, 1), :] = row[:, :128]
            sin_ref[pl.ds(b, 1), :] = row[:, 128:]
        return carry

    lax.fori_loop(0, rows // 8, look_up, 0)

    def norm(k, carry):
        at = pl.ds(pl.multiple_of(k * 16, 16), 16)
        x = x_ref[at, :].astype(jnp.float32)
        inv = lax.rsqrt(jnp.mean(x * x, axis=-1, keepdims=True) + NORM_EPS)
        normed[at, :] = (x * inv * gain).astype(jnp.bfloat16)
        return carry

    for k in range(4):
        x_loads[k].wait()
        if k == 1:
            load(1).start()
        lax.fori_loop(k * rows // 64, (k + 1) * rows // 64, norm, 0)

    outs = ((q_part, q_ref), (k_part, k_ref), (v_part, v_ref))
    sends, writes = [], []
    for i, (_, part, turn, mine, j, done) in enumerate(plan):
        load(i).wait()
        if i + 2 < len(plan):
            load(i + 2).start()
        heads = mine // 128
        acc = jnp.dot(normed[...], weight[i], preferred_element_type=jnp.float32)
        for t in range(per):
            value = acc[:, t * 128:(t + 1) * 128]
            if turn:
                value = value * cos_ref[...] + pltpu.roll(value, 64, 1) * sin_ref[...]
            part[core, pl.ds(j * per + t, rows, stride=heads), :] = value
        if done:
            n = len(sends)
            copy = pltpu.make_async_remote_copy(src_ref=part.at[core], dst_ref=part.at[core], send_sem=send_sem.at[n],
                                                recv_sem=recv_sem.at[n], device_id=peer, device_id_type=mesh_id)
            copy.start()
            sends.append(copy)
            out = pltpu.make_async_copy(part.at[core], outs[n][1].at[core], out_sem.at[0, n])
            out.start()
            writes.append(out)
    for n, copy in enumerate(sends):
        copy.wait_recv()
        out = pltpu.make_async_copy(outs[n][0].at[1 - core], outs[n][1].at[1 - core], out_sem.at[1, n])
        out.start()
        writes.append(out)
    for copy in sends:
        copy.wait_send()
    for copy in writes:
        copy.wait()


def project(cur_pos, x_in, w_pre, table, w_q, w_k, w_v):
    rows, width = x_in.shape
    block = 512
    q_cols, kv_cols = w_q.shape[1], w_k.shape[1]
    n_blocks = (q_cols + 2 * kv_cols) // 2 // block
    vmem = pl.BlockSpec(memory_space=pltpu.VMEM)
    hbm = pl.BlockSpec(memory_space=pltpu.HBM)
    f32, bf = jnp.float32, jnp.bfloat16
    dma = pltpu.SemaphoreType.DMA
    return pl.pallas_call(
        project_kernel,
        out_shape=(pltpu.HBM((2, rows * q_cols // 256, 128), f32), pltpu.HBM((2, rows * kv_cols // 256, 128), f32),
                   pltpu.HBM((2, rows * kv_cols // 256, 128), f32)),
        in_specs=[pl.BlockSpec(memory_space=pltpu.SMEM), hbm, vmem, vmem] + [hbm] * 3,
        out_specs=(hbm,) * 3,
        scratch_shapes=[
            pltpu.VMEM((rows, width), bf),
            pltpu.VMEM((1, width), f32),
            pltpu.VMEM((rows, 128), f32),
            pltpu.VMEM((rows, 128), f32),
            pltpu.VMEM((n_blocks, width, block), bf),
            pltpu.VMEM((rows, width), bf),
            pltpu.VMEM((2, rows * q_cols // 256, 128), f32),
            pltpu.VMEM((2, rows * kv_cols // 256, 128), f32),
            pltpu.VMEM((2, rows * kv_cols // 256, 128), f32),
            dma((4,)), dma((n_blocks,)), dma((3,)), dma((3,)), dma((2, 3)),
        ],
        compiler_params=pltpu.CompilerParams(vmem_limit_bytes=62 * 1024 * 1024, collective_id=1, has_side_effects=True),
        cost_estimate=pl.CostEstimate(flops=rows * width * (q_cols + 2 * kv_cols), bytes_accessed=width * (q_cols + 2 * kv_cols), transcendentals=0),
        name='project',
    )(cur_pos, x_in, w_pre, table, w_q, w_k, w_v)


def attend_kernel(n_steps, first_row, kv_heads, seq_block, pos_ref, base_ref, q_hbm, kn_hbm, vn_hbm, k_hbm, v_hbm,
                  *rest):
    (ko_hbm, vo_hbm, o0_hbm, o1_hbm, o2_hbm, o3_hbm, m_ref, l_ref, kbuf, vbuf, qbuf, knbuf, vnbuf, obuf, key_ref, s_ref, p_ref, in_sem, out_sem, o_sem, st_sem) = rest[-21:]
    step_rows = ROWS_STEP
    piece_steps = n_steps // 4
    heads, head_dim = m_ref.shape
    q_half, kv_half = heads // 2, kv_heads // 2
    cols = seq_block * kv_heads
    base = base_ref[0]

    row_id = lax.broadcasted_iota(jnp.int32, (heads, cols), 0)
    col_id = lax.broadcasted_iota(jnp.int32, (heads, cols), 1)
    mine = lax.rem(col_id, kv_heads) == row_id // (heads // kv_heads)
    key_ref[...] = jnp.where(mine, col_id, cols * 4)
    lane_id = lax.broadcasted_iota(jnp.int32, m_ref.shape, 1)
    half_id = lax.broadcasted_iota(jnp.int32, (2 * kv_heads, head_dim), 0) // kv_heads

    def heads_of(step, count):
        return pl.ds((first_row + step * step_rows) * count, step_rows * count)

    def both_halves(ref, slot, r, count):
        at = slice(r * count, (r + 1) * count)
        return [ref[slot, 0, at, :], ref[slot, 1, at, :]]

    def loads(step, slot):
        rows = pl.ds(first_row + step * step_rows, step_rows)
        return (pltpu.make_async_copy(k_hbm.at[rows], kbuf.at[slot], in_sem.at[slot, 0]),
                pltpu.make_async_copy(v_hbm.at[rows], vbuf.at[slot], in_sem.at[slot, 1]),
                pltpu.make_async_copy(q_hbm.at[:, heads_of(step, q_half)], qbuf.at[slot], in_sem.at[slot, 2]),
                pltpu.make_async_copy(kn_hbm.at[:, heads_of(step, kv_half)], knbuf.at[slot], in_sem.at[slot, 3]),
                pltpu.make_async_copy(vn_hbm.at[:, heads_of(step, kv_half)], vnbuf.at[slot], in_sem.at[slot, 4]))

    def stores(step, slot):
        rows = pl.ds(first_row + step * step_rows, step_rows)
        return (pltpu.make_async_copy(kbuf.at[slot], ko_hbm.at[rows], out_sem.at[slot, 0]),
                pltpu.make_async_copy(vbuf.at[slot], vo_hbm.at[rows], out_sem.at[slot, 1]))

    def o_store(step, slot, d=0):
        at = pl.ds(lax.rem(step, piece_steps) * step_rows * heads, step_rows * heads)
        o_hbm = (o0_hbm, o1_hbm, o2_hbm, o3_hbm)[d]
        return pltpu.make_async_copy(obuf.at[slot], o_hbm.at[at], o_sem.at[slot])

    def o_start(step, slot):
        turn = jnp.bitwise_xor(step // piece_steps, base // seq_block)
        for d in range(4):
            @pl.when(turn == d)
            def _():
                o_store(step, slot, d).start()

    for step in range(min(START, n_steps)):
        for copy in loads(step, step):
            copy.start()
    m_ref[...] = jnp.zeros_like(m_ref)
    l_ref[...] = jnp.zeros_like(l_ref)
    scale = head_dim ** -0.5 / SOFT_CAP

    def body(step, carry):
        slot = lax.rem(step, SLOTS)
        oslot = lax.rem(step, 2)
        for copy in loads(step, slot):
            copy.wait()
        issued = jnp.minimum(step + AHEAD, START + 2 * step)
        wanted = jnp.minimum(jnp.minimum(step + 1 + AHEAD, START + 2 * step + 2), n_steps)
        for extra in range(2):
            nxt = issued + extra

            @pl.when(nxt < wanted)
            def _():
                nslot = lax.rem(nxt, SLOTS)

                @pl.when(nxt >= SLOTS)
                def _():
                    for copy in stores(nxt - SLOTS, nslot):
                        copy.wait()

                for copy in loads(nxt, nslot):
                    copy.start()

        for r in range(step_rows):
            local = pos_ref[first_row + step * step_rows + r] - base
            inside = (local >= 0) & (local < seq_block)
            at = jnp.clip(local, 0, seq_block - 1)
            pair = pl.ds(pl.multiple_of((at // 2) * (2 * kv_heads), 2 * kv_heads), 2 * kv_heads)
            hit = half_id == jnp.where(inside, lax.rem(at, 2), 2)
            k_row = jnp.concatenate(both_halves(knbuf, slot, r, kv_half) * 2, axis=0).astype(jnp.bfloat16)
            v_row = jnp.concatenate(both_halves(vnbuf, slot, r, kv_half) * 2, axis=0).astype(jnp.bfloat16)
            kbuf[slot, r, pair, :] = jnp.where(hit, k_row, kbuf[slot, r, pair, :])
            vbuf[slot, r, pair, :] = jnp.where(hit, v_row, vbuf[slot, r, pair, :])

        @pl.when(step >= 2)
        def _():
            o_store(step - 2, oslot).wait()

        m_all = m_ref[...]
        l_all = l_ref[...]
        half = cols // 2
        for tick in range(step_rows + LAG_OUT):
            r = tick
            if r < step_rows:
                q_row = jnp.concatenate(both_halves(qbuf, slot, r, q_half), axis=0).astype(jnp.bfloat16)
                raw = lax.dot_general(q_row, kbuf[slot, r], (((1,), (1,)), ((), ())),
                                      preferred_element_type=jnp.float32)
                s_ref[r] = raw
            r = tick - LAG_SOFT
            if 0 <= r < step_rows:
                local = pos_ref[first_row + step * step_rows + r] - base
                seen = key_ref[...] < (local + 1) * kv_heads
                soft = jnp.where(seen, jnp.tanh(s_ref[r] * scale), -4.0)
                top = jnp.maximum(jnp.max(soft, axis=-1, keepdims=True), -1.0)
                weight = jnp.exp2((soft - top) * (SOFT_CAP * LOG2E))
                total = jnp.sum(weight, axis=-1, keepdims=True)
                weight = weight.astype(jnp.bfloat16)
                p_ref[r, :heads] = weight[:, :half]
                p_ref[r, heads:] = weight[:, half:]
                here = lane_id == step * step_rows + r
                m_all = jnp.where(here, top * SOFT_CAP, m_all)
                l_all = jnp.where(here, total, l_all)
            r = tick - LAG_OUT
            if 0 <= r < step_rows:
                right = jnp.concatenate([vbuf[slot, r, :half, :], vbuf[slot, r, half:, :]], axis=1)
                both = jnp.dot(p_ref[r], right, preferred_element_type=jnp.float32)
                obuf[oslot, r * heads:(r + 1) * heads, :] = both[:heads, :head_dim] + both[heads:, head_dim:]
        m_ref[...] = m_all
        l_ref[...] = l_all
        o_start(step, oslot)
        for copy in stores(step, slot):
            copy.start()

        return carry

    lax.fori_loop(0, n_steps, body, 0)
    tail = piece_steps * step_rows * heads
    stat_copies = []
    for d, o_hbm in enumerate((o0_hbm, o1_hbm, o2_hbm, o3_hbm)):
        stat_copies.append(pltpu.make_async_copy(m_ref, o_hbm.at[pl.ds(tail, heads)], st_sem.at[d, 0]))
        stat_copies.append(pltpu.make_async_copy(l_ref, o_hbm.at[pl.ds(tail + heads, heads)], st_sem.at[d, 1]))
    for copy in stat_copies:
        copy.start()
    for copy in stat_copies:
        copy.wait()
    for step in range(max(0, n_steps - SLOTS), n_steps):
        for copy in stores(step, step % SLOTS):
            copy.wait()
    for step in range(max(0, n_steps - 2), n_steps):
        o_store(step, step % 2).wait()


def attend(pos, base, q, kn, vn, k_cache, v_cache, prev, first_row, n_rows):
    rows, cols, head_dim = k_cache.shape
    heads = 2 * q.shape[1] // rows
    kv_heads = 2 * kn.shape[1] // rows
    seq_block = cols // kv_heads
    n_steps = n_rows // ROWS_STEP
    hbm = pl.BlockSpec(memory_space=pl.ANY)
    piece = pltpu.HBM((n_rows // 4 * heads + 2 * heads, head_dim), jnp.float32)
    smem = pl.BlockSpec(memory_space=pltpu.SMEM)
    bf = jnp.bfloat16
    aliases = {} if prev is None else {7: 0, 8: 1}
    extra = () if prev is None else tuple(prev)
    return pl.pallas_call(
        functools.partial(attend_kernel, n_steps, first_row, kv_heads, seq_block),
        out_shape=(jax.ShapeDtypeStruct(k_cache.shape, bf), jax.ShapeDtypeStruct(v_cache.shape, bf)) + (piece,) * 4,
        in_specs=[smem, smem, hbm, hbm, hbm, hbm, hbm] + [hbm] * len(extra),
        out_specs=(hbm, hbm) + (pl.BlockSpec(memory_space=pltpu.HBM),) * 4,
        scratch_shapes=[
            pltpu.VMEM((heads, 128), jnp.float32),
            pltpu.VMEM((heads, 128), jnp.float32),
            pltpu.VMEM((SLOTS, ROWS_STEP, cols, head_dim), bf),
            pltpu.VMEM((SLOTS, ROWS_STEP, cols, head_dim), bf),
            pltpu.VMEM((SLOTS, 2, ROWS_STEP * heads // 2, head_dim), jnp.float32),
            pltpu.VMEM((SLOTS, 2, ROWS_STEP * kv_heads // 2, head_dim), jnp.float32),
            pltpu.VMEM((SLOTS, 2, ROWS_STEP * kv_heads // 2, head_dim), jnp.float32),
            pltpu.VMEM((2, ROWS_STEP * heads, head_dim), jnp.float32),
            pltpu.VMEM((heads, cols), jnp.int32),
            pltpu.VMEM((ROWS_STEP, heads, cols), jnp.float32),
            pltpu.VMEM((ROWS_STEP, 2 * heads, cols // 2), bf),
            pltpu.SemaphoreType.DMA((SLOTS, 5)),
            pltpu.SemaphoreType.DMA((SLOTS, 2)),
            pltpu.SemaphoreType.DMA((2,)),
            pltpu.SemaphoreType.DMA((4, 2)),
        ],
        input_output_aliases=aliases,
        compiler_params=pltpu.CompilerParams(vmem_limit_bytes=62 * 1024 * 1024),
        cost_estimate=pl.CostEstimate(flops=n_rows * heads * cols * head_dim * 4,
                                      bytes_accessed=n_rows * cols * head_dim * 8, transcendentals=0),
        name='attend',
    )(pos, base, q, kn, vn, k_cache, v_cache, *extra)


def merge_kernel(chunks, *refs):
    n_in = 4 * len(chunks)
    source = [refs[4 * c:4 * c + 4] for c in range(len(chunks))]
    pieces = [[b.at[d] for d in range(4)] for b in refs[-len(chunks):]]
    refs = refs[:-len(chunks)]
    (x_hbm, wpost_hbm, wo_hbm, out_ref, wo, xbuf, wpost_ref, last_in, osum, lhs, y_out, y_in, sums,
     in_sem, p_sem, w_sem, o_send, o_recv, y_send, y_recv, g_send, g_recv, d_send, d_recv, f_send, f_recv) = refs[n_in:]
    sp = lax.axis_index('sp')
    tp = lax.axis_index('tp')
    core = lax.rem(sp, 2)
    xpos = sp // 2
    _, width = xbuf.shape
    n_chunks, quarter, chunk = y_out.shape
    heads = lhs.shape[1] // 128
    parts = [c // 4 for c in chunks]
    core_peer = {'sp': 2 * xpos + (1 - core)}
    x_peer = {'sp': 2 * (1 - xpos) + core}
    far_peer = {'sp': 2 * (1 - xpos) + (1 - core)}
    y_peer = {'tp': 1 - tp}
    mesh_id = pl.DeviceIdType.MESH

    def remote(src, dst, send, recv, peer):
        return pltpu.make_async_remote_copy(src_ref=src, dst_ref=dst, send_sem=send, recv_sem=recv,
                                            device_id=peer, device_id_type=mesh_id)

    def w_load(n):
        return pltpu.make_async_copy(wo_hbm.at[:, pl.ds(n * chunk, chunk)], wo.at[n], w_sem.at[n])

    small = [pltpu.make_async_copy(x_hbm, xbuf, in_sem.at[0]), pltpu.make_async_copy(wpost_hbm, wpost_ref, in_sem.at[1])]
    local = [[pltpu.make_async_copy(source[c][d], pieces[c][d], p_sem.at[c, d]) for d in range(4)] for c in range(len(chunks))]
    for group in local:
        for copy in group:
            copy.start()
    for n in range(2):
        w_load(n).start()
    barrier = pltpu.get_barrier_semaphore()
    for peer in (core_peer, x_peer, far_peer, y_peer):
        pl.semaphore_signal(barrier, inc=1, device_id=peer, device_id_type=mesh_id)
    pl.semaphore_wait(barrier, 4)

    for copy in local[-1]:
        copy.wait()
    last = [remote(pieces[-1][d], last_in.at[d - 1], o_send.at[d - 1], o_recv.at[d - 1], peer)
            for d, peer in ((2, x_peer), (3, far_peer), (1, core_peer))]
    for copy in last:
        copy.start()

    def combine(blocks, part, row0):
        count = part * heads
        stats = [block[count:count + 2 * heads, :] for block in blocks]
        top = functools.reduce(jnp.maximum, [st[:heads] for st in stats])
        grown = [jnp.exp(st[:heads] - top) for st in stats]
        total = sum(st[heads:] * g for st, g in zip(stats, grown))
        shift = lax.rem(128 - sp * part, 128)
        factors = [pltpu.roll(g / total, shift, 1) for g in grown]
        for b in range(part):
            at = slice(b * heads, (b + 1) * heads)
            osum[at, :] = sum(block[at, :] * f[:, b:b + 1] for block, f in zip(blocks, factors))
        for h in range(heads):
            lhs[row0:row0 + part, h * 128:(h + 1) * 128] = osum[pl.ds(h, part, stride=heads), :].astype(jnp.bfloat16)

    first = sum(parts[:-1])
    row0 = 0
    for c in range(len(chunks) - 1):
        for copy in local[c]:
            copy.wait()
        combine(pieces[c], parts[c], row0)
        row0 += parts[c]

    first_at, last_at = pl.ds(0, first), pl.ds(first, quarter - first)
    split = ((2, 2, 2, 2, 1), (1, 2, 2, 2, 2))
    wide = 3
    orders = []
    for sizes in split:
        begin, order = 0, []
        for size in sizes:
            order.append((begin, size, first_at))
            begin += size
        orders.append(order + [(n, wide, last_at) for n in range(0, n_chunks, wide)])
    n_pieces = len(orders[0])

    def to_y(v, t):
        n, size, r = orders[v][t]
        ns = pl.ds(n, size)
        return remote(y_out.at[ns, r], y_in.at[ns, r], y_send.at[t], y_recv.at[t], y_peer)

    def to_x(v, t):
        n, size, r = orders[v][t]
        ns = pl.ds(n, size)
        return remote(sums.at[sp, ns, r], sums.at[sp, ns, r], g_send.at[t], g_recv.at[t], x_peer)

    def to_core(v, t):
        n, size, r = orders[v][t]
        ns = pl.ds(n, size)
        return remote(sums.at[sp, ns, r], sums.at[sp, ns, r], d_send.at[t], d_recv.at[t], core_peer)

    def relay(v, t):
        n, size, r = orders[v][t]
        ns = pl.ds(n, size)
        other = 2 * (1 - xpos) + core
        return remote(sums.at[other, ns, r], sums.at[other, ns, r], f_send.at[t], f_recv.at[t], core_peer)

    def project_rows(n, r0, count):
        y_out[n, r0:r0 + count, :] = jnp.dot(lhs[r0:r0 + count, :], wo[n], preferred_element_type=jnp.float32)

    for n in range(n_chunks):
        w_load(n).wait()
        if n + 2 < n_chunks:
            w_load(n + 2).start()
        else:
            small[n + 2 - n_chunks].start()
        project_rows(n, 0, first)
        for v in range(2):
            for t in range(2):
                if sum(orders[v][t][:2]) == n + 1:
                    @pl.when(core == v)
                    def _():
                        to_y(v, t).start()

    def step(v, t):
        if t < n_pieces:
            n, size, r = orders[v][t]
            ns = pl.ds(n, size)
            to_y(v, t).wait()
            if t + 2 < n_pieces:
                to_y(v, t + 2).start()
            sums[sp, ns, r, :] = y_out[ns, r, :] + y_in[ns, r, :]
            to_x(v, t).start()
            to_core(v, t).start()
        if t >= 1:
            to_x(v, t - 1).wait_recv()
            relay(v, t - 1).start()

    for t in range(n_pieces + 1):
        if t == 1:
            for copy in last:
                copy.wait()
            combine([pieces[-1][0]] + [last_in.at[d] for d in range(3)], parts[-1], first)
        if 1 <= t < 1 + n_chunks // wide:
            for n in range((t - 1) * wide, t * wide):
                project_rows(n, first, quarter - first)
        for v in range(2):
            @pl.when(core == v)
            def _():
                step(v, t)
    for copy in small:
        copy.wait()
    for v in range(2):
        @pl.when(core == v)
        def _():
            for t in range(n_pieces):
                to_x(v, t).wait_send()
                to_core(v, t).wait_send()
                relay(v, t).wait_send()
                to_core(1 - v, t).wait_recv()
                relay(1 - v, t).wait_recv()

    starts = []
    base = 0
    for c, part in zip(chunks, parts):
        starts += [(base, part, k) for k in range(0, part, 16)]
        base += c
    for q in range(4):
        for k, (base, part, off) in enumerate(starts):
            at = slice(k * 16, (k + 1) * 16)
            out_at = slice(base + q * part + off, base + q * part + off + 16)
            square = jnp.zeros((16, chunk), jnp.float32)
            for n in range(n_chunks):
                u = sums[q, n, at, :]
                square = square + u * u
            inv = lax.rsqrt(jnp.sum(square, axis=-1, keepdims=True) * (1.0 / width) + NORM_EPS)
            for n in range(n_chunks):
                col = slice(n * chunk, (n + 1) * chunk)
                y = xbuf[out_at, col].astype(jnp.float32) + sums[q, n, at, :] * inv * (1.0 + wpost_ref[:, col])
                out_ref[out_at, col] = y.astype(jnp.bfloat16)


def merge(chunks, pieces, x_in, w_post, w_o, n_chunks):
    rows, width = x_in.shape
    inner = w_o.shape[0]
    heads = inner // 128
    quarter = rows // 4
    chunk = width // n_chunks
    vmem = pl.BlockSpec(memory_space=pltpu.VMEM)
    hbm = pl.BlockSpec(memory_space=pl.ANY)
    f32 = jnp.float32
    dma = pltpu.SemaphoreType.DMA
    per_piece = dma((n_chunks + 3,))
    flat = [p for piece in pieces for p in piece]
    big = max(chunks) // 4 * heads
    return pl.pallas_call(
        functools.partial(merge_kernel, chunks),
        out_shape=jax.ShapeDtypeStruct(x_in.shape, x_in.dtype),
        in_specs=[pl.BlockSpec(memory_space=pltpu.HBM)] * (len(flat) + 3),
        out_specs=vmem,
        scratch_shapes=[
            pltpu.VMEM((n_chunks, inner, chunk), jnp.bfloat16),
            pltpu.VMEM(x_in.shape, x_in.dtype),
            pltpu.VMEM(w_post.shape, f32),
            pltpu.VMEM((3,) + pieces[-1][0].shape, f32),
            pltpu.VMEM((big, 128), f32),
            pltpu.VMEM((quarter, inner), jnp.bfloat16),
            pltpu.VMEM((n_chunks, quarter, chunk), f32),
            pltpu.VMEM((n_chunks, quarter, chunk), f32),
            pltpu.VMEM((4, n_chunks, quarter, chunk), f32),
            dma((2,)), dma((len(chunks), 4)), dma((n_chunks,)), dma((3,)), dma((3,)),
        ] + [per_piece] * 8 + [pltpu.VMEM((4,) + piece[0].shape, f32) for piece in pieces],
        compiler_params=pltpu.CompilerParams(vmem_limit_bytes=56 * 1024 * 1024, collective_id=0, has_side_effects=True),
        cost_estimate=pl.CostEstimate(flops=2 * quarter * inner * width, bytes_accessed=2 * inner * width, transcendentals=0),
        name='merge',
    )(*flat, x_in, w_post, pltpu.with_memory_space_constraint(w_o, pltpu.HBM))


def solution(mesh):
    cache_spec = P('dp', 'sp', 'tp', None)
    sp_size = mesh.shape['sp']

    def local_step(x_in, cur_pos, w_pre, w_q, w_k, w_v, w_o, w_post, k_cache, v_cache):
        row_count, seq_block, kv_local, head_dim = k_cache.shape
        sp_index = lax.axis_index('sp')
        table = rotary_table(sp_size * seq_block, head_dim)
        q_rot, kn2, vn2 = project(cur_pos, x_in, w_pre.reshape(-1, 128), table, w_q, w_k, w_v)
        base = (sp_index * seq_block).astype(jnp.int32).reshape(1)
        kc = k_cache.reshape(row_count, seq_block * kv_local, head_dim)
        vc = v_cache.reshape(row_count, seq_block * kv_local, head_dim)
        chunks = (row_count // 2, row_count // 4, row_count // 4)
        prev, first_row, pieces = None, 0, []
        for index, n_rows in enumerate(chunks):
            *prev, p0, p1, p2, p3 = attend(cur_pos, base, q_rot, kn2, vn2, kc, vc, prev, first_row, n_rows)
            first_row += n_rows
            if index < len(chunks) - 1:
                moved = []
                for d, p in ((1, p1), (2, p2), (3, p3)):
                    moved.append(lax.ppermute(p, 'sp', [(i, i ^ d) for i in range(sp_size)]))
                p1, p2, p3 = moved
            pieces.append((p0, p1, p2, p3))
        k_out, v_out = prev
        x_out = merge(chunks, pieces, x_in, w_post.reshape(1, -1), w_o, 9)
        return x_out, k_out.reshape(k_cache.shape), v_out.reshape(v_cache.shape)

    return jax.shard_map(local_step, mesh=mesh,
                         in_specs=(P('dp', None), P('dp'), P(None), P(None, 'tp'), P(None, 'tp'), P(None, 'tp'), P('tp', None), P(None), cache_spec, cache_spec),
                         out_specs=(P('dp', None), cache_spec, cache_spec), check_vma=False)
```

```python
import functools

import jax
import jax.numpy as jnp
import numpy as np
from jax import lax
from jax.experimental import pallas as pl
from jax.experimental.pallas import tpu as pltpu
from jax.sharding import PartitionSpec as P


SOFT_CAP = 50.0
ROPE_BASE = 10000.0
NORM_EPS = 1e-6
LOG2E = 1.4426950408889634

ROWS_STEP = 8
SLOTS = 12
AHEAD = 6
START = 2
LAG_SOFT = 2
LAG_OUT = 4


def rotary_table(length, head_dim):
    half_dim = head_dim // 2
    inv_freq = np.power(np.float32(ROPE_BASE), -2.0 * np.arange(half_dim, dtype=np.float32) / np.float32(2 * half_dim)).astype(np.float32)
    angles = np.arange(length, dtype=np.float32)[:, None] * inv_freq[None, :]
    cos_tab = np.cos(angles.astype(np.float64))
    sin_tab = np.sin(angles.astype(np.float64))
    return np.concatenate([cos_tab, cos_tab, -sin_tab, sin_tab], axis=-1).astype(np.float32)


def project_kernel(pos_ref, x_hbm, wpre_ref, table_ref, wq_hbm, wk_hbm, wv_hbm, q_ref, k_ref, v_ref,
                   x_ref, gain_ref, cos_ref, sin_ref, weight, normed, q_part, k_part, v_part, x_sem, w_sem, send_sem, recv_sem,
                   out_sem):
    sp = lax.axis_index('sp')
    core = lax.rem(sp, 2)
    peer = {'sp': sp + 1 - 2 * core}
    mesh_id = pl.DeviceIdType.MESH
    rows = x_ref.shape[0]
    block = weight.shape[2]
    per = block // 128
    plan = []
    for w_hbm, part, turn in ((wq_hbm, q_part, True), (wk_hbm, k_part, True), (wv_hbm, v_part, False)):
        mine = w_hbm.shape[1] // 2
        for j in range(mine // block):
            plan.append((w_hbm, part, turn, mine, j, j == mine // block - 1))

    def load(i):
        w_hbm, _, _, mine, j, _ = plan[i]
        col = pl.multiple_of(core * mine + j * block, block)
        return pltpu.make_async_copy(w_hbm.at[:, pl.ds(col, block)], weight.at[i], w_sem.at[i])

    x_loads = [pltpu.make_async_copy(x_hbm.at[pl.ds(k * (rows // 4), rows // 4)], x_ref.at[pl.ds(k * (rows // 4), rows // 4)],
                                     x_sem.at[k]) for k in range(4)]
    for copy in x_loads:
        copy.start()
    load(0).start()
    barrier = pltpu.get_barrier_semaphore()
    pl.semaphore_signal(barrier, inc=1, device_id=peer, device_id_type=mesh_id)
    pl.semaphore_wait(barrier, 1)

    for j in range(wpre_ref.shape[0]):
        gain_ref[:, j * 128:(j + 1) * 128] = 1.0 + wpre_ref[j:j + 1, :]
    gain = gain_ref[...]

    def look_up(k, carry):
        for r in range(8):
            b = k * 8 + r
            row = table_ref[pl.ds(pos_ref[b], 1), :]
            cos_ref[pl.ds(b, 1), :] = row[:, :128]
            sin_ref[pl.ds(b, 1), :] = row[:, 128:]
        return carry

    lax.fori_loop(0, rows // 8, look_up, 0)

    def norm(k, carry):
        at = pl.ds(pl.multiple_of(k * 16, 16), 16)
        x = x_ref[at, :].astype(jnp.float32)
        inv = lax.rsqrt(jnp.mean(x * x, axis=-1, keepdims=True) + NORM_EPS)
        normed[at, :] = (x * inv * gain).astype(jnp.bfloat16)
        return carry

    for k in range(4):
        x_loads[k].wait()
        if k == 1:
            load(1).start()
        lax.fori_loop(k * rows // 64, (k + 1) * rows // 64, norm, 0)

    outs = ((q_part, q_ref), (k_part, k_ref), (v_part, v_ref))
    sends, writes = [], []
    for i, (_, part, turn, mine, j, done) in enumerate(plan):
        load(i).wait()
        if i + 2 < len(plan):
            load(i + 2).start()
        heads = mine // 128
        acc = jnp.dot(normed[...], weight[i], preferred_element_type=jnp.float32)
        for t in range(per):
            value = acc[:, t * 128:(t + 1) * 128]
            if turn:
                value = value * cos_ref[...] + pltpu.roll(value, 64, 1) * sin_ref[...]
            part[core, pl.ds(j * per + t, rows, stride=heads), :] = value
        if done:
            n = len(sends)
            copy = pltpu.make_async_remote_copy(src_ref=part.at[core], dst_ref=part.at[core], send_sem=send_sem.at[n],
                                                recv_sem=recv_sem.at[n], device_id=peer, device_id_type=mesh_id)
            copy.start()
            sends.append(copy)
            out = pltpu.make_async_copy(part.at[core], outs[n][1].at[core], out_sem.at[0, n])
            out.start()
            writes.append(out)
    for n, copy in enumerate(sends):
        copy.wait_recv()
        out = pltpu.make_async_copy(outs[n][0].at[1 - core], outs[n][1].at[1 - core], out_sem.at[1, n])
        out.start()
        writes.append(out)
    for copy in sends:
        copy.wait_send()
    for copy in writes:
        copy.wait()


def project(cur_pos, x_in, w_pre, table, w_q, w_k, w_v):
    rows, width = x_in.shape
    block = 512
    q_cols, kv_cols = w_q.shape[1], w_k.shape[1]
    n_blocks = (q_cols + 2 * kv_cols) // 2 // block
    vmem = pl.BlockSpec(memory_space=pltpu.VMEM)
    hbm = pl.BlockSpec(memory_space=pltpu.HBM)
    f32, bf = jnp.float32, jnp.bfloat16
    dma = pltpu.SemaphoreType.DMA
    return pl.pallas_call(
        project_kernel,
        out_shape=(pltpu.HBM((2, rows * q_cols // 256, 128), f32), pltpu.HBM((2, rows * kv_cols // 256, 128), f32),
                   pltpu.HBM((2, rows * kv_cols // 256, 128), f32)),
        in_specs=[pl.BlockSpec(memory_space=pltpu.SMEM), hbm, vmem, vmem] + [hbm] * 3,
        out_specs=(hbm,) * 3,
        scratch_shapes=[
            pltpu.VMEM((rows, width), bf),
            pltpu.VMEM((1, width), f32),
            pltpu.VMEM((rows, 128), f32),
            pltpu.VMEM((rows, 128), f32),
            pltpu.VMEM((n_blocks, width, block), bf),
            pltpu.VMEM((rows, width), bf),
            pltpu.VMEM((2, rows * q_cols // 256, 128), f32),
            pltpu.VMEM((2, rows * kv_cols // 256, 128), f32),
            pltpu.VMEM((2, rows * kv_cols // 256, 128), f32),
            dma((4,)), dma((n_blocks,)), dma((3,)), dma((3,)), dma((2, 3)),
        ],
        compiler_params=pltpu.CompilerParams(vmem_limit_bytes=62 * 1024 * 1024, collective_id=1, has_side_effects=True),
        cost_estimate=pl.CostEstimate(flops=rows * width * (q_cols + 2 * kv_cols), bytes_accessed=width * (q_cols + 2 * kv_cols), transcendentals=0),
        name='project',
    )(cur_pos, x_in, w_pre, table, w_q, w_k, w_v)


def attend_kernel(n_steps, quarter, first_row, kv_heads, seq_block, pos_ref, base_ref, q_hbm, kn_hbm, vn_hbm, k_hbm, v_hbm,
                  *rest):
    (ko_hbm, vo_hbm, o0_hbm, o1_hbm, o2_hbm, o3_hbm, m_ref, l_ref, kbuf, vbuf, qbuf, knbuf, vnbuf, obuf, key_ref, s_ref, p_ref, in_sem, out_sem, o_sem, st_sem) = rest[-21:]
    step_rows = ROWS_STEP
    piece_steps = n_steps // 4
    heads, head_dim = m_ref.shape
    q_half, kv_half = heads // 2, kv_heads // 2
    cols = seq_block * kv_heads
    base = base_ref[0]

    row_id = lax.broadcasted_iota(jnp.int32, (heads, cols), 0)
    col_id = lax.broadcasted_iota(jnp.int32, (heads, cols), 1)
    mine = lax.rem(col_id, kv_heads) == row_id // (heads // kv_heads)
    key_ref[...] = jnp.where(mine, col_id, cols * 4)
    lane_id = lax.broadcasted_iota(jnp.int32, m_ref.shape, 1)
    half_id = lax.broadcasted_iota(jnp.int32, (2 * kv_heads, head_dim), 0) // kv_heads

    def row_of(step):
        piece = step // piece_steps
        return piece * quarter + first_row + (step - piece * piece_steps) * step_rows

    def heads_of(step, count):
        return pl.ds(row_of(step) * count, step_rows * count)

    def both_halves(ref, slot, r, count):
        at = slice(r * count, (r + 1) * count)
        return [ref[slot, 0, at, :], ref[slot, 1, at, :]]

    def loads(step, slot):
        rows = pl.ds(row_of(step), step_rows)
        return (pltpu.make_async_copy(k_hbm.at[rows], kbuf.at[slot], in_sem.at[slot, 0]),
                pltpu.make_async_copy(v_hbm.at[rows], vbuf.at[slot], in_sem.at[slot, 1]),
                pltpu.make_async_copy(q_hbm.at[:, heads_of(step, q_half)], qbuf.at[slot], in_sem.at[slot, 2]),
                pltpu.make_async_copy(kn_hbm.at[:, heads_of(step, kv_half)], knbuf.at[slot], in_sem.at[slot, 3]),
                pltpu.make_async_copy(vn_hbm.at[:, heads_of(step, kv_half)], vnbuf.at[slot], in_sem.at[slot, 4]))

    def stores(step, slot):
        rows = pl.ds(row_of(step), step_rows)
        return (pltpu.make_async_copy(kbuf.at[slot], ko_hbm.at[rows], out_sem.at[slot, 0]),
                pltpu.make_async_copy(vbuf.at[slot], vo_hbm.at[rows], out_sem.at[slot, 1]))

    def o_store(step, slot, d=0):
        at = pl.ds((step - step // piece_steps * piece_steps) * step_rows * heads, step_rows * heads)
        o_hbm = (o0_hbm, o1_hbm, o2_hbm, o3_hbm)[d]
        return pltpu.make_async_copy(obuf.at[slot], o_hbm.at[at], o_sem.at[slot])

    def o_start(step, slot):
        turn = jnp.bitwise_xor(step // piece_steps, base // seq_block)
        for d in range(4):
            @pl.when(turn == d)
            def _():
                o_store(step, slot, d).start()

    for step in range(min(START, n_steps)):
        for copy in loads(step, step):
            copy.start()
    m_ref[...] = jnp.zeros_like(m_ref)
    l_ref[...] = jnp.zeros_like(l_ref)
    scale = head_dim ** -0.5 / SOFT_CAP

    def body(step, carry):
        slot = lax.rem(step, SLOTS)
        oslot = lax.rem(step, 2)
        for copy in loads(step, slot):
            copy.wait()
        issued = jnp.minimum(step + AHEAD, START + 2 * step)
        wanted = jnp.minimum(jnp.minimum(step + 1 + AHEAD, START + 2 * step + 2), n_steps)
        for extra in range(2):
            nxt = issued + extra

            @pl.when(nxt < wanted)
            def _():
                nslot = lax.rem(nxt, SLOTS)

                @pl.when(nxt >= SLOTS)
                def _():
                    for copy in stores(nxt - SLOTS, nslot):
                        copy.wait()

                for copy in loads(nxt, nslot):
                    copy.start()

        for r in range(step_rows):
            local = pos_ref[row_of(step) + r] - base
            inside = (local >= 0) & (local < seq_block)
            at = jnp.clip(local, 0, seq_block - 1)
            pair = pl.ds(pl.multiple_of((at // 2) * (2 * kv_heads), 2 * kv_heads), 2 * kv_heads)
            hit = half_id == jnp.where(inside, lax.rem(at, 2), 2)
            k_row = jnp.concatenate(both_halves(knbuf, slot, r, kv_half) * 2, axis=0).astype(jnp.bfloat16)
            v_row = jnp.concatenate(both_halves(vnbuf, slot, r, kv_half) * 2, axis=0).astype(jnp.bfloat16)
            kbuf[slot, r, pair, :] = jnp.where(hit, k_row, kbuf[slot, r, pair, :])
            vbuf[slot, r, pair, :] = jnp.where(hit, v_row, vbuf[slot, r, pair, :])

        @pl.when(step >= 2)
        def _():
            o_store(step - 2, oslot).wait()

        m_all = m_ref[...]
        l_all = l_ref[...]
        half = cols // 2
        for tick in range(step_rows + LAG_OUT):
            r = tick
            if r < step_rows:
                q_row = jnp.concatenate(both_halves(qbuf, slot, r, q_half), axis=0).astype(jnp.bfloat16)
                raw = lax.dot_general(q_row, kbuf[slot, r], (((1,), (1,)), ((), ())),
                                      preferred_element_type=jnp.float32)
                s_ref[r] = raw
            r = tick - LAG_SOFT
            if 0 <= r < step_rows:
                local = pos_ref[row_of(step) + r] - base
                seen = key_ref[...] < (local + 1) * kv_heads
                soft = jnp.where(seen, jnp.tanh(s_ref[r] * scale), -4.0)
                top = jnp.maximum(jnp.max(soft, axis=-1, keepdims=True), -1.0)
                weight = jnp.exp2((soft - top) * (SOFT_CAP * LOG2E))
                total = jnp.sum(weight, axis=-1, keepdims=True)
                weight = weight.astype(jnp.bfloat16)
                p_ref[r, :heads] = weight[:, :half]
                p_ref[r, heads:] = weight[:, half:]
                here = lane_id == step * step_rows + r
                m_all = jnp.where(here, top * SOFT_CAP, m_all)
                l_all = jnp.where(here, total, l_all)
            r = tick - LAG_OUT
            if 0 <= r < step_rows:
                right = jnp.concatenate([vbuf[slot, r, :half, :], vbuf[slot, r, half:, :]], axis=1)
                both = jnp.dot(p_ref[r], right, preferred_element_type=jnp.float32)
                obuf[oslot, r * heads:(r + 1) * heads, :] = both[:heads, :head_dim] + both[heads:, head_dim:]
        m_ref[...] = m_all
        l_ref[...] = l_all
        o_start(step, oslot)
        for copy in stores(step, slot):
            copy.start()

        return carry

    lax.fori_loop(0, n_steps, body, 0)
    tail = piece_steps * step_rows * heads
    stat_copies = []
    for d, o_hbm in enumerate((o0_hbm, o1_hbm, o2_hbm, o3_hbm)):
        stat_copies.append(pltpu.make_async_copy(m_ref, o_hbm.at[pl.ds(tail, heads)], st_sem.at[d, 0]))
        stat_copies.append(pltpu.make_async_copy(l_ref, o_hbm.at[pl.ds(tail + heads, heads)], st_sem.at[d, 1]))
    for copy in stat_copies:
        copy.start()
    for copy in stat_copies:
        copy.wait()
    for step in range(max(0, n_steps - SLOTS), n_steps):
        for copy in stores(step, step % SLOTS):
            copy.wait()
    for step in range(max(0, n_steps - 2), n_steps):
        o_store(step, step % 2).wait()


def attend(pos, base, q, kn, vn, k_cache, v_cache, prev, first_row, n_rows):
    rows, cols, head_dim = k_cache.shape
    heads = 2 * q.shape[1] // rows
    kv_heads = 2 * kn.shape[1] // rows
    seq_block = cols // kv_heads
    n_steps = n_rows // ROWS_STEP
    hbm = pl.BlockSpec(memory_space=pl.ANY)
    piece = pltpu.HBM((n_rows // 4 * heads + 2 * heads, head_dim), jnp.float32)
    smem = pl.BlockSpec(memory_space=pltpu.SMEM)
    bf = jnp.bfloat16
    aliases = {} if prev is None else {7: 0, 8: 1}
    extra = () if prev is None else tuple(prev)
    return pl.pallas_call(
        functools.partial(attend_kernel, n_steps, rows // 4, first_row, kv_heads, seq_block),
        out_shape=(jax.ShapeDtypeStruct(k_cache.shape, bf), jax.ShapeDtypeStruct(v_cache.shape, bf)) + (piece,) * 4,
        in_specs=[smem, smem, hbm, hbm, hbm, hbm, hbm] + [hbm] * len(extra),
        out_specs=(hbm, hbm) + (pl.BlockSpec(memory_space=pltpu.HBM),) * 4,
        scratch_shapes=[
            pltpu.VMEM((heads, 128), jnp.float32),
            pltpu.VMEM((heads, 128), jnp.float32),
            pltpu.VMEM((SLOTS, ROWS_STEP, cols, head_dim), bf),
            pltpu.VMEM((SLOTS, ROWS_STEP, cols, head_dim), bf),
            pltpu.VMEM((SLOTS, 2, ROWS_STEP * heads // 2, head_dim), jnp.float32),
            pltpu.VMEM((SLOTS, 2, ROWS_STEP * kv_heads // 2, head_dim), jnp.float32),
            pltpu.VMEM((SLOTS, 2, ROWS_STEP * kv_heads // 2, head_dim), jnp.float32),
            pltpu.VMEM((2, ROWS_STEP * heads, head_dim), jnp.float32),
            pltpu.VMEM((heads, cols), jnp.int32),
            pltpu.VMEM((ROWS_STEP, heads, cols), jnp.float32),
            pltpu.VMEM((ROWS_STEP, 2 * heads, cols // 2), bf),
            pltpu.SemaphoreType.DMA((SLOTS, 5)),
            pltpu.SemaphoreType.DMA((SLOTS, 2)),
            pltpu.SemaphoreType.DMA((2,)),
            pltpu.SemaphoreType.DMA((4, 2)),
        ],
        input_output_aliases=aliases,
        compiler_params=pltpu.CompilerParams(vmem_limit_bytes=62 * 1024 * 1024),
        cost_estimate=pl.CostEstimate(flops=n_rows * heads * cols * head_dim * 4,
                                      bytes_accessed=n_rows * cols * head_dim * 8, transcendentals=0),
        name='attend',
    )(pos, base, q, kn, vn, k_cache, v_cache, *extra)


def merge_kernel(chunks, *refs):
    n_in = 4 * len(chunks)
    source = [refs[4 * c:4 * c + 4] for c in range(len(chunks))]
    pieces = [[b.at[d] for d in range(4)] for b in refs[-len(chunks):]]
    refs = refs[:-len(chunks)]
    (wo_hbm, out_hbm, wo, last_in, last_out, osum, lhs, y_out, y_in, sums,
     p_sem, w_sem, o_send, o_recv, y_send, y_recv, g_send, g_recv, d_send, d_recv, f_send, f_recv, out_sem) = refs[n_in:]
    sp = lax.axis_index('sp')
    tp = lax.axis_index('tp')
    core = lax.rem(sp, 2)
    xpos = sp // 2
    n_chunks, _, chunk = y_out.shape
    heads = lhs.shape[1] // 128
    parts = [c // 4 for c in chunks]
    core_id = 2 * xpos + (1 - core)
    x_id = 2 * (1 - xpos) + core
    far_id = 2 * (1 - xpos) + (1 - core)
    core_peer, x_peer, y_peer = {'sp': core_id}, {'sp': x_id}, {'tp': 1 - tp}
    mesh_id = pl.DeviceIdType.MESH

    def remote(src, dst, send, recv, peer):
        return pltpu.make_async_remote_copy(src_ref=src, dst_ref=dst, send_sem=send, recv_sem=recv,
                                            device_id=peer, device_id_type=mesh_id)

    def w_load(n):
        return pltpu.make_async_copy(wo_hbm.at[:, pl.ds(n * chunk, chunk)], wo.at[n], w_sem.at[n])

    local = [[pltpu.make_async_copy(source[c][d], pieces[c][d], p_sem.at[c, d]) for d in range(4)] for c in range(len(chunks))]
    for group in (local[-1], local[0]):
        for copy in group:
            copy.start()
    for n in range(2):
        w_load(n).start()
    barrier = pltpu.get_barrier_semaphore()
    for peer in (core_peer, x_peer, y_peer):
        pl.semaphore_signal(barrier, inc=1, device_id=peer, device_id_type=mesh_id)
    pl.semaphore_wait(barrier, 3)

    for copy in local[-1]:
        copy.wait()
    last = [remote(pieces[-1][3], last_in.at[0], o_send.at[0], o_recv.at[0], core_peer),
            remote(pieces[-1][1], last_in.at[1], o_send.at[1], o_recv.at[1], core_peer),
            remote(last_out, last_in.at[2], o_send.at[2], o_recv.at[2], x_peer)]
    last[0].start()
    last[1].start()

    def shares(blocks, part):
        count = part * heads
        stats = [block[count:count + 2 * heads, :] for block in blocks]
        top = functools.reduce(jnp.maximum, [st[:heads] for st in stats])
        grown = [jnp.exp(st[:heads] - top) for st in stats]
        return top, sum(st[heads:] * g for st, g in zip(stats, grown)), grown

    def mix(blocks, weights, owner, part, out):
        shift = lax.rem(128 - owner * part, 128)
        factors = [pltpu.roll(w, shift, 1) for w in weights]
        for b in range(part):
            at = slice(b * heads, (b + 1) * heads)
            out[at, :] = sum(block[at, :] * f[:, b:b + 1] for block, f in zip(blocks, factors))

    def combine(blocks, part, row0):
        _, total, grown = shares(blocks, part)
        mix(blocks, [g / total for g in grown], sp, part, osum)
        for h in range(heads):
            lhs[row0:row0 + part, h * 128:(h + 1) * 128] = osum[pl.ds(h, part, stride=heads), :].astype(jnp.bfloat16)

    for copy in local[0]:
        copy.wait()
    combine(pieces[0], parts[0], 0)

    last[0].wait_recv()
    pair = [pieces[-1][2], last_in.at[0]]
    top, total, grown = shares(pair, parts[-1])
    mix(pair, grown, x_id, parts[-1], last_out)
    count = parts[-1] * heads
    last_out[count:count + heads, :] = top
    last_out[count + heads:count + 2 * heads, :] = total
    last[2].start()

    sizes = (2, 2, 2, 2, 1)
    order = []
    for c, part in enumerate(parts):
        begin = 0
        for size in sizes:
            order.append((pl.ds(begin, size), pl.ds(sum(parts[:c]), part), range(begin, begin + size)))
            begin += size
    n_pieces = len(order)
    n_first = len(sizes)

    def to_y(t):
        ns, r, _ = order[t]
        return remote(y_out.at[ns, r], y_in.at[ns, r], y_send.at[t], y_recv.at[t], y_peer)

    def gather(t, owner, send, recv, peer):
        ns, r, _ = order[t]
        return remote(sums.at[owner, ns, r], sums.at[owner, ns, r], send.at[t], recv.at[t], peer)

    def to_x(t):
        return gather(t, sp, g_send, g_recv, x_peer)

    def to_core(t):
        return gather(t, sp, d_send, d_recv, core_peer)

    def relay(t):
        return gather(t, x_id, f_send, f_recv, core_peer)

    def keep(t, turn, owner):
        ns, r, _ = order[t]
        return pltpu.make_async_copy(sums.at[owner, ns, r], out_hbm.at[owner, ns, r], out_sem.at[turn, t])

    def project_rows(n, r0, count):
        y_out[n, r0:r0 + count, :] = jnp.dot(lhs[r0:r0 + count, :], wo[n], preferred_element_type=jnp.float32)

    for t in range(n_first):
        for n in order[t][2]:
            w_load(n).wait()
            if n + 2 < n_chunks:
                w_load(n + 2).start()
            project_rows(n, 0, parts[0])
        if t < 2:
            to_y(t).start()

    for t in range(n_pieces + 3):
        if t == 2:
            for copy in last[1:]:
                copy.wait_recv()
            combine([pieces[-1][0], last_in.at[1], last_in.at[2]], parts[-1], parts[0])
        if 2 <= t < 2 + n_first:
            for n in order[n_first + t - 2][2]:
                project_rows(n, parts[0], parts[-1])
        if t < n_pieces:
            ns, r, _ = order[t]
            to_y(t).wait()
            if t + 2 < n_pieces:
                to_y(t + 2).start()
            sums[sp, ns, r, :] = y_out[ns, r, :] + y_in[ns, r, :]
            to_x(t).start()
            to_core(t).start()
            keep(t, 0, sp).start()
        if 1 <= t < n_pieces + 1:
            to_x(t - 1).wait_recv()
            relay(t - 1).start()
            keep(t - 1, 1, x_id).start()
        if t >= 3:
            to_core(t - 3).wait_recv()
            keep(t - 3, 2, core_id).start()
            relay(t - 3).wait_recv()
            keep(t - 3, 3, far_id).start()
    for copy in last:
        copy.wait_send()
    for t in range(n_pieces):
        to_x(t).wait_send()
        to_core(t).wait_send()
        relay(t).wait_send()
        for turn in range(4):
            keep(t, turn, sp).wait()


def merge(chunks, pieces, w_o, n_chunks):
    inner, width = w_o.shape
    heads = inner // 128
    quarter = sum(chunks) // 4
    chunk = width // n_chunks
    hbm = pl.BlockSpec(memory_space=pltpu.HBM)
    f32 = jnp.float32
    dma = pltpu.SemaphoreType.DMA
    flat = [p for piece in pieces for p in piece]
    block = pieces[-1][0].shape
    return pl.pallas_call(
        functools.partial(merge_kernel, chunks),
        out_shape=pltpu.HBM((4, n_chunks, quarter, chunk), f32),
        in_specs=[hbm] * (len(flat) + 1),
        out_specs=hbm,
        scratch_shapes=[
            pltpu.VMEM((n_chunks, inner, chunk), jnp.bfloat16),
            pltpu.VMEM((3,) + block, f32),
            pltpu.VMEM(block, f32),
            pltpu.VMEM((max(chunks) // 4 * heads, 128), f32),
            pltpu.VMEM((quarter, inner), jnp.bfloat16),
            pltpu.VMEM((n_chunks, quarter, chunk), f32),
            pltpu.VMEM((n_chunks, quarter, chunk), f32),
            pltpu.VMEM((4, n_chunks, quarter, chunk), f32),
            dma((len(chunks), 4)), dma((n_chunks,)), dma((3,)), dma((3,)),
        ] + [dma((10,))] * 8 + [dma((4, 10))] + [pltpu.VMEM((4,) + piece[0].shape, f32) for piece in pieces],
        compiler_params=pltpu.CompilerParams(vmem_limit_bytes=56 * 1024 * 1024, collective_id=0, has_side_effects=True),
        cost_estimate=pl.CostEstimate(flops=2 * quarter * inner * width, bytes_accessed=2 * inner * width, transcendentals=0),
        name='merge',
    )(*flat, pltpu.with_memory_space_constraint(w_o, pltpu.HBM))


def finish_kernel(sums_ref, x_ref, wpost_ref, out_ref, gain_ref):
    _, n_chunks, rows, chunk = sums_ref.shape
    for j in range(wpost_ref.shape[0]):
        gain_ref[:, j * 128:(j + 1) * 128] = 1.0 + wpost_ref[j:j + 1, :]
    for k in range(rows // 16):
        at = slice(k * 16, (k + 1) * 16)
        square = jnp.zeros((16, chunk), jnp.float32)
        for n in range(n_chunks):
            u = sums_ref[0, n, at, :]
            square = square + u * u
        inv = lax.rsqrt(jnp.sum(square, axis=-1, keepdims=True) * (1.0 / (n_chunks * chunk)) + NORM_EPS)
        for n in range(n_chunks):
            col = slice(n * chunk, (n + 1) * chunk)
            y = x_ref[at, col].astype(jnp.float32) + sums_ref[0, n, at, :] * inv * gain_ref[:, col]
            out_ref[at, col] = y.astype(jnp.bfloat16)


def finish(sums, x_in, w_post):
    parts, n_chunks, quarter, chunk = sums.shape
    width = n_chunks * chunk
    return pl.pallas_call(
        finish_kernel,
        grid=(parts,),
        out_shape=jax.ShapeDtypeStruct(x_in.shape, x_in.dtype),
        in_specs=[pl.BlockSpec((1, n_chunks, quarter, chunk), lambda q: (q, 0, 0, 0)),
                  pl.BlockSpec((quarter, width), lambda q: (q, 0)),
                  pl.BlockSpec(w_post.shape, lambda q: (0, 0))],
        out_specs=pl.BlockSpec((quarter, width), lambda q: (q, 0)),
        scratch_shapes=[pltpu.VMEM((1, width), jnp.float32)],
        compiler_params=pltpu.CompilerParams(vmem_limit_bytes=62 * 1024 * 1024),
        name='finish',
    )(sums, x_in, w_post)


def solution(mesh):
    cache_spec = P('dp', 'sp', 'tp', None)
    sp_size = mesh.shape['sp']

    def local_step(x_in, cur_pos, w_pre, w_q, w_k, w_v, w_o, w_post, k_cache, v_cache):
        row_count, seq_block, kv_local, head_dim = k_cache.shape
        sp_index = lax.axis_index('sp')
        table = rotary_table(sp_size * seq_block, head_dim)
        q_rot, kn2, vn2 = project(cur_pos, x_in, w_pre.reshape(-1, 128), table, w_q, w_k, w_v)
        base = (sp_index * seq_block).astype(jnp.int32).reshape(1)
        kc = k_cache.reshape(row_count, seq_block * kv_local, head_dim)
        vc = v_cache.reshape(row_count, seq_block * kv_local, head_dim)
        chunks = (row_count // 2, row_count // 2)
        prev, first_row, pieces = None, 0, []
        for index, n_rows in enumerate(chunks):
            *prev, p0, p1, p2, p3 = attend(cur_pos, base, q_rot, kn2, vn2, kc, vc, prev, first_row, n_rows)
            first_row += n_rows // 4
            if index < len(chunks) - 1:
                moved = []
                for d, p in ((1, p1), (2, p2), (3, p3)):
                    moved.append(lax.ppermute(p, 'sp', [(i, i ^ d) for i in range(sp_size)]))
                p1, p2, p3 = moved
            pieces.append((p0, p1, p2, p3))
        k_out, v_out = prev
        x_out = finish(merge(chunks, pieces, w_o, 9), x_in, w_post.reshape(-1, 128))
        return x_out, k_out.reshape(k_cache.shape), v_out.reshape(v_cache.shape)

    return jax.shard_map(local_step, mesh=mesh,
                         in_specs=(P('dp', None), P('dp'), P(None), P(None, 'tp'), P(None, 'tp'), P(None, 'tp'), P('tp', None), P(None), cache_spec, cache_spec),
                         out_specs=(P('dp', None), cache_spec, cache_spec), check_vma=False)
```

```python
import functools

import jax
import jax.numpy as jnp
import numpy as np
from jax import lax
from jax.experimental import pallas as pl
from jax.experimental.pallas import tpu as pltpu
from jax.sharding import PartitionSpec as P


SOFT_CAP = 50.0
ROPE_BASE = 10000.0
NORM_EPS = 1e-6
LOG2E = 1.4426950408889634

ROWS_STEP = 8
SLOTS = 12
AHEAD = 6
START = 2
LAG_SOFT = 2
LAG_OUT = 4


def rotary_table(length, head_dim):
    half_dim = head_dim // 2
    inv_freq = np.power(np.float32(ROPE_BASE), -2.0 * np.arange(half_dim, dtype=np.float32) / np.float32(2 * half_dim)).astype(np.float32)
    angles = np.arange(length, dtype=np.float32)[:, None] * inv_freq[None, :]
    cos_tab = np.cos(angles.astype(np.float64))
    sin_tab = np.sin(angles.astype(np.float64))
    return np.concatenate([cos_tab, cos_tab, -sin_tab, sin_tab], axis=-1).astype(np.float32)


def project_kernel(pos_ref, x_hbm, wpre_ref, table_ref, wq_hbm, wk_hbm, wv_hbm, q_ref, k_ref, v_ref,
                   x_ref, gain_ref, cos_ref, sin_ref, weight, normed, q_part, k_part, v_part, x_sem, w_sem, send_sem, recv_sem,
                   out_sem):
    sp = lax.axis_index('sp')
    core = lax.rem(sp, 2)
    peer = {'sp': sp + 1 - 2 * core}
    mesh_id = pl.DeviceIdType.MESH
    rows = x_ref.shape[0]
    block = weight.shape[2]
    per = block // 128
    plan = []
    for w_hbm, part, turn in ((wq_hbm, q_part, True), (wk_hbm, k_part, True), (wv_hbm, v_part, False)):
        mine = w_hbm.shape[1] // 2
        for j in range(mine // block):
            plan.append((w_hbm, part, turn, mine, j, j == mine // block - 1))

    def load(i):
        w_hbm, _, _, mine, j, _ = plan[i]
        col = pl.multiple_of(core * mine + j * block, block)
        return pltpu.make_async_copy(w_hbm.at[:, pl.ds(col, block)], weight.at[i], w_sem.at[i])

    x_loads = [pltpu.make_async_copy(x_hbm.at[pl.ds(k * (rows // 4), rows // 4)], x_ref.at[pl.ds(k * (rows // 4), rows // 4)],
                                     x_sem.at[k]) for k in range(4)]
    for copy in x_loads:
        copy.start()
    load(0).start()
    barrier = pltpu.get_barrier_semaphore()
    pl.semaphore_signal(barrier, inc=1, device_id=peer, device_id_type=mesh_id)
    pl.semaphore_wait(barrier, 1)

    for j in range(wpre_ref.shape[0]):
        gain_ref[:, j * 128:(j + 1) * 128] = 1.0 + wpre_ref[j:j + 1, :]
    gain = gain_ref[...]

    def look_up(k, carry):
        for r in range(8):
            b = k * 8 + r
            row = table_ref[pl.ds(pos_ref[b], 1), :]
            cos_ref[pl.ds(b, 1), :] = row[:, :128]
            sin_ref[pl.ds(b, 1), :] = row[:, 128:]
        return carry

    lax.fori_loop(0, rows // 8, look_up, 0)

    def norm(k, carry):
        at = pl.ds(pl.multiple_of(k * 32, 32), 32)
        x = x_ref[at, :].astype(jnp.float32)
        inv = lax.rsqrt(jnp.mean(x * x, axis=-1, keepdims=True) + NORM_EPS)
        normed[at, :] = (x * inv * gain).astype(jnp.bfloat16)
        return carry

    for k in range(4):
        x_loads[k].wait()
        if k == 1:
            load(1).start()
        lax.fori_loop(k * rows // 128, (k + 1) * rows // 128, norm, 0)

    outs = ((q_part, q_ref), (k_part, k_ref), (v_part, v_ref))
    sends, writes = [], []
    for i, (_, part, turn, mine, j, done) in enumerate(plan):
        load(i).wait()
        if i + 2 < len(plan):
            load(i + 2).start()
        heads = mine // 128
        acc = jnp.dot(normed[...], weight[i], preferred_element_type=jnp.float32)
        for t in range(per):
            value = acc[:, t * 128:(t + 1) * 128]
            if turn:
                value = value * cos_ref[...] + pltpu.roll(value, 64, 1) * sin_ref[...]
            part[pl.ds(j * per + t, rows, stride=heads), :] = value
        if done:
            n = len(sends)
            copy = pltpu.make_async_remote_copy(src_ref=part, dst_ref=outs[n][1].at[core], send_sem=send_sem.at[n],
                                                recv_sem=recv_sem.at[n], device_id=peer, device_id_type=mesh_id)
            copy.start()
            sends.append(copy)
            out = pltpu.make_async_copy(part, outs[n][1].at[core], out_sem.at[n])
            out.start()
            writes.append(out)
    for copy in sends:
        copy.wait()
    for copy in writes:
        copy.wait()


def project(cur_pos, x_in, w_pre, table, w_q, w_k, w_v):
    rows, width = x_in.shape
    block = 512
    q_cols, kv_cols = w_q.shape[1], w_k.shape[1]
    n_blocks = (q_cols + 2 * kv_cols) // 2 // block
    vmem = pl.BlockSpec(memory_space=pltpu.VMEM)
    hbm = pl.BlockSpec(memory_space=pltpu.HBM)
    f32, bf = jnp.float32, jnp.bfloat16
    dma = pltpu.SemaphoreType.DMA
    return pl.pallas_call(
        project_kernel,
        out_shape=(pltpu.HBM((2, rows * q_cols // 256, 128), f32), pltpu.HBM((2, rows * kv_cols // 256, 128), f32),
                   pltpu.HBM((2, rows * kv_cols // 256, 128), f32)),
        in_specs=[pl.BlockSpec(memory_space=pltpu.SMEM), hbm, vmem, vmem] + [hbm] * 3,
        out_specs=(hbm,) * 3,
        scratch_shapes=[
            pltpu.VMEM((rows, width), bf),
            pltpu.VMEM((1, width), f32),
            pltpu.VMEM((rows, 128), f32),
            pltpu.VMEM((rows, 128), f32),
            pltpu.VMEM((n_blocks, width, block), bf),
            pltpu.VMEM((rows, width), bf),
            pltpu.VMEM((rows * q_cols // 256, 128), f32),
            pltpu.VMEM((rows * kv_cols // 256, 128), f32),
            pltpu.VMEM((rows * kv_cols // 256, 128), f32),
            dma((4,)), dma((n_blocks,)), dma((3,)), dma((3,)), dma((3,)),
        ],
        compiler_params=pltpu.CompilerParams(vmem_limit_bytes=62 * 1024 * 1024, collective_id=1, has_side_effects=True),
        cost_estimate=pl.CostEstimate(flops=rows * width * (q_cols + 2 * kv_cols), bytes_accessed=width * (q_cols + 2 * kv_cols), transcendentals=0),
        name='project',
    )(cur_pos, x_in, w_pre, table, w_q, w_k, w_v)


def attend_kernel(n_steps, quarter, first_row, kv_heads, seq_block, pos_ref, base_ref, q_hbm, kn_hbm, vn_hbm, k_hbm, v_hbm,
                  *rest):
    (ko_hbm, vo_hbm, o0_hbm, o1_hbm, o2_hbm, o3_hbm, m_ref, l_ref, kbuf, vbuf, qbuf, knbuf, vnbuf, obuf, key_ref, s_ref, p_ref, in_sem, out_sem, o_sem, st_sem) = rest[-21:]
    step_rows = ROWS_STEP
    piece_steps = n_steps // 4
    heads, head_dim = m_ref.shape
    q_half, kv_half = heads // 2, kv_heads // 2
    cols = seq_block * kv_heads
    base = base_ref[0]

    row_id = lax.broadcasted_iota(jnp.int32, (heads, cols), 0)
    col_id = lax.broadcasted_iota(jnp.int32, (heads, cols), 1)
    mine = lax.rem(col_id, kv_heads) == row_id // (heads // kv_heads)
    key_ref[...] = jnp.where(mine, col_id, cols * 4)
    lane_id = lax.broadcasted_iota(jnp.int32, m_ref.shape, 1)
    half_id = lax.broadcasted_iota(jnp.int32, (2 * kv_heads, head_dim), 0) // kv_heads

    def row_of(step):
        piece = step // piece_steps
        return piece * quarter + first_row + (step - piece * piece_steps) * step_rows

    def heads_of(step, count):
        return pl.ds(row_of(step) * count, step_rows * count)

    def both_halves(ref, slot, r, count):
        at = slice(r * count, (r + 1) * count)
        return [ref[slot, 0, at, :], ref[slot, 1, at, :]]

    def loads(step, slot):
        rows = pl.ds(row_of(step), step_rows)
        return (pltpu.make_async_copy(k_hbm.at[rows], kbuf.at[slot], in_sem.at[slot, 0]),
                pltpu.make_async_copy(v_hbm.at[rows], vbuf.at[slot], in_sem.at[slot, 1]),
                pltpu.make_async_copy(q_hbm.at[:, heads_of(step, q_half)], qbuf.at[slot], in_sem.at[slot, 2]),
                pltpu.make_async_copy(kn_hbm.at[:, heads_of(step, kv_half)], knbuf.at[slot], in_sem.at[slot, 3]),
                pltpu.make_async_copy(vn_hbm.at[:, heads_of(step, kv_half)], vnbuf.at[slot], in_sem.at[slot, 4]))

    def stores(step, slot):
        rows = pl.ds(row_of(step), step_rows)
        return (pltpu.make_async_copy(kbuf.at[slot], ko_hbm.at[rows], out_sem.at[slot, 0]),
                pltpu.make_async_copy(vbuf.at[slot], vo_hbm.at[rows], out_sem.at[slot, 1]))

    def o_store(step, slot, d=0):
        at = pl.ds((step - step // piece_steps * piece_steps) * step_rows * heads, step_rows * heads)
        o_hbm = (o0_hbm, o1_hbm, o2_hbm, o3_hbm)[d]
        return pltpu.make_async_copy(obuf.at[slot], o_hbm.at[at], o_sem.at[slot])

    def o_start(step, slot):
        turn = jnp.bitwise_xor(step // piece_steps, base // seq_block)
        for d in range(4):
            @pl.when(turn == d)
            def _():
                o_store(step, slot, d).start()

    for step in range(min(START, n_steps)):
        for copy in loads(step, step):
            copy.start()
    m_ref[...] = jnp.zeros_like(m_ref)
    l_ref[...] = jnp.zeros_like(l_ref)
    scale = head_dim ** -0.5 / SOFT_CAP

    def body(step, carry):
        slot = lax.rem(step, SLOTS)
        oslot = lax.rem(step, 2)
        for copy in loads(step, slot):
            copy.wait()
        issued = jnp.minimum(step + AHEAD, START + 2 * step)
        wanted = jnp.minimum(jnp.minimum(step + 1 + AHEAD, START + 2 * step + 2), n_steps)
        for extra in range(2):
            nxt = issued + extra

            @pl.when(nxt < wanted)
            def _():
                nslot = lax.rem(nxt, SLOTS)

                @pl.when(nxt >= SLOTS)
                def _():
                    for copy in stores(nxt - SLOTS, nslot):
                        copy.wait()

                for copy in loads(nxt, nslot):
                    copy.start()

        for r in range(step_rows):
            local = pos_ref[row_of(step) + r] - base
            inside = (local >= 0) & (local < seq_block)
            at = jnp.clip(local, 0, seq_block - 1)
            pair = pl.ds(pl.multiple_of((at // 2) * (2 * kv_heads), 2 * kv_heads), 2 * kv_heads)
            hit = half_id == jnp.where(inside, lax.rem(at, 2), 2)
            k_row = jnp.concatenate(both_halves(knbuf, slot, r, kv_half) * 2, axis=0).astype(jnp.bfloat16)
            v_row = jnp.concatenate(both_halves(vnbuf, slot, r, kv_half) * 2, axis=0).astype(jnp.bfloat16)
            kbuf[slot, r, pair, :] = jnp.where(hit, k_row, kbuf[slot, r, pair, :])
            vbuf[slot, r, pair, :] = jnp.where(hit, v_row, vbuf[slot, r, pair, :])

        @pl.when(step >= 2)
        def _():
            o_store(step - 2, oslot).wait()

        m_all = m_ref[...]
        l_all = l_ref[...]
        half = cols // 2
        for tick in range(step_rows + LAG_OUT):
            r = tick
            if r < step_rows:
                q_row = jnp.concatenate(both_halves(qbuf, slot, r, q_half), axis=0).astype(jnp.bfloat16)
                raw = lax.dot_general(q_row, kbuf[slot, r], (((1,), (1,)), ((), ())),
                                      preferred_element_type=jnp.float32)
                s_ref[r] = raw
            r = tick - LAG_SOFT
            if 0 <= r < step_rows:
                local = pos_ref[row_of(step) + r] - base
                seen = key_ref[...] < (local + 1) * kv_heads
                soft = jnp.where(seen, jnp.tanh(s_ref[r] * scale), -4.0)
                top = jnp.maximum(jnp.max(soft, axis=-1, keepdims=True), -1.0)
                weight = jnp.exp2((soft - top) * (SOFT_CAP * LOG2E))
                total = jnp.sum(weight, axis=-1, keepdims=True)
                weight = weight.astype(jnp.bfloat16)
                p_ref[r, :heads] = weight[:, :half]
                p_ref[r, heads:] = weight[:, half:]
                here = lane_id == step * step_rows + r
                m_all = jnp.where(here, top * SOFT_CAP, m_all)
                l_all = jnp.where(here, total, l_all)
            r = tick - LAG_OUT
            if 0 <= r < step_rows:
                right = jnp.concatenate([vbuf[slot, r, :half, :], vbuf[slot, r, half:, :]], axis=1)
                both = jnp.dot(p_ref[r], right, preferred_element_type=jnp.float32)
                obuf[oslot, r * heads:(r + 1) * heads, :] = both[:heads, :head_dim] + both[heads:, head_dim:]
        m_ref[...] = m_all
        l_ref[...] = l_all
        o_start(step, oslot)
        for copy in stores(step, slot):
            copy.start()

        return carry

    lax.fori_loop(0, n_steps, body, 0)
    tail = piece_steps * step_rows * heads
    stat_copies = []
    for d, o_hbm in enumerate((o0_hbm, o1_hbm, o2_hbm, o3_hbm)):
        stat_copies.append(pltpu.make_async_copy(m_ref, o_hbm.at[pl.ds(tail, heads)], st_sem.at[d, 0]))
        stat_copies.append(pltpu.make_async_copy(l_ref, o_hbm.at[pl.ds(tail + heads, heads)], st_sem.at[d, 1]))
    for copy in stat_copies:
        copy.start()
    for copy in stat_copies:
        copy.wait()
    for step in range(max(0, n_steps - SLOTS), n_steps):
        for copy in stores(step, step % SLOTS):
            copy.wait()
    for step in range(max(0, n_steps - 2), n_steps):
        o_store(step, step % 2).wait()


def attend(pos, base, q, kn, vn, k_cache, v_cache, prev, first_row, n_rows):
    rows, cols, head_dim = k_cache.shape
    heads = 2 * q.shape[1] // rows
    kv_heads = 2 * kn.shape[1] // rows
    seq_block = cols // kv_heads
    n_steps = n_rows // ROWS_STEP
    hbm = pl.BlockSpec(memory_space=pl.ANY)
    piece = pltpu.HBM((n_rows // 4 * heads + 2 * heads, head_dim), jnp.float32)
    smem = pl.BlockSpec(memory_space=pltpu.SMEM)
    bf = jnp.bfloat16
    aliases = {} if prev is None else {7: 0, 8: 1}
    extra = () if prev is None else tuple(prev)
    return pl.pallas_call(
        functools.partial(attend_kernel, n_steps, rows // 4, first_row, kv_heads, seq_block),
        out_shape=(jax.ShapeDtypeStruct(k_cache.shape, bf), jax.ShapeDtypeStruct(v_cache.shape, bf)) + (piece,) * 4,
        in_specs=[smem, smem, hbm, hbm, hbm, hbm, hbm] + [hbm] * len(extra),
        out_specs=(hbm, hbm) + (pl.BlockSpec(memory_space=pltpu.HBM),) * 4,
        scratch_shapes=[
            pltpu.VMEM((heads, 128), jnp.float32),
            pltpu.VMEM((heads, 128), jnp.float32),
            pltpu.VMEM((SLOTS, ROWS_STEP, cols, head_dim), bf),
            pltpu.VMEM((SLOTS, ROWS_STEP, cols, head_dim), bf),
            pltpu.VMEM((SLOTS, 2, ROWS_STEP * heads // 2, head_dim), jnp.float32),
            pltpu.VMEM((SLOTS, 2, ROWS_STEP * kv_heads // 2, head_dim), jnp.float32),
            pltpu.VMEM((SLOTS, 2, ROWS_STEP * kv_heads // 2, head_dim), jnp.float32),
            pltpu.VMEM((2, ROWS_STEP * heads, head_dim), jnp.float32),
            pltpu.VMEM((heads, cols), jnp.int32),
            pltpu.VMEM((ROWS_STEP, heads, cols), jnp.float32),
            pltpu.VMEM((ROWS_STEP, 2 * heads, cols // 2), bf),
            pltpu.SemaphoreType.DMA((SLOTS, 5)),
            pltpu.SemaphoreType.DMA((SLOTS, 2)),
            pltpu.SemaphoreType.DMA((2,)),
            pltpu.SemaphoreType.DMA((4, 2)),
        ],
        input_output_aliases=aliases,
        compiler_params=pltpu.CompilerParams(vmem_limit_bytes=62 * 1024 * 1024),
        cost_estimate=pl.CostEstimate(flops=n_rows * heads * cols * head_dim * 4,
                                      bytes_accessed=n_rows * cols * head_dim * 8, transcendentals=0),
        name='attend',
    )(pos, base, q, kn, vn, k_cache, v_cache, *extra)


def merge_kernel(chunks, *refs):
    n_in = 4 * len(chunks)
    source = [refs[4 * c:4 * c + 4] for c in range(len(chunks))]
    pieces = [[b.at[d] for d in range(4)] for b in refs[-len(chunks):]]
    refs = refs[:-len(chunks)]
    (wo_hbm, out_hbm, wo, last_in, last_out, osum, lhs, y_out, y_in, sums,
     p_sem, w_sem, o_send, o_recv, y_send, y_recv, g_send, g_recv, d_send, d_recv, f_send, f_recv, out_sem) = refs[n_in:]
    sp = lax.axis_index('sp')
    tp = lax.axis_index('tp')
    core = lax.rem(sp, 2)
    xpos = sp // 2
    n_chunks, _, chunk = y_out.shape
    heads = lhs.shape[1] // 128
    parts = [c // 4 for c in chunks]
    core_id = 2 * xpos + (1 - core)
    x_id = 2 * (1 - xpos) + core
    far_id = 2 * (1 - xpos) + (1 - core)
    core_peer, x_peer, y_peer = {'sp': core_id}, {'sp': x_id}, {'tp': 1 - tp}
    mesh_id = pl.DeviceIdType.MESH

    def remote(src, dst, send, recv, peer):
        return pltpu.make_async_remote_copy(src_ref=src, dst_ref=dst, send_sem=send, recv_sem=recv,
                                            device_id=peer, device_id_type=mesh_id)

    def w_load(n):
        return pltpu.make_async_copy(wo_hbm.at[:, pl.ds(n * chunk, chunk)], wo.at[n], w_sem.at[n])

    local = [[pltpu.make_async_copy(source[c][d], pieces[c][d], p_sem.at[c, d]) for d in range(4)] for c in range(len(chunks))]
    for group in (local[-1], local[0]):
        for copy in group:
            copy.start()
    for n in range(2):
        w_load(n).start()
    barrier = pltpu.get_barrier_semaphore()
    for peer in (core_peer, x_peer, y_peer):
        pl.semaphore_signal(barrier, inc=1, device_id=peer, device_id_type=mesh_id)
    pl.semaphore_wait(barrier, 3)

    for copy in local[-1]:
        copy.wait()
    last = [remote(pieces[-1][3], last_in.at[0], o_send.at[0], o_recv.at[0], core_peer),
            remote(pieces[-1][1], last_in.at[1], o_send.at[1], o_recv.at[1], core_peer),
            remote(last_out, last_in.at[2], o_send.at[2], o_recv.at[2], x_peer)]
    last[0].start()
    last[1].start()

    def shares(blocks, part):
        count = part * heads
        stats = [block[count:count + 2 * heads, :] for block in blocks]
        top = functools.reduce(jnp.maximum, [st[:heads] for st in stats])
        grown = [jnp.exp(st[:heads] - top) for st in stats]
        return top, sum(st[heads:] * g for st, g in zip(stats, grown)), grown

    def mix(blocks, weights, owner, part, out):
        shift = lax.rem(128 - owner * part, 128)
        factors = [pltpu.roll(w, shift, 1) for w in weights]
        for b in range(part):
            at = slice(b * heads, (b + 1) * heads)
            out[at, :] = sum(block[at, :] * f[:, b:b + 1] for block, f in zip(blocks, factors))

    def combine(blocks, part, row0):
        _, total, grown = shares(blocks, part)
        mix(blocks, [g / total for g in grown], sp, part, osum)
        for h in range(heads):
            lhs[row0:row0 + part, h * 128:(h + 1) * 128] = osum[pl.ds(h, part, stride=heads), :].astype(jnp.bfloat16)

    last[0].wait_recv()
    pair = [pieces[-1][2], last_in.at[0]]
    top, total, grown = shares(pair, parts[-1])
    mix(pair, grown, x_id, parts[-1], last_out)
    count = parts[-1] * heads
    last_out[count:count + heads, :] = top
    last_out[count + heads:count + 2 * heads, :] = total
    last[2].start()

    for copy in local[0]:
        copy.wait()
    combine(pieces[0], parts[0], 0)

    sizes = (2, 2, 2, 2, 1)
    order = []
    for c, part in enumerate(parts):
        begin = 0
        for size in sizes:
            order.append((pl.ds(begin, size), pl.ds(sum(parts[:c]), part), range(begin, begin + size)))
            begin += size
    n_pieces = len(order)
    n_first = len(sizes)

    def to_y(t):
        ns, r, _ = order[t]
        return remote(y_out.at[ns, r], y_in.at[ns, r], y_send.at[t], y_recv.at[t], y_peer)

    def gather(t, owner, send, recv, peer):
        ns, r, _ = order[t]
        return remote(sums.at[owner, ns, r], sums.at[owner, ns, r], send.at[t], recv.at[t], peer)

    def to_x(t):
        return gather(t, sp, g_send, g_recv, x_peer)

    def to_core(t):
        return gather(t, sp, d_send, d_recv, core_peer)

    def relay(t):
        return gather(t, x_id, f_send, f_recv, core_peer)

    def keep(t, turn, owner):
        ns, r, _ = order[t]
        return pltpu.make_async_copy(sums.at[owner, ns, r], out_hbm.at[owner, ns, r], out_sem.at[turn, t])

    def project_rows(n, r0, count):
        y_out[n, r0:r0 + count, :] = jnp.dot(lhs[r0:r0 + count, :], wo[n], preferred_element_type=jnp.float32)

    for t in range(n_first):
        for n in order[t][2]:
            w_load(n).wait()
            if n + 2 < n_chunks:
                w_load(n + 2).start()
            project_rows(n, 0, parts[0])
        to_y(t).start()

    for t in range(n_pieces + 3):
        if t == 2:
            for copy in last[1:]:
                copy.wait_recv()
            combine([pieces[-1][0], last_in.at[1], last_in.at[2]], parts[-1], parts[0])
        if 2 <= t < 2 + n_first:
            for n in order[n_first + t - 2][2]:
                project_rows(n, parts[0], parts[-1])
            to_y(n_first + t - 2).start()
        if t < n_pieces:
            ns, r, _ = order[t]
            to_y(t).wait()
            sums[sp, ns, r, :] = y_out[ns, r, :] + y_in[ns, r, :]
            to_x(t).start()
            to_core(t).start()
            keep(t, 0, sp).start()
        if 1 <= t < n_pieces + 1:
            to_x(t - 1).wait_recv()
            relay(t - 1).start()
            keep(t - 1, 1, x_id).start()
        if t >= 3:
            to_core(t - 3).wait_recv()
            keep(t - 3, 2, core_id).start()
            relay(t - 3).wait_recv()
            keep(t - 3, 3, far_id).start()
    for copy in last:
        copy.wait_send()
    for t in range(n_pieces):
        to_x(t).wait_send()
        to_core(t).wait_send()
        relay(t).wait_send()
        for turn in range(4):
            keep(t, turn, sp).wait()


def merge(chunks, pieces, w_o, n_chunks):
    inner, width = w_o.shape
    heads = inner // 128
    quarter = sum(chunks) // 4
    chunk = width // n_chunks
    hbm = pl.BlockSpec(memory_space=pltpu.HBM)
    f32 = jnp.float32
    dma = pltpu.SemaphoreType.DMA
    flat = [p for piece in pieces for p in piece]
    block = pieces[-1][0].shape
    return pl.pallas_call(
        functools.partial(merge_kernel, chunks),
        out_shape=pltpu.HBM((4, n_chunks, quarter, chunk), f32),
        in_specs=[hbm] * (len(flat) + 1),
        out_specs=hbm,
        scratch_shapes=[
            pltpu.VMEM((n_chunks, inner, chunk), jnp.bfloat16),
            pltpu.VMEM((3,) + block, f32),
            pltpu.VMEM(block, f32),
            pltpu.VMEM((max(chunks) // 4 * heads, 128), f32),
            pltpu.VMEM((quarter, inner), jnp.bfloat16),
            pltpu.VMEM((n_chunks, quarter, chunk), f32),
            pltpu.VMEM((n_chunks, quarter, chunk), f32),
            pltpu.VMEM((4, n_chunks, quarter, chunk), f32),
            dma((len(chunks), 4)), dma((n_chunks,)), dma((3,)), dma((3,)),
        ] + [dma((10,))] * 8 + [dma((4, 10))] + [pltpu.VMEM((4,) + piece[0].shape, f32) for piece in pieces],
        compiler_params=pltpu.CompilerParams(vmem_limit_bytes=56 * 1024 * 1024, collective_id=0, has_side_effects=True),
        cost_estimate=pl.CostEstimate(flops=2 * quarter * inner * width, bytes_accessed=2 * inner * width, transcendentals=0),
        name='merge',
    )(*flat, pltpu.with_memory_space_constraint(w_o, pltpu.HBM))


def finish_kernel(sums_ref, x_ref, wpost_ref, out_ref, gain_ref):
    _, n_chunks, rows, chunk = sums_ref.shape
    for j in range(wpost_ref.shape[0]):
        gain_ref[:, j * 128:(j + 1) * 128] = 1.0 + wpost_ref[j:j + 1, :]
    for k in range(rows // 16):
        at = slice(k * 16, (k + 1) * 16)
        square = jnp.zeros((16, chunk), jnp.float32)
        for n in range(n_chunks):
            u = sums_ref[0, n, at, :]
            square = square + u * u
        inv = lax.rsqrt(jnp.sum(square, axis=-1, keepdims=True) * (1.0 / (n_chunks * chunk)) + NORM_EPS)
        for n in range(n_chunks):
            col = slice(n * chunk, (n + 1) * chunk)
            y = x_ref[at, col].astype(jnp.float32) + sums_ref[0, n, at, :] * inv * gain_ref[:, col]
            out_ref[at, col] = y.astype(jnp.bfloat16)


def finish(sums, x_in, w_post):
    parts, n_chunks, quarter, chunk = sums.shape
    width = n_chunks * chunk
    return pl.pallas_call(
        finish_kernel,
        grid=(parts, 2),
        out_shape=jax.ShapeDtypeStruct(x_in.shape, x_in.dtype),
        in_specs=[pl.BlockSpec((1, n_chunks, quarter // 2, chunk), lambda q, k: (q, 0, k, 0)),
                  pl.BlockSpec((quarter // 2, width), lambda q, k: (2 * q + k, 0)),
                  pl.BlockSpec(w_post.shape, lambda q, k: (0, 0))],
        out_specs=pl.BlockSpec((quarter // 2, width), lambda q, k: (2 * q + k, 0)),
        scratch_shapes=[pltpu.VMEM((1, width), jnp.float32)],
        compiler_params=pltpu.CompilerParams(vmem_limit_bytes=62 * 1024 * 1024),
        name='finish',
    )(sums, x_in, w_post)


def solution(mesh):
    cache_spec = P('dp', 'sp', 'tp', None)
    sp_size = mesh.shape['sp']

    def local_step(x_in, cur_pos, w_pre, w_q, w_k, w_v, w_o, w_post, k_cache, v_cache):
        row_count, seq_block, kv_local, head_dim = k_cache.shape
        sp_index = lax.axis_index('sp')
        table = rotary_table(sp_size * seq_block, head_dim)
        q_rot, kn2, vn2 = project(cur_pos, x_in, w_pre.reshape(-1, 128), table, w_q, w_k, w_v)
        base = (sp_index * seq_block).astype(jnp.int32).reshape(1)
        kc = k_cache.reshape(row_count, seq_block * kv_local, head_dim)
        vc = v_cache.reshape(row_count, seq_block * kv_local, head_dim)
        chunks = (row_count // 2, row_count // 2)
        prev, first_row, pieces = None, 0, []
        for index, n_rows in enumerate(chunks):
            *prev, p0, p1, p2, p3 = attend(cur_pos, base, q_rot, kn2, vn2, kc, vc, prev, first_row, n_rows)
            first_row += n_rows // 4
            if index < len(chunks) - 1:
                moved = []
                for d, p in ((1, p1), (2, p2), (3, p3)):
                    moved.append(lax.ppermute(p, 'sp', [(i, i ^ d) for i in range(sp_size)]))
                p1, p2, p3 = moved
            pieces.append((p0, p1, p2, p3))
        k_out, v_out = prev
        x_out = finish(merge(chunks, pieces, w_o, 9), x_in, w_post.reshape(-1, 128))
        return x_out, k_out.reshape(k_cache.shape), v_out.reshape(v_cache.shape)

    return jax.shard_map(local_step, mesh=mesh,
                         in_specs=(P('dp', None), P('dp'), P(None), P(None, 'tp'), P(None, 'tp'), P(None, 'tp'), P('tp', None), P(None), cache_spec, cache_spec),
                         out_specs=(P('dp', None), cache_spec, cache_spec), check_vma=False)
```

```python
import functools

import jax
import jax.numpy as jnp
import numpy as np
from jax import lax
from jax.experimental import pallas as pl
from jax.experimental.pallas import tpu as pltpu
from jax.sharding import PartitionSpec as P


SOFT_CAP = 50.0
ROPE_BASE = 10000.0
NORM_EPS = 1e-6
LOG2E = 1.4426950408889634

ROWS_STEP = 8
SLOTS = 12
AHEAD = 6
START = 2
LAG_SOFT = 2
LAG_OUT = 4


def rotary_table(length, head_dim):
    half_dim = head_dim // 2
    inv_freq = np.power(np.float32(ROPE_BASE), -2.0 * np.arange(half_dim, dtype=np.float32) / np.float32(2 * half_dim)).astype(np.float32)
    angles = np.arange(length, dtype=np.float32)[:, None] * inv_freq[None, :]
    cos_tab = np.cos(angles.astype(np.float64))
    sin_tab = np.sin(angles.astype(np.float64))
    return np.concatenate([cos_tab, cos_tab, -sin_tab, sin_tab], axis=-1).astype(np.float32)


def project_kernel(pos_ref, x_hbm, wpre_ref, table_ref, wq_hbm, wk_hbm, wv_hbm, q_ref, k_ref, v_ref,
                   x_ref, gain_ref, cos_ref, sin_ref, weight, normed, q_part, k_part, v_part, x_sem, w_sem, send_sem, recv_sem,
                   out_sem):
    sp = lax.axis_index('sp')
    core = lax.rem(sp, 2)
    peer = {'sp': sp + 1 - 2 * core}
    mesh_id = pl.DeviceIdType.MESH
    rows = x_ref.shape[0]
    block = weight.shape[2]
    per = block // 128
    plan = []
    for w_hbm, part, turn in ((wq_hbm, q_part, True), (wk_hbm, k_part, True), (wv_hbm, v_part, False)):
        mine = w_hbm.shape[1] // 2
        for j in range(mine // block):
            plan.append((w_hbm, part, turn, mine, j, j == mine // block - 1))

    def load(i):
        w_hbm, _, _, mine, j, _ = plan[i]
        col = pl.multiple_of(core * mine + j * block, block)
        return pltpu.make_async_copy(w_hbm.at[:, pl.ds(col, block)], weight.at[i], w_sem.at[i])

    x_loads = [pltpu.make_async_copy(x_hbm.at[pl.ds(k * (rows // 4), rows // 4)], x_ref.at[pl.ds(k * (rows // 4), rows // 4)],
                                     x_sem.at[k]) for k in range(4)]
    for copy in x_loads:
        copy.start()
    load(0).start()
    barrier = pltpu.get_barrier_semaphore()
    pl.semaphore_signal(barrier, inc=1, device_id=peer, device_id_type=mesh_id)
    pl.semaphore_wait(barrier, 1)

    for j in range(wpre_ref.shape[0]):
        gain_ref[:, j * 128:(j + 1) * 128] = 1.0 + wpre_ref[j:j + 1, :]
    gain = gain_ref[...]

    def look_up(k, carry):
        for r in range(8):
            b = k * 8 + r
            row = table_ref[pl.ds(pos_ref[b], 1), :]
            cos_ref[pl.ds(b, 1), :] = row[:, :128]
            sin_ref[pl.ds(b, 1), :] = row[:, 128:]
        return carry

    lax.fori_loop(0, rows // 8, look_up, 0)

    def norm(k, carry):
        at = pl.ds(pl.multiple_of(k * 32, 32), 32)
        x = x_ref[at, :].astype(jnp.float32)
        inv = lax.rsqrt(jnp.mean(x * x, axis=-1, keepdims=True) + NORM_EPS)
        normed[at, :] = (x * inv * gain).astype(jnp.bfloat16)
        return carry

    for k in range(4):
        x_loads[k].wait()
        if k == 1:
            load(1).start()
        lax.fori_loop(k * rows // 128, (k + 1) * rows // 128, norm, 0)

    outs = ((q_part, q_ref), (k_part, k_ref), (v_part, v_ref))
    sends, writes = [], []
    for i, (_, part, turn, mine, j, done) in enumerate(plan):
        load(i).wait()
        if i + 2 < len(plan):
            load(i + 2).start()
        heads = mine // 128
        acc = jnp.dot(normed[...], weight[i], preferred_element_type=jnp.float32)
        for t in range(per):
            value = acc[:, t * 128:(t + 1) * 128]
            if turn:
                value = value * cos_ref[...] + pltpu.roll(value, 64, 1) * sin_ref[...]
            part[pl.ds(j * per + t, rows, stride=heads), :] = value
        if done:
            n = len(sends)
            copy = pltpu.make_async_remote_copy(src_ref=part, dst_ref=outs[n][1].at[core], send_sem=send_sem.at[n],
                                                recv_sem=recv_sem.at[n], device_id=peer, device_id_type=mesh_id)
            copy.start()
            sends.append(copy)
            out = pltpu.make_async_copy(part, outs[n][1].at[core], out_sem.at[n])
            out.start()
            writes.append(out)
    for copy in sends:
        copy.wait()
    for copy in writes:
        copy.wait()


def project(cur_pos, x_in, w_pre, table, w_q, w_k, w_v):
    rows, width = x_in.shape
    block = 512
    q_cols, kv_cols = w_q.shape[1], w_k.shape[1]
    n_blocks = (q_cols + 2 * kv_cols) // 2 // block
    vmem = pl.BlockSpec(memory_space=pltpu.VMEM)
    hbm = pl.BlockSpec(memory_space=pltpu.HBM)
    f32, bf = jnp.float32, jnp.bfloat16
    dma = pltpu.SemaphoreType.DMA
    return pl.pallas_call(
        project_kernel,
        out_shape=(pltpu.HBM((2, rows * q_cols // 256, 128), f32), pltpu.HBM((2, rows * kv_cols // 256, 128), f32),
                   pltpu.HBM((2, rows * kv_cols // 256, 128), f32)),
        in_specs=[pl.BlockSpec(memory_space=pltpu.SMEM), hbm, vmem, vmem] + [hbm] * 3,
        out_specs=(hbm,) * 3,
        scratch_shapes=[
            pltpu.VMEM((rows, width), bf),
            pltpu.VMEM((1, width), f32),
            pltpu.VMEM((rows, 128), f32),
            pltpu.VMEM((rows, 128), f32),
            pltpu.VMEM((n_blocks, width, block), bf),
            pltpu.VMEM((rows, width), bf),
            pltpu.VMEM((rows * q_cols // 256, 128), f32),
            pltpu.VMEM((rows * kv_cols // 256, 128), f32),
            pltpu.VMEM((rows * kv_cols // 256, 128), f32),
            dma((4,)), dma((n_blocks,)), dma((3,)), dma((3,)), dma((3,)),
        ],
        compiler_params=pltpu.CompilerParams(vmem_limit_bytes=62 * 1024 * 1024, collective_id=1, has_side_effects=True),
        cost_estimate=pl.CostEstimate(flops=rows * width * (q_cols + 2 * kv_cols), bytes_accessed=width * (q_cols + 2 * kv_cols), transcendentals=0),
        name='project',
    )(cur_pos, x_in, w_pre, table, w_q, w_k, w_v)


def attend_kernel(n_steps, quarter, first_row, kv_heads, seq_block, pos_ref, base_ref, q_hbm, kn_hbm, vn_hbm, k_hbm, v_hbm,
                  *rest):
    (ko_hbm, vo_hbm, o0_hbm, o1_hbm, o2_hbm, o3_hbm, m_ref, l_ref, kbuf, vbuf, qbuf, knbuf, vnbuf, obuf, key_ref, s_ref, p_ref, in_sem, out_sem, o_sem, st_sem) = rest[-21:]
    step_rows = ROWS_STEP
    piece_steps = n_steps // 4
    heads, head_dim = m_ref.shape
    q_half, kv_half = heads // 2, kv_heads // 2
    cols = seq_block * kv_heads
    base = base_ref[0]

    row_id = lax.broadcasted_iota(jnp.int32, (heads, cols), 0)
    col_id = lax.broadcasted_iota(jnp.int32, (heads, cols), 1)
    mine = lax.rem(col_id, kv_heads) == row_id // (heads // kv_heads)
    key_ref[...] = jnp.where(mine, col_id, cols * 4)
    lane_id = lax.broadcasted_iota(jnp.int32, m_ref.shape, 1)
    half_id = lax.broadcasted_iota(jnp.int32, (2 * kv_heads, head_dim), 0) // kv_heads

    def row_of(step):
        piece = step // piece_steps
        return piece * quarter + first_row + (step - piece * piece_steps) * step_rows

    def heads_of(step, count):
        return pl.ds(row_of(step) * count, step_rows * count)

    def both_halves(ref, slot, r, count):
        at = slice(r * count, (r + 1) * count)
        return [ref[slot, 0, at, :], ref[slot, 1, at, :]]

    def loads(step, slot):
        rows = pl.ds(row_of(step), step_rows)
        return (pltpu.make_async_copy(k_hbm.at[rows], kbuf.at[slot], in_sem.at[slot, 0]),
                pltpu.make_async_copy(v_hbm.at[rows], vbuf.at[slot], in_sem.at[slot, 1]),
                pltpu.make_async_copy(q_hbm.at[:, heads_of(step, q_half)], qbuf.at[slot], in_sem.at[slot, 2]),
                pltpu.make_async_copy(kn_hbm.at[:, heads_of(step, kv_half)], knbuf.at[slot], in_sem.at[slot, 3]),
                pltpu.make_async_copy(vn_hbm.at[:, heads_of(step, kv_half)], vnbuf.at[slot], in_sem.at[slot, 4]))

    def stores(step, slot):
        rows = pl.ds(row_of(step), step_rows)
        return (pltpu.make_async_copy(kbuf.at[slot], ko_hbm.at[rows], out_sem.at[slot, 0]),
                pltpu.make_async_copy(vbuf.at[slot], vo_hbm.at[rows], out_sem.at[slot, 1]))

    def o_store(step, slot, d=0):
        at = pl.ds((step - step // piece_steps * piece_steps) * step_rows * heads, step_rows * heads)
        o_hbm = (o0_hbm, o1_hbm, o2_hbm, o3_hbm)[d]
        return pltpu.make_async_copy(obuf.at[slot], o_hbm.at[at], o_sem.at[slot])

    def o_start(step, slot):
        turn = jnp.bitwise_xor(step // piece_steps, base // seq_block)
        for d in range(4):
            @pl.when(turn == d)
            def _():
                o_store(step, slot, d).start()

    for step in range(min(START, n_steps)):
        for copy in loads(step, step):
            copy.start()
    m_ref[...] = jnp.zeros_like(m_ref)
    l_ref[...] = jnp.zeros_like(l_ref)
    scale = head_dim ** -0.5 / SOFT_CAP

    def body(step, carry):
        slot = lax.rem(step, SLOTS)
        oslot = lax.rem(step, 2)
        for copy in loads(step, slot):
            copy.wait()
        issued = jnp.minimum(step + AHEAD, START + 2 * step)
        wanted = jnp.minimum(jnp.minimum(step + 1 + AHEAD, START + 2 * step + 2), n_steps)
        for extra in range(2):
            nxt = issued + extra

            @pl.when(nxt < wanted)
            def _():
                nslot = lax.rem(nxt, SLOTS)

                @pl.when(nxt >= SLOTS)
                def _():
                    for copy in stores(nxt - SLOTS, nslot):
                        copy.wait()

                for copy in loads(nxt, nslot):
                    copy.start()

        for r in range(step_rows):
            local = pos_ref[row_of(step) + r] - base
            inside = (local >= 0) & (local < seq_block)
            at = jnp.clip(local, 0, seq_block - 1)
            pair = pl.ds(pl.multiple_of((at // 2) * (2 * kv_heads), 2 * kv_heads), 2 * kv_heads)
            hit = half_id == jnp.where(inside, lax.rem(at, 2), 2)
            k_row = jnp.concatenate(both_halves(knbuf, slot, r, kv_half) * 2, axis=0).astype(jnp.bfloat16)
            v_row = jnp.concatenate(both_halves(vnbuf, slot, r, kv_half) * 2, axis=0).astype(jnp.bfloat16)
            kbuf[slot, r, pair, :] = jnp.where(hit, k_row, kbuf[slot, r, pair, :])
            vbuf[slot, r, pair, :] = jnp.where(hit, v_row, vbuf[slot, r, pair, :])

        @pl.when(step >= 2)
        def _():
            o_store(step - 2, oslot).wait()

        m_all = m_ref[...]
        l_all = l_ref[...]
        half = cols // 2
        for tick in range(step_rows + LAG_OUT):
            r = tick
            if r < step_rows:
                q_row = jnp.concatenate(both_halves(qbuf, slot, r, q_half), axis=0).astype(jnp.bfloat16)
                raw = lax.dot_general(q_row, kbuf[slot, r], (((1,), (1,)), ((), ())),
                                      preferred_element_type=jnp.float32)
                s_ref[r] = raw
            r = tick - LAG_SOFT
            if 0 <= r < step_rows:
                local = pos_ref[row_of(step) + r] - base
                seen = key_ref[...] < (local + 1) * kv_heads
                soft = jnp.where(seen, jnp.tanh(s_ref[r] * scale), -4.0)
                top = jnp.maximum(jnp.max(soft, axis=-1, keepdims=True), -1.0)
                weight = jnp.exp2((soft - top) * (SOFT_CAP * LOG2E))
                total = jnp.sum(weight, axis=-1, keepdims=True)
                weight = weight.astype(jnp.bfloat16)
                p_ref[r, :heads] = weight[:, :half]
                p_ref[r, heads:] = weight[:, half:]
                here = lane_id == step * step_rows + r
                m_all = jnp.where(here, top * SOFT_CAP, m_all)
                l_all = jnp.where(here, total, l_all)
            r = tick - LAG_OUT
            if 0 <= r < step_rows:
                right = jnp.concatenate([vbuf[slot, r, :half, :], vbuf[slot, r, half:, :]], axis=1)
                both = jnp.dot(p_ref[r], right, preferred_element_type=jnp.float32)
                obuf[oslot, r * heads:(r + 1) * heads, :] = both[:heads, :head_dim] + both[heads:, head_dim:]
        m_ref[...] = m_all
        l_ref[...] = l_all
        o_start(step, oslot)
        for copy in stores(step, slot):
            copy.start()

        return carry

    lax.fori_loop(0, n_steps, body, 0)
    tail = piece_steps * step_rows * heads
    stat_copies = []
    for d, o_hbm in enumerate((o0_hbm, o1_hbm, o2_hbm, o3_hbm)):
        stat_copies.append(pltpu.make_async_copy(m_ref, o_hbm.at[pl.ds(tail, heads)], st_sem.at[d, 0]))
        stat_copies.append(pltpu.make_async_copy(l_ref, o_hbm.at[pl.ds(tail + heads, heads)], st_sem.at[d, 1]))
    for copy in stat_copies:
        copy.start()
    for copy in stat_copies:
        copy.wait()
    for step in range(max(0, n_steps - SLOTS), n_steps):
        for copy in stores(step, step % SLOTS):
            copy.wait()
    for step in range(max(0, n_steps - 2), n_steps):
        o_store(step, step % 2).wait()


def attend(pos, base, q, kn, vn, k_cache, v_cache, prev, first_row, n_rows):
    rows, cols, head_dim = k_cache.shape
    heads = 2 * q.shape[1] // rows
    kv_heads = 2 * kn.shape[1] // rows
    seq_block = cols // kv_heads
    n_steps = n_rows // ROWS_STEP
    hbm = pl.BlockSpec(memory_space=pl.ANY)
    piece = pltpu.HBM((n_rows // 4 * heads + 2 * heads, head_dim), jnp.float32)
    smem = pl.BlockSpec(memory_space=pltpu.SMEM)
    bf = jnp.bfloat16
    aliases = {} if prev is None else {7: 0, 8: 1}
    extra = () if prev is None else tuple(prev)
    return pl.pallas_call(
        functools.partial(attend_kernel, n_steps, rows // 4, first_row, kv_heads, seq_block),
        out_shape=(jax.ShapeDtypeStruct(k_cache.shape, bf), jax.ShapeDtypeStruct(v_cache.shape, bf)) + (piece,) * 4,
        in_specs=[smem, smem, hbm, hbm, hbm, hbm, hbm] + [hbm] * len(extra),
        out_specs=(hbm, hbm) + (pl.BlockSpec(memory_space=pltpu.HBM),) * 4,
        scratch_shapes=[
            pltpu.VMEM((heads, 128), jnp.float32),
            pltpu.VMEM((heads, 128), jnp.float32),
            pltpu.VMEM((SLOTS, ROWS_STEP, cols, head_dim), bf),
            pltpu.VMEM((SLOTS, ROWS_STEP, cols, head_dim), bf),
            pltpu.VMEM((SLOTS, 2, ROWS_STEP * heads // 2, head_dim), jnp.float32),
            pltpu.VMEM((SLOTS, 2, ROWS_STEP * kv_heads // 2, head_dim), jnp.float32),
            pltpu.VMEM((SLOTS, 2, ROWS_STEP * kv_heads // 2, head_dim), jnp.float32),
            pltpu.VMEM((2, ROWS_STEP * heads, head_dim), jnp.float32),
            pltpu.VMEM((heads, cols), jnp.int32),
            pltpu.VMEM((ROWS_STEP, heads, cols), jnp.float32),
            pltpu.VMEM((ROWS_STEP, 2 * heads, cols // 2), bf),
            pltpu.SemaphoreType.DMA((SLOTS, 5)),
            pltpu.SemaphoreType.DMA((SLOTS, 2)),
            pltpu.SemaphoreType.DMA((2,)),
            pltpu.SemaphoreType.DMA((4, 2)),
        ],
        input_output_aliases=aliases,
        compiler_params=pltpu.CompilerParams(vmem_limit_bytes=62 * 1024 * 1024),
        cost_estimate=pl.CostEstimate(flops=n_rows * heads * cols * head_dim * 4,
                                      bytes_accessed=n_rows * cols * head_dim * 8, transcendentals=0),
        name='attend',
    )(pos, base, q, kn, vn, k_cache, v_cache, *extra)


def merge_kernel(chunks, *refs):
    n_in = 4 * len(chunks)
    source = [refs[4 * c:4 * c + 4] for c in range(len(chunks))]
    pieces = [[b.at[d] for d in range(4)] for b in refs[-len(chunks):]]
    refs = refs[:-len(chunks)]
    (wo_hbm, out_hbm, wo, last_in, last_out, osum, lhs, y_out, y_in, sums,
     p_sem, w_sem, o_send, o_recv, y_send, y_recv, g_send, g_recv, d_send, d_recv, f_send, f_recv, out_sem) = refs[n_in:]
    sp = lax.axis_index('sp')
    tp = lax.axis_index('tp')
    core = lax.rem(sp, 2)
    xpos = sp // 2
    n_chunks, _, chunk = y_out.shape
    heads = lhs.shape[1] // 128
    parts = [c // 4 for c in chunks]
    core_id = 2 * xpos + (1 - core)
    x_id = 2 * (1 - xpos) + core
    far_id = 2 * (1 - xpos) + (1 - core)
    core_peer, x_peer, y_peer = {'sp': core_id}, {'sp': x_id}, {'tp': 1 - tp}
    mesh_id = pl.DeviceIdType.MESH

    def remote(src, dst, send, recv, peer):
        return pltpu.make_async_remote_copy(src_ref=src, dst_ref=dst, send_sem=send, recv_sem=recv,
                                            device_id=peer, device_id_type=mesh_id)

    def w_load(n):
        return pltpu.make_async_copy(wo_hbm.at[:, pl.ds(n * chunk, chunk)], wo.at[n], w_sem.at[n])

    local = [[pltpu.make_async_copy(source[c][d], pieces[c][d], p_sem.at[c, d]) for d in range(4)] for c in range(len(chunks))]
    for copy in local[-1]:
        copy.start()
    barrier = pltpu.get_barrier_semaphore()
    for peer in (core_peer, x_peer, y_peer):
        pl.semaphore_signal(barrier, inc=1, device_id=peer, device_id_type=mesh_id)
    pl.semaphore_wait(barrier, 3)

    for copy in local[-1]:
        copy.wait()
    last = [remote(pieces[-1][3], last_in.at[0], o_send.at[0], o_recv.at[0], core_peer),
            remote(pieces[-1][1], last_in.at[1], o_send.at[1], o_recv.at[1], core_peer),
            remote(last_out, last_in.at[2], o_send.at[2], o_recv.at[2], x_peer)]
    last[0].start()
    last[1].start()
    for copy in local[0]:
        copy.start()
    for n in range(3):
        w_load(n).start()

    def shares(blocks, part):
        count = part * heads
        stats = [block[count:count + 2 * heads, :] for block in blocks]
        top = functools.reduce(jnp.maximum, [st[:heads] for st in stats])
        grown = [jnp.exp(st[:heads] - top) for st in stats]
        return top, sum(st[heads:] * g for st, g in zip(stats, grown)), grown

    def mix(blocks, weights, owner, part, out):
        shift = lax.rem(128 - owner * part, 128)
        factors = [pltpu.roll(w, shift, 1) for w in weights]
        for b in range(part):
            at = slice(b * heads, (b + 1) * heads)
            out[at, :] = sum(block[at, :] * f[:, b:b + 1] for block, f in zip(blocks, factors))

    def combine(blocks, part, row0):
        _, total, grown = shares(blocks, part)
        mix(blocks, [g / total for g in grown], sp, part, osum)
        for h in range(heads):
            lhs[row0:row0 + part, h * 128:(h + 1) * 128] = osum[pl.ds(h, part, stride=heads), :].astype(jnp.bfloat16)

    last[0].wait_recv()
    pair = [pieces[-1][2], last_in.at[0]]
    top, total, grown = shares(pair, parts[-1])
    mix(pair, grown, x_id, parts[-1], last_out)
    count = parts[-1] * heads
    last_out[count:count + heads, :] = top
    last_out[count + heads:count + 2 * heads, :] = total
    last[2].start()

    for copy in local[0]:
        copy.wait()
    combine(pieces[0], parts[0], 0)

    sizes = (2, 2, 2, 2, 1)
    order = []
    for c, part in enumerate(parts):
        begin = 0
        for size in sizes:
            order.append((pl.ds(begin, size), pl.ds(sum(parts[:c]), part), range(begin, begin + size)))
            begin += size
    n_pieces = len(order)
    n_first = len(sizes)

    def to_y(t):
        ns, r, _ = order[t]
        return remote(y_out.at[ns, r], y_in.at[ns, r], y_send.at[t], y_recv.at[t], y_peer)

    def gather(t, owner, send, recv, peer):
        ns, r, _ = order[t]
        return remote(sums.at[owner, ns, r], sums.at[owner, ns, r], send.at[t], recv.at[t], peer)

    def to_x(t):
        return gather(t, sp, g_send, g_recv, x_peer)

    def to_core(t):
        return gather(t, sp, d_send, d_recv, core_peer)

    def relay(t):
        return gather(t, x_id, f_send, f_recv, core_peer)

    def keep(t, turn, owner):
        ns, r, _ = order[t]
        return pltpu.make_async_copy(sums.at[owner, ns, r], out_hbm.at[owner, ns, r], out_sem.at[turn, t])

    def project_rows(n, r0, count):
        y_out[n, r0:r0 + count, :] = jnp.dot(lhs[r0:r0 + count, :], wo[n], preferred_element_type=jnp.float32)

    for t in range(n_first):
        for n in order[t][2]:
            w_load(n).wait()
            if n + 3 < n_chunks:
                w_load(n + 3).start()
            project_rows(n, 0, parts[0])
        to_y(t).start()

    for t in range(n_pieces + 3):
        if t == 2:
            for copy in last[1:]:
                copy.wait_recv()
            combine([pieces[-1][0], last_in.at[1], last_in.at[2]], parts[-1], parts[0])
        if 2 <= t < 2 + n_first:
            for n in order[n_first + t - 2][2]:
                project_rows(n, parts[0], parts[-1])
            to_y(n_first + t - 2).start()
        if t < n_pieces:
            ns, r, _ = order[t]
            to_y(t).wait()
            sums[sp, ns, r, :] = y_out[ns, r, :] + y_in[ns, r, :]
            to_x(t).start()
            to_core(t).start()
            keep(t, 0, sp).start()
        if 1 <= t < n_pieces + 1:
            to_x(t - 1).wait_recv()
            relay(t - 1).start()
            keep(t - 1, 1, x_id).start()
        if t >= 3:
            to_core(t - 3).wait_recv()
            keep(t - 3, 2, core_id).start()
            relay(t - 3).wait_recv()
            keep(t - 3, 3, far_id).start()
    for copy in last:
        copy.wait_send()
    for t in range(n_pieces):
        to_x(t).wait_send()
        to_core(t).wait_send()
        relay(t).wait_send()
        for turn in range(4):
            keep(t, turn, sp).wait()


def merge(chunks, pieces, w_o, n_chunks):
    inner, width = w_o.shape
    heads = inner // 128
    quarter = sum(chunks) // 4
    chunk = width // n_chunks
    hbm = pl.BlockSpec(memory_space=pltpu.HBM)
    f32 = jnp.float32
    dma = pltpu.SemaphoreType.DMA
    flat = [p for piece in pieces for p in piece]
    block = pieces[-1][0].shape
    return pl.pallas_call(
        functools.partial(merge_kernel, chunks),
        out_shape=pltpu.HBM((4, n_chunks, quarter, chunk), f32),
        in_specs=[hbm] * (len(flat) + 1),
        out_specs=hbm,
        scratch_shapes=[
            pltpu.VMEM((n_chunks, inner, chunk), jnp.bfloat16),
            pltpu.VMEM((3,) + block, f32),
            pltpu.VMEM(block, f32),
            pltpu.VMEM((max(chunks) // 4 * heads, 128), f32),
            pltpu.VMEM((quarter, inner), jnp.bfloat16),
            pltpu.VMEM((n_chunks, quarter, chunk), f32),
            pltpu.VMEM((n_chunks, quarter, chunk), f32),
            pltpu.VMEM((4, n_chunks, quarter, chunk), f32),
            dma((len(chunks), 4)), dma((n_chunks,)), dma((3,)), dma((3,)),
        ] + [dma((10,))] * 8 + [dma((4, 10))] + [pltpu.VMEM((4,) + piece[0].shape, f32) for piece in pieces],
        compiler_params=pltpu.CompilerParams(vmem_limit_bytes=56 * 1024 * 1024, collective_id=0, has_side_effects=True),
        cost_estimate=pl.CostEstimate(flops=2 * quarter * inner * width, bytes_accessed=2 * inner * width, transcendentals=0),
        name='merge',
    )(*flat, pltpu.with_memory_space_constraint(w_o, pltpu.HBM))


def finish_kernel(sums_hbm, x_hbm, wpost_ref, out_hbm, gain_ref, sums, xbuf, obuf, in_sem, out_sem):
    parts, n_chunks, rows, chunk = sums.shape

    def loads(q):
        at = pl.ds(q * rows, rows)
        return (pltpu.make_async_copy(sums_hbm.at[q], sums.at[q], in_sem.at[q, 0]),
                pltpu.make_async_copy(x_hbm.at[at], xbuf.at[at], in_sem.at[q, 1]))

    def store(q):
        at = pl.ds(q * rows, rows)
        return pltpu.make_async_copy(obuf.at[at], out_hbm.at[at], out_sem.at[q])

    for q in range(2):
        for copy in loads(q):
            copy.start()
    for j in range(wpost_ref.shape[0]):
        gain_ref[:, j * 128:(j + 1) * 128] = 1.0 + wpost_ref[j:j + 1, :]
    for q in range(parts):
        for copy in loads(q):
            copy.wait()
        if q + 2 < parts:
            for copy in loads(q + 2):
                copy.start()
        for k in range(rows // 16):
            at = slice(k * 16, (k + 1) * 16)
            to = slice(q * rows + k * 16, q * rows + (k + 1) * 16)
            square = jnp.zeros((16, chunk), jnp.float32)
            for n in range(n_chunks):
                u = sums[q, n, at, :]
                square = square + u * u
            inv = lax.rsqrt(jnp.sum(square, axis=-1, keepdims=True) * (1.0 / (n_chunks * chunk)) + NORM_EPS)
            for n in range(n_chunks):
                col = slice(n * chunk, (n + 1) * chunk)
                y = xbuf[to, col].astype(jnp.float32) + sums[q, n, at, :] * inv * gain_ref[:, col]
                obuf[to, col] = y.astype(jnp.bfloat16)
        store(q).start()
    for q in range(parts):
        store(q).wait()


def finish(sums, x_in, w_post):
    parts = sums.shape[0]
    hbm = pl.BlockSpec(memory_space=pltpu.HBM)
    dma = pltpu.SemaphoreType.DMA
    return pl.pallas_call(
        finish_kernel,
        out_shape=jax.ShapeDtypeStruct(x_in.shape, x_in.dtype),
        in_specs=[hbm, hbm, pl.BlockSpec(memory_space=pltpu.VMEM)],
        out_specs=hbm,
        scratch_shapes=[pltpu.VMEM((1, x_in.shape[1]), jnp.float32), pltpu.VMEM(sums.shape, jnp.float32),
                        pltpu.VMEM(x_in.shape, x_in.dtype), pltpu.VMEM(x_in.shape, x_in.dtype), dma((parts, 2)), dma((parts,))],
        compiler_params=pltpu.CompilerParams(vmem_limit_bytes=62 * 1024 * 1024),
        name='finish',
    )(sums, x_in, w_post)


def solution(mesh):
    cache_spec = P('dp', 'sp', 'tp', None)
    sp_size = mesh.shape['sp']

    def local_step(x_in, cur_pos, w_pre, w_q, w_k, w_v, w_o, w_post, k_cache, v_cache):
        row_count, seq_block, kv_local, head_dim = k_cache.shape
        sp_index = lax.axis_index('sp')
        table = rotary_table(sp_size * seq_block, head_dim)
        q_rot, kn2, vn2 = project(cur_pos, x_in, w_pre.reshape(-1, 128), table, w_q, w_k, w_v)
        base = (sp_index * seq_block).astype(jnp.int32).reshape(1)
        kc = k_cache.reshape(row_count, seq_block * kv_local, head_dim)
        vc = v_cache.reshape(row_count, seq_block * kv_local, head_dim)
        chunks = (row_count // 2, row_count // 2)
        prev, first_row, pieces = None, 0, []
        for index, n_rows in enumerate(chunks):
            *prev, p0, p1, p2, p3 = attend(cur_pos, base, q_rot, kn2, vn2, kc, vc, prev, first_row, n_rows)
            first_row += n_rows // 4
            if index < len(chunks) - 1:
                moved = []
                for d, p in ((1, p1), (2, p2), (3, p3)):
                    moved.append(lax.ppermute(p, 'sp', [(i, i ^ d) for i in range(sp_size)]))
                p1, p2, p3 = moved
            pieces.append((p0, p1, p2, p3))
        k_out, v_out = prev
        x_out = finish(merge(chunks, pieces, w_o, 9), x_in, w_post.reshape(-1, 128))
        return x_out, k_out.reshape(k_cache.shape), v_out.reshape(v_cache.shape)

    return jax.shard_map(local_step, mesh=mesh,
                         in_specs=(P('dp', None), P('dp'), P(None), P(None, 'tp'), P(None, 'tp'), P(None, 'tp'), P('tp', None), P(None), cache_spec, cache_spec),
                         out_specs=(P('dp', None), cache_spec, cache_spec), check_vma=False)
```

```python
import functools

import jax
import jax.numpy as jnp
import numpy as np
from jax import lax
from jax.experimental import pallas as pl
from jax.experimental.pallas import tpu as pltpu
from jax.sharding import PartitionSpec as P

SOFT_CAP = 50.0
ROPE_BASE = 10000.0
NORM_EPS = 1e-6
LOG2E = 1.4426950408889634

ROWS_STEP = 8
SLOTS = 12
AHEAD = 6
START = 2
LAG_SOFT = 2
LAG_OUT = 4


def rotary_table(length, head_dim):
    half_dim = head_dim // 2
    inv_freq = np.power(np.float32(ROPE_BASE), -2.0 * np.arange(half_dim, dtype=np.float32) / np.float32(2 * half_dim)).astype(np.float32)
    angles = np.arange(length, dtype=np.float32)[:, None] * inv_freq[None, :]
    cos_tab = np.cos(angles.astype(np.float64))
    sin_tab = np.sin(angles.astype(np.float64))
    return np.concatenate([cos_tab, cos_tab, -sin_tab, sin_tab], axis=-1).astype(np.float32)


def project_kernel(pos_ref, x_hbm, wpre_ref, table_ref, wq_hbm, wk_hbm, wv_hbm, q_ref, k_ref, v_ref,
                   x_ref, gain_ref, cos_ref, sin_ref, weight, normed, q_part, k_part, v_part, x_sem, w_sem, send_sem, recv_sem,
                   out_sem):
    sp = lax.axis_index('sp')
    core = lax.rem(sp, 2)
    peer = {'sp': sp + 1 - 2 * core}
    mesh_id = pl.DeviceIdType.MESH
    rows = x_ref.shape[0]
    block = weight.shape[2]
    per = block // 128
    plan = []
    for w_hbm, part, turn in ((wq_hbm, q_part, True), (wk_hbm, k_part, True), (wv_hbm, v_part, False)):
        mine = w_hbm.shape[1] // 2
        for j in range(mine // block):
            plan.append((w_hbm, part, turn, mine, j, j == mine // block - 1))

    def load(i):
        w_hbm, _, _, mine, j, _ = plan[i]
        col = pl.multiple_of(core * mine + j * block, block)
        return pltpu.make_async_copy(w_hbm.at[:, pl.ds(col, block)], weight.at[i], w_sem.at[i])

    x_loads = [pltpu.make_async_copy(x_hbm.at[pl.ds(k * (rows // 4), rows // 4)], x_ref.at[pl.ds(k * (rows // 4), rows // 4)],
                                     x_sem.at[k]) for k in range(4)]
    for copy in x_loads:
        copy.start()
    load(0).start()
    barrier = pltpu.get_barrier_semaphore()
    pl.semaphore_signal(barrier, inc=1, device_id=peer, device_id_type=mesh_id)
    pl.semaphore_wait(barrier, 1)

    for j in range(wpre_ref.shape[0]):
        gain_ref[:, j * 128:(j + 1) * 128] = 1.0 + wpre_ref[j:j + 1, :]
    gain = gain_ref[...]

    def look_up(k, carry):
        for r in range(8):
            b = k * 8 + r
            row = table_ref[pl.ds(pos_ref[b], 1), :]
            cos_ref[pl.ds(b, 1), :] = row[:, :128]
            sin_ref[pl.ds(b, 1), :] = row[:, 128:]
        return carry

    lax.fori_loop(0, rows // 8, look_up, 0)

    def norm(k, carry):
        at = pl.ds(pl.multiple_of(k * 32, 32), 32)
        x = x_ref[at, :].astype(jnp.float32)
        inv = lax.rsqrt(jnp.mean(x * x, axis=-1, keepdims=True) + NORM_EPS)
        normed[at, :] = (x * inv * gain).astype(jnp.bfloat16)
        return carry

    for k in range(4):
        x_loads[k].wait()
        if k == 1:
            load(1).start()
        lax.fori_loop(k * rows // 128, (k + 1) * rows // 128, norm, 0)

    outs = ((q_part, q_ref), (k_part, k_ref), (v_part, v_ref))
    sends, writes = [], []
    for i, (_, part, turn, mine, j, done) in enumerate(plan):
        load(i).wait()
        if i + 2 < len(plan):
            load(i + 2).start()
        heads = mine // 128
        acc = jnp.dot(normed[...], weight[i], preferred_element_type=jnp.float32)
        for t in range(per):
            value = acc[:, t * 128:(t + 1) * 128]
            if turn:
                value = value * cos_ref[...] + pltpu.roll(value, 64, 1) * sin_ref[...]
            part[pl.ds(j * per + t, rows, stride=heads), :] = value
        if done:
            n = len(sends)
            copy = pltpu.make_async_remote_copy(src_ref=part, dst_ref=outs[n][1].at[core], send_sem=send_sem.at[n],
                                                recv_sem=recv_sem.at[n], device_id=peer, device_id_type=mesh_id)
            copy.start()
            sends.append(copy)
            out = pltpu.make_async_copy(part, outs[n][1].at[core], out_sem.at[n])
            out.start()
            writes.append(out)
    for copy in sends:
        copy.wait()
    for copy in writes:
        copy.wait()


def project(cur_pos, x_in, w_pre, table, w_q, w_k, w_v):
    rows, width = x_in.shape
    block = 512
    q_cols, kv_cols = w_q.shape[1], w_k.shape[1]
    n_blocks = (q_cols + 2 * kv_cols) // 2 // block
    vmem = pl.BlockSpec(memory_space=pltpu.VMEM)
    hbm = pl.BlockSpec(memory_space=pltpu.HBM)
    f32, bf = jnp.float32, jnp.bfloat16
    dma = pltpu.SemaphoreType.DMA
    return pl.pallas_call(
        project_kernel,
        out_shape=(pltpu.HBM((2, rows * q_cols // 256, 128), f32), pltpu.HBM((2, rows * kv_cols // 256, 128), f32),
                   pltpu.HBM((2, rows * kv_cols // 256, 128), f32)),
        in_specs=[pl.BlockSpec(memory_space=pltpu.SMEM), hbm, vmem, vmem] + [hbm] * 3,
        out_specs=(hbm,) * 3,
        scratch_shapes=[
            pltpu.VMEM((rows, width), bf),
            pltpu.VMEM((1, width), f32),
            pltpu.VMEM((rows, 128), f32),
            pltpu.VMEM((rows, 128), f32),
            pltpu.VMEM((n_blocks, width, block), bf),
            pltpu.VMEM((rows, width), bf),
            pltpu.VMEM((rows * q_cols // 256, 128), f32),
            pltpu.VMEM((rows * kv_cols // 256, 128), f32),
            pltpu.VMEM((rows * kv_cols // 256, 128), f32),
            dma((4,)), dma((n_blocks,)), dma((3,)), dma((3,)), dma((3,)),
        ],
        compiler_params=pltpu.CompilerParams(vmem_limit_bytes=62 * 1024 * 1024, collective_id=1, has_side_effects=True),
        cost_estimate=pl.CostEstimate(flops=rows * width * (q_cols + 2 * kv_cols), bytes_accessed=width * (q_cols + 2 * kv_cols), transcendentals=0),
        name='project',
    )(cur_pos, x_in, w_pre, table, w_q, w_k, w_v)


def attend_kernel(n_steps, quarter, n_groups, kv_heads, seq_block, pos_ref, base_ref, q_hbm, kn_hbm, vn_hbm, k_hbm, v_hbm,
                  *rest):
    (ko_hbm, vo_hbm, o0_hbm, o1_hbm, o2_hbm, o3_hbm, m_ref, l_ref, kbuf, vbuf, qbuf, knbuf, vnbuf, obuf, key_ref, s_ref, p_ref, in_sem, out_sem, o_sem, st_sem) = rest[-21:]
    step_rows = ROWS_STEP
    group_steps = n_steps // n_groups
    piece_steps = group_steps // 4
    _, heads, head_dim = m_ref.shape
    q_half, kv_half = heads // 2, kv_heads // 2
    cols = seq_block * kv_heads
    base = base_ref[0]

    row_id = lax.broadcasted_iota(jnp.int32, (heads, cols), 0)
    col_id = lax.broadcasted_iota(jnp.int32, (heads, cols), 1)
    mine = lax.rem(col_id, kv_heads) == row_id // (heads // kv_heads)
    key_ref[...] = jnp.where(mine, col_id, cols * 4)
    lane_id = lax.broadcasted_iota(jnp.int32, m_ref.shape[1:], 1)
    half_id = lax.broadcasted_iota(jnp.int32, (2 * kv_heads, head_dim), 0) // kv_heads

    def split_of(step):
        group = step // group_steps
        inner = step - group * group_steps
        piece = inner // piece_steps
        return group, inner, piece, inner - piece * piece_steps

    def row_of(step):
        group, _, piece, turn = split_of(step)
        return piece * quarter + (group * piece_steps + turn) * step_rows

    def heads_of(step, count):
        return pl.ds(row_of(step) * count, step_rows * count)

    def both_halves(ref, slot, r, count):
        at = slice(r * count, (r + 1) * count)
        return [ref[slot, 0, at, :], ref[slot, 1, at, :]]

    def loads(step, slot):
        rows = pl.ds(row_of(step), step_rows)
        return (pltpu.make_async_copy(k_hbm.at[rows], kbuf.at[slot], in_sem.at[slot, 0]),
                pltpu.make_async_copy(v_hbm.at[rows], vbuf.at[slot], in_sem.at[slot, 1]),
                pltpu.make_async_copy(q_hbm.at[:, heads_of(step, q_half)], qbuf.at[slot], in_sem.at[slot, 2]),
                pltpu.make_async_copy(kn_hbm.at[:, heads_of(step, kv_half)], knbuf.at[slot], in_sem.at[slot, 3]),
                pltpu.make_async_copy(vn_hbm.at[:, heads_of(step, kv_half)], vnbuf.at[slot], in_sem.at[slot, 4]))

    def stores(step, slot):
        rows = pl.ds(row_of(step), step_rows)
        return (pltpu.make_async_copy(kbuf.at[slot], ko_hbm.at[rows], out_sem.at[slot, 0]),
                pltpu.make_async_copy(vbuf.at[slot], vo_hbm.at[rows], out_sem.at[slot, 1]))

    def o_store(step, slot, d=0):
        group, _, _, turn = split_of(step)
        at = pl.ds(turn * step_rows * heads, step_rows * heads)
        o_hbm = (o0_hbm, o1_hbm, o2_hbm, o3_hbm)[d]
        return pltpu.make_async_copy(obuf.at[slot], o_hbm.at[group, at], o_sem.at[slot])

    def o_start(step, slot):
        turn = jnp.bitwise_xor(split_of(step)[2], base // seq_block)
        for d in range(4):
            @pl.when(turn == d)
            def _():
                o_store(step, slot, d).start()

    for step in range(min(START, n_steps)):
        for copy in loads(step, step):
            copy.start()
    m_ref[...] = jnp.zeros_like(m_ref)
    l_ref[...] = jnp.zeros_like(l_ref)
    scale = head_dim ** -0.5 / SOFT_CAP

    def body(step, carry):
        slot = lax.rem(step, SLOTS)
        oslot = lax.rem(step, 2)
        for copy in loads(step, slot):
            copy.wait()
        issued = jnp.minimum(step + AHEAD, START + 2 * step)
        wanted = jnp.minimum(jnp.minimum(step + 1 + AHEAD, START + 2 * step + 2), n_steps)
        for extra in range(2):
            nxt = issued + extra

            @pl.when(nxt < wanted)
            def _():
                nslot = lax.rem(nxt, SLOTS)

                @pl.when(nxt >= SLOTS)
                def _():
                    for copy in stores(nxt - SLOTS, nslot):
                        copy.wait()
                for copy in loads(nxt, nslot):
                    copy.start()

        for r in range(step_rows):
            local = pos_ref[row_of(step) + r] - base
            inside = (local >= 0) & (local < seq_block)
            at = jnp.clip(local, 0, seq_block - 1)
            pair = pl.ds(pl.multiple_of((at // 2) * (2 * kv_heads), 2 * kv_heads), 2 * kv_heads)
            hit = half_id == jnp.where(inside, lax.rem(at, 2), 2)
            k_row = jnp.concatenate(both_halves(knbuf, slot, r, kv_half) * 2, axis=0).astype(jnp.bfloat16)
            v_row = jnp.concatenate(both_halves(vnbuf, slot, r, kv_half) * 2, axis=0).astype(jnp.bfloat16)
            kbuf[slot, r, pair, :] = jnp.where(hit, k_row, kbuf[slot, r, pair, :])
            vbuf[slot, r, pair, :] = jnp.where(hit, v_row, vbuf[slot, r, pair, :])

        @pl.when(step >= 2)
        def _():
            o_store(step - 2, oslot).wait()

        group, inner, _, _ = split_of(step)
        m_all = m_ref[group]
        l_all = l_ref[group]
        half = cols // 2
        for tick in range(step_rows + LAG_OUT):
            r = tick
            if r < step_rows:
                q_row = jnp.concatenate(both_halves(qbuf, slot, r, q_half), axis=0).astype(jnp.bfloat16)
                raw = lax.dot_general(q_row, kbuf[slot, r], (((1,), (1,)), ((), ())),
                                      preferred_element_type=jnp.float32)
                s_ref[r] = raw
            r = tick - LAG_SOFT
            if 0 <= r < step_rows:
                local = pos_ref[row_of(step) + r] - base
                seen = key_ref[...] < (local + 1) * kv_heads
                soft = jnp.where(seen, jnp.tanh(s_ref[r] * scale), -4.0)
                top = jnp.maximum(jnp.max(soft, axis=-1, keepdims=True), -1.0)
                weight = jnp.exp2((soft - top) * (SOFT_CAP * LOG2E))
                total = jnp.sum(weight, axis=-1, keepdims=True)
                weight = weight.astype(jnp.bfloat16)
                p_ref[r, :heads] = weight[:, :half]
                p_ref[r, heads:] = weight[:, half:]
                here = lane_id == inner * step_rows + r
                m_all = jnp.where(here, top * SOFT_CAP, m_all)
                l_all = jnp.where(here, total, l_all)
            r = tick - LAG_OUT
            if 0 <= r < step_rows:
                right = jnp.concatenate([vbuf[slot, r, :half, :], vbuf[slot, r, half:, :]], axis=1)
                both = jnp.dot(p_ref[r], right, preferred_element_type=jnp.float32)
                obuf[oslot, r * heads:(r + 1) * heads, :] = both[:heads, :head_dim] + both[heads:, head_dim:]
        m_ref[group] = m_all
        l_ref[group] = l_all
        o_start(step, oslot)
        for copy in stores(step, slot):
            copy.start()

        return carry

    lax.fori_loop(0, n_steps, body, 0)
    tail = piece_steps * step_rows * heads
    stat_copies = []
    for d, o_hbm in enumerate((o0_hbm, o1_hbm, o2_hbm, o3_hbm)):
        stat_copies.append(pltpu.make_async_copy(m_ref, o_hbm.at[:, pl.ds(tail, heads)], st_sem.at[d, 0]))
        stat_copies.append(pltpu.make_async_copy(l_ref, o_hbm.at[:, pl.ds(tail + heads, heads)], st_sem.at[d, 1]))
    for copy in stat_copies:
        copy.start()
    for copy in stat_copies:
        copy.wait()
    for step in range(max(0, n_steps - SLOTS), n_steps):
        for copy in stores(step, step % SLOTS):
            copy.wait()
    for step in range(max(0, n_steps - 2), n_steps):
        o_store(step, step % 2).wait()


def attend(pos, base, q, kn, vn, k_cache, v_cache, n_groups):
    rows, cols, head_dim = k_cache.shape
    heads = 2 * q.shape[1] // rows
    kv_heads = 2 * kn.shape[1] // rows
    seq_block = cols // kv_heads
    n_steps = rows // ROWS_STEP
    hbm = pl.BlockSpec(memory_space=pl.ANY)
    piece = pltpu.HBM((n_groups, rows // (4 * n_groups) * heads + 2 * heads, head_dim), jnp.float32)
    smem = pl.BlockSpec(memory_space=pltpu.SMEM)
    bf = jnp.bfloat16
    return pl.pallas_call(
        functools.partial(attend_kernel, n_steps, rows // 4, n_groups, kv_heads, seq_block),
        out_shape=(jax.ShapeDtypeStruct(k_cache.shape, bf), jax.ShapeDtypeStruct(v_cache.shape, bf)) + (piece,) * 4,
        in_specs=[smem, smem, hbm, hbm, hbm, hbm, hbm],
        out_specs=(hbm, hbm) + (pl.BlockSpec(memory_space=pltpu.HBM),) * 4,
        scratch_shapes=[
            pltpu.VMEM((n_groups, heads, 128), jnp.float32),
            pltpu.VMEM((n_groups, heads, 128), jnp.float32),
            pltpu.VMEM((SLOTS, ROWS_STEP, cols, head_dim), bf),
            pltpu.VMEM((SLOTS, ROWS_STEP, cols, head_dim), bf),
            pltpu.VMEM((SLOTS, 2, ROWS_STEP * heads // 2, head_dim), jnp.float32),
            pltpu.VMEM((SLOTS, 2, ROWS_STEP * kv_heads // 2, head_dim), jnp.float32),
            pltpu.VMEM((SLOTS, 2, ROWS_STEP * kv_heads // 2, head_dim), jnp.float32),
            pltpu.VMEM((2, ROWS_STEP * heads, head_dim), jnp.float32),
            pltpu.VMEM((heads, cols), jnp.int32),
            pltpu.VMEM((ROWS_STEP, heads, cols), jnp.float32),
            pltpu.VMEM((ROWS_STEP, 2 * heads, cols // 2), bf),
            pltpu.SemaphoreType.DMA((SLOTS, 5)),
            pltpu.SemaphoreType.DMA((SLOTS, 2)),
            pltpu.SemaphoreType.DMA((2,)),
            pltpu.SemaphoreType.DMA((4, 2)),
        ],
        compiler_params=pltpu.CompilerParams(vmem_limit_bytes=62 * 1024 * 1024),
        cost_estimate=pl.CostEstimate(flops=rows * heads * cols * head_dim * 4,
                                      bytes_accessed=rows * cols * head_dim * 8, transcendentals=0),
        name='attend',
    )(pos, base, q, kn, vn, k_cache, v_cache)


def merge_kernel(b0, b1, b2, b3, wo_hbm, out_hbm, wo, mine, near, pair_in, x_in, pair_out, osum, lhs, y_out, y_in, sums,
                 p_sem, w_sem, o_send, o_recv, y_send, y_recv, g_send, g_recv, d_send, d_recv, f_send, f_recv, out_sem):
    sp = lax.axis_index('sp')
    tp = lax.axis_index('tp')
    core = lax.rem(sp, 2)
    xpos = sp // 2
    n_chunks, quarter, chunk = y_out.shape
    heads = lhs.shape[1] // 128
    n_groups = mine.shape[1]
    part = quarter // n_groups
    count = part * heads
    core_id = 2 * xpos + (1 - core)
    x_id = 2 * (1 - xpos) + core
    far_id = 2 * (1 - xpos) + (1 - core)
    core_peer, x_peer, y_peer = {'sp': core_id}, {'sp': x_id}, {'tp': 1 - tp}
    mesh_id = pl.DeviceIdType.MESH

    def remote(src, dst, send, recv, peer):
        return pltpu.make_async_remote_copy(src_ref=src, dst_ref=dst, send_sem=send, recv_sem=recv,
                                            device_id=peer, device_id_type=mesh_id)

    def w_load(n):
        return pltpu.make_async_copy(wo_hbm.at[:, pl.ds(n * chunk, chunk)], wo.at[n], w_sem.at[n])

    local = [pltpu.make_async_copy(b, mine.at[d], p_sem.at[d]) for d, b in enumerate((b0, b1, b2, b3))]
    local[3].start()
    local[2].start()
    barrier = pltpu.get_barrier_semaphore()
    for peer in (core_peer, x_peer, y_peer):
        pl.semaphore_signal(barrier, inc=1, device_id=peer, device_id_type=mesh_id)
    pl.semaphore_wait(barrier, 3)

    far = [remote(mine.at[3, c], pair_in.at[c], o_send.at[0, c], o_recv.at[0, c], core_peer) for c in range(n_groups)]
    to_near = [remote(mine.at[1, c], near.at[c], o_send.at[1, c], o_recv.at[1, c], core_peer) for c in range(n_groups)]
    over_x = [remote(pair_out.at[c], x_in.at[c], o_send.at[2, c], o_recv.at[2, c], x_peer) for c in range(n_groups)]
    local[3].wait()
    for copy in far:
        copy.start()
    local[1].start()
    local[0].start()
    for n in range(3):
        w_load(n).start()

    def shares(blocks):
        stats = [block[count:count + 2 * heads, :] for block in blocks]
        top = functools.reduce(jnp.maximum, [st[:heads] for st in stats])
        grown = [jnp.exp(st[:heads] - top) for st in stats]
        return top, sum(st[heads:] * g for st, g in zip(stats, grown)), grown

    def mix(blocks, weights, owner, out):
        shift = lax.rem(128 - owner * part, 128)
        factors = [pltpu.roll(w, shift, 1) for w in weights]
        for b in range(part):
            at = slice(b * heads, (b + 1) * heads)
            out[at, :] = sum(block[at, :] * f[:, b:b + 1] for block, f in zip(blocks, factors))

    local[2].wait()
    for c in range(n_groups):
        far[c].wait_recv()
        pair = [mine.at[2, c], pair_in.at[c]]
        top, total, grown = shares(pair)
        mix(pair, grown, x_id, pair_out.at[c])
        pair_out[c, count:count + heads, :] = top
        pair_out[c, count + heads:count + 2 * heads, :] = total
        over_x[c].start()
        if c == 0:
            local[1].wait()
            for copy in to_near:
                copy.start()
    local[0].wait()

    def combine(c):
        to_near[c].wait_recv()
        over_x[c].wait_recv()
        blocks = [mine.at[0, c], near.at[c], x_in.at[c]]
        _, total, grown = shares(blocks)
        mix(blocks, [g / total for g in grown], sp, osum)
        for h in range(heads):
            lhs[c * part:(c + 1) * part, h * 128:(h + 1) * 128] = osum[pl.ds(h, part, stride=heads), :].astype(jnp.bfloat16)

    wide = 3
    order = [(c, n) for c in range(n_groups) for n in range(0, n_chunks, wide)]
    n_pieces = len(order)
    per = n_chunks // wide

    def where(t):
        c, n = order[t]
        return pl.ds(n, wide), pl.ds(c * part, part)

    def to_y(t):
        ns, r = where(t)
        return remote(y_out.at[ns, r], y_in.at[ns, r], y_send.at[t], y_recv.at[t], y_peer)

    def gather(t, owner, send, recv, peer):
        ns, r = where(t)
        return remote(sums.at[owner, ns, r], sums.at[owner, ns, r], send.at[t], recv.at[t], peer)

    def to_x(t):
        return gather(t, sp, g_send, g_recv, x_peer)

    def to_core(t):
        return gather(t, sp, d_send, d_recv, core_peer)

    def relay(t):
        return gather(t, x_id, f_send, f_recv, core_peer)

    def keep(t, turn, owner):
        ns, r = where(t)
        return pltpu.make_async_copy(sums.at[owner, ns, r], out_hbm.at[owner, ns, r], out_sem.at[turn, t])

    def project(t):
        c, first = order[t]
        at = slice(c * part, (c + 1) * part)
        for n in range(first, first + wide):
            if c == 0:
                w_load(n).wait()
                if n + 3 < n_chunks:
                    w_load(n + 3).start()
            y_out[n, at, :] = jnp.dot(lhs[at, :], wo[n], preferred_element_type=jnp.float32)
        to_y(t).start()

    combine(0)
    for t in range(per):
        project(t)
    ahead = per
    for t in range(n_pieces + 3):
        for _ in range(2 if t < per else 1):
            if t >= 0 and ahead < n_pieces:
                if ahead % per == 0:
                    combine(ahead // per)
                project(ahead)
                ahead += 1
        if t < n_pieces:
            ns, r = where(t)
            to_y(t).wait()
            sums[sp, ns, r, :] = y_out[ns, r, :] + y_in[ns, r, :]
            to_x(t).start()
            to_core(t).start()
            keep(t, 0, sp).start()
        if 1 <= t < n_pieces + 1:
            to_x(t - 1).wait_recv()
            relay(t - 1).start()
            keep(t - 1, 1, x_id).start()
        if t >= 3:
            to_core(t - 3).wait_recv()
            keep(t - 3, 2, core_id).start()
            relay(t - 3).wait_recv()
            keep(t - 3, 3, far_id).start()
    for copy in far + to_near + over_x:
        copy.wait_send()
    for t in range(n_pieces):
        to_x(t).wait_send()
        to_core(t).wait_send()
        relay(t).wait_send()
        for turn in range(4):
            keep(t, turn, sp).wait()


def merge(blocks, w_o, n_chunks):
    inner, width = w_o.shape
    n_groups, height, head_dim = blocks[0].shape
    heads = inner // head_dim
    quarter = n_groups * (height // heads - 2)
    chunk = width // n_chunks
    hbm = pl.BlockSpec(memory_space=pltpu.HBM)
    f32 = jnp.float32
    dma = pltpu.SemaphoreType.DMA
    n_pieces = n_groups * n_chunks // 3
    block = pltpu.VMEM((n_groups, height, head_dim), f32)
    return pl.pallas_call(
        merge_kernel,
        out_shape=pltpu.HBM((4, n_chunks, quarter, chunk), f32),
        in_specs=[hbm] * 5,
        out_specs=hbm,
        scratch_shapes=[
            pltpu.VMEM((n_chunks, inner, chunk), jnp.bfloat16),
            pltpu.VMEM((4, n_groups, height, head_dim), f32),
            block, block, block, block,
            pltpu.VMEM((height, head_dim), f32),
            pltpu.VMEM((quarter, inner), jnp.bfloat16),
            pltpu.VMEM((n_chunks, quarter, chunk), f32),
            pltpu.VMEM((n_chunks, quarter, chunk), f32),
            pltpu.VMEM((4, n_chunks, quarter, chunk), f32),
            dma((4,)), dma((n_chunks,)), dma((3, n_groups)), dma((3, n_groups)),
        ] + [dma((n_pieces,))] * 8 + [dma((4, n_pieces))],
        compiler_params=pltpu.CompilerParams(vmem_limit_bytes=56 * 1024 * 1024, collective_id=0, has_side_effects=True),
        cost_estimate=pl.CostEstimate(flops=2 * quarter * inner * width, bytes_accessed=2 * inner * width, transcendentals=0),
        name='merge',
    )(*blocks, pltpu.with_memory_space_constraint(w_o, pltpu.HBM))


def finish_kernel(sums_hbm, x_hbm, wpost_ref, out_hbm, gain_ref, sums, xbuf, obuf, in_sem, out_sem):
    parts, n_chunks, rows, chunk = sums.shape

    def loads(q):
        at = pl.ds(q * rows, rows)
        return (pltpu.make_async_copy(sums_hbm.at[q], sums.at[q], in_sem.at[q, 0]),
                pltpu.make_async_copy(x_hbm.at[at], xbuf.at[at], in_sem.at[q, 1]))

    def store(q):
        at = pl.ds(q * rows, rows)
        return pltpu.make_async_copy(obuf.at[at], out_hbm.at[at], out_sem.at[q])

    for q in range(2):
        for copy in loads(q):
            copy.start()
    for j in range(wpost_ref.shape[0]):
        gain_ref[:, j * 128:(j + 1) * 128] = 1.0 + wpost_ref[j:j + 1, :]
    for q in range(parts):
        for copy in loads(q):
            copy.wait()
        if q + 2 < parts:
            for copy in loads(q + 2):
                copy.start()
        for k in range(rows // 16):
            at = slice(k * 16, (k + 1) * 16)
            to = slice(q * rows + k * 16, q * rows + (k + 1) * 16)
            square = jnp.zeros((16, chunk), jnp.float32)
            for n in range(n_chunks):
                u = sums[q, n, at, :]
                square = square + u * u
            inv = lax.rsqrt(jnp.sum(square, axis=-1, keepdims=True) * (1.0 / (n_chunks * chunk)) + NORM_EPS)
            for n in range(n_chunks):
                col = slice(n * chunk, (n + 1) * chunk)
                y = xbuf[to, col].astype(jnp.float32) + sums[q, n, at, :] * inv * gain_ref[:, col]
                obuf[to, col] = y.astype(jnp.bfloat16)
        store(q).start()
    for q in range(parts):
        store(q).wait()


def finish(sums, x_in, w_post):
    parts = sums.shape[0]
    hbm = pl.BlockSpec(memory_space=pltpu.HBM)
    dma = pltpu.SemaphoreType.DMA
    return pl.pallas_call(
        finish_kernel,
        out_shape=jax.ShapeDtypeStruct(x_in.shape, x_in.dtype),
        in_specs=[hbm, hbm, pl.BlockSpec(memory_space=pltpu.VMEM)],
        out_specs=hbm,
        scratch_shapes=[pltpu.VMEM((1, x_in.shape[1]), jnp.float32), pltpu.VMEM(sums.shape, jnp.float32),
                        pltpu.VMEM(x_in.shape, x_in.dtype), pltpu.VMEM(x_in.shape, x_in.dtype), dma((parts, 2)), dma((parts,))],
        compiler_params=pltpu.CompilerParams(vmem_limit_bytes=62 * 1024 * 1024),
        name='finish',
    )(sums, x_in, w_post)


def solution(mesh):
    cache_spec = P('dp', 'sp', 'tp', None)
    sp_size = mesh.shape['sp']

    def local_step(x_in, cur_pos, w_pre, w_q, w_k, w_v, w_o, w_post, k_cache, v_cache):
        row_count, seq_block, kv_local, head_dim = k_cache.shape
        sp_index = lax.axis_index('sp')
        table = rotary_table(sp_size * seq_block, head_dim)
        q_rot, kn2, vn2 = project(cur_pos, x_in, w_pre.reshape(-1, 128), table, w_q, w_k, w_v)
        base = (sp_index * seq_block).astype(jnp.int32).reshape(1)
        kc = k_cache.reshape(row_count, seq_block * kv_local, head_dim)
        vc = v_cache.reshape(row_count, seq_block * kv_local, head_dim)
        k_out, v_out, *blocks = attend(cur_pos, base, q_rot, kn2, vn2, kc, vc, 4)
        x_out = finish(merge(blocks, w_o, 9), x_in, w_post.reshape(-1, 128))
        return x_out, k_out.reshape(k_cache.shape), v_out.reshape(v_cache.shape)

    return jax.shard_map(local_step, mesh=mesh,
                         in_specs=(P('dp', None), P('dp'), P(None), P(None, 'tp'), P(None, 'tp'), P(None, 'tp'), P('tp', None), P(None), cache_spec, cache_spec),
                         out_specs=(P('dp', None), cache_spec, cache_spec), check_vma=False)
```

```python
import functools

import jax
import jax.numpy as jnp
import numpy as np
from jax import lax
from jax.experimental import pallas as pl
from jax.experimental.pallas import tpu as pltpu
from jax.sharding import PartitionSpec as P


SOFT_CAP = 50.0
ROPE_BASE = 10000.0
NORM_EPS = 1e-6
LOG2E = 1.4426950408889634

ROWS_STEP = 8
SLOTS = 12
AHEAD = 6
START = 2
LAG_SOFT = 2
LAG_OUT = 4


def rotary_table(length, head_dim):
    half_dim = head_dim // 2
    inv_freq = np.power(np.float32(ROPE_BASE), -2.0 * np.arange(half_dim, dtype=np.float32) / np.float32(2 * half_dim)).astype(np.float32)
    angles = np.arange(length, dtype=np.float32)[:, None] * inv_freq[None, :]
    cos_tab = np.cos(angles.astype(np.float64))
    sin_tab = np.sin(angles.astype(np.float64))
    return np.concatenate([cos_tab, cos_tab, -sin_tab, sin_tab], axis=-1).astype(np.float32)


def project_kernel(pos_ref, x_hbm, wpre_ref, table_ref, wq_hbm, wk_hbm, wv_hbm, q_ref, k_ref, v_ref,
                   x_ref, gain_ref, cos_ref, sin_ref, weight, normed, q_part, k_part, v_part, x_sem, w_sem, send_sem, recv_sem,
                   out_sem):
    sp = lax.axis_index('sp')
    core = lax.rem(sp, 2)
    peer = {'sp': sp + 1 - 2 * core}
    mesh_id = pl.DeviceIdType.MESH
    rows = x_ref.shape[0]
    block = weight.shape[2]
    per = block // 128
    plan = []
    for w_hbm, part, turn in ((wq_hbm, q_part, True), (wk_hbm, k_part, True), (wv_hbm, v_part, False)):
        mine = w_hbm.shape[1] // 2
        for j in range(mine // block):
            plan.append((w_hbm, part, turn, mine, j, j == mine // block - 1))

    def load(i):
        w_hbm, _, _, mine, j, _ = plan[i]
        col = pl.multiple_of(core * mine + j * block, block)
        return pltpu.make_async_copy(w_hbm.at[:, pl.ds(col, block)], weight.at[i], w_sem.at[i])

    x_loads = [pltpu.make_async_copy(x_hbm.at[pl.ds(k * (rows // 4), rows // 4)], x_ref.at[pl.ds(k * (rows // 4), rows // 4)],
                                     x_sem.at[k]) for k in range(4)]
    for copy in x_loads:
        copy.start()
    load(0).start()
    barrier = pltpu.get_barrier_semaphore()
    pl.semaphore_signal(barrier, inc=1, device_id=peer, device_id_type=mesh_id)
    pl.semaphore_wait(barrier, 1)

    for j in range(wpre_ref.shape[0]):
        gain_ref[:, j * 128:(j + 1) * 128] = 1.0 + wpre_ref[j:j + 1, :]
    gain = gain_ref[...]

    def look_up(k, carry):
        for r in range(8):
            b = k * 8 + r
            row = table_ref[pl.ds(pos_ref[b], 1), :]
            cos_ref[pl.ds(b, 1), :] = row[:, :128]
            sin_ref[pl.ds(b, 1), :] = row[:, 128:]
        return carry

    lax.fori_loop(0, rows // 8, look_up, 0)

    def norm(k, carry):
        at = pl.ds(pl.multiple_of(k * 32, 32), 32)
        x = x_ref[at, :].astype(jnp.float32)
        inv = lax.rsqrt(jnp.mean(x * x, axis=-1, keepdims=True) + NORM_EPS)
        normed[at, :] = (x * inv * gain).astype(jnp.bfloat16)
        return carry

    for k in range(4):
        x_loads[k].wait()
        if k == 1:
            load(1).start()
        lax.fori_loop(k * rows // 128, (k + 1) * rows // 128, norm, 0)

    outs = ((q_part, q_ref), (k_part, k_ref), (v_part, v_ref))
    sends, writes = [], []
    for i, (_, part, turn, mine, j, done) in enumerate(plan):
        load(i).wait()
        if i + 2 < len(plan):
            load(i + 2).start()
        heads = mine // 128
        acc = jnp.dot(normed[...], weight[i], preferred_element_type=jnp.float32)
        for t in range(per):
            value = acc[:, t * 128:(t + 1) * 128]
            if turn:
                value = value * cos_ref[...] + pltpu.roll(value, 64, 1) * sin_ref[...]
            part[pl.ds(j * per + t, rows, stride=heads), :] = value
        if done:
            n = len(sends)
            copy = pltpu.make_async_remote_copy(src_ref=part, dst_ref=outs[n][1].at[core], send_sem=send_sem.at[n],
                                                recv_sem=recv_sem.at[n], device_id=peer, device_id_type=mesh_id)
            copy.start()
            sends.append(copy)
            out = pltpu.make_async_copy(part, outs[n][1].at[core], out_sem.at[n])
            out.start()
            writes.append(out)
    for copy in sends:
        copy.wait()
    for copy in writes:
        copy.wait()


def project(cur_pos, x_in, w_pre, table, w_q, w_k, w_v):
    rows, width = x_in.shape
    block = 512
    q_cols, kv_cols = w_q.shape[1], w_k.shape[1]
    n_blocks = (q_cols + 2 * kv_cols) // 2 // block
    vmem = pl.BlockSpec(memory_space=pltpu.VMEM)
    hbm = pl.BlockSpec(memory_space=pltpu.HBM)
    f32, bf = jnp.float32, jnp.bfloat16
    dma = pltpu.SemaphoreType.DMA
    return pl.pallas_call(
        project_kernel,
        out_shape=(pltpu.HBM((2, rows * q_cols // 256, 128), f32), pltpu.HBM((2, rows * kv_cols // 256, 128), f32),
                   pltpu.HBM((2, rows * kv_cols // 256, 128), f32)),
        in_specs=[pl.BlockSpec(memory_space=pltpu.SMEM), hbm, vmem, vmem] + [hbm] * 3,
        out_specs=(hbm,) * 3,
        scratch_shapes=[
            pltpu.VMEM((rows, width), bf),
            pltpu.VMEM((1, width), f32),
            pltpu.VMEM((rows, 128), f32),
            pltpu.VMEM((rows, 128), f32),
            pltpu.VMEM((n_blocks, width, block), bf),
            pltpu.VMEM((rows, width), bf),
            pltpu.VMEM((rows * q_cols // 256, 128), f32),
            pltpu.VMEM((rows * kv_cols // 256, 128), f32),
            pltpu.VMEM((rows * kv_cols // 256, 128), f32),
            dma((4,)), dma((n_blocks,)), dma((3,)), dma((3,)), dma((3,)),
        ],
        compiler_params=pltpu.CompilerParams(vmem_limit_bytes=62 * 1024 * 1024, collective_id=1, has_side_effects=True),
        cost_estimate=pl.CostEstimate(flops=rows * width * (q_cols + 2 * kv_cols), bytes_accessed=width * (q_cols + 2 * kv_cols), transcendentals=0),
        name='project',
    )(cur_pos, x_in, w_pre, table, w_q, w_k, w_v)


def attend_kernel(n_steps, quarter, first_row, kv_heads, seq_block, pos_ref, base_ref, q_hbm, kn_hbm, vn_hbm, k_hbm, v_hbm,
                  *rest):
    (ko_hbm, vo_hbm, o0_hbm, o1_hbm, o2_hbm, o3_hbm, m_ref, l_ref, kbuf, vbuf, qbuf, knbuf, vnbuf, obuf, key_ref, s_ref, p_ref, in_sem, out_sem, o_sem, st_sem) = rest[-21:]
    step_rows = ROWS_STEP
    piece_steps = n_steps // 4
    heads, head_dim = m_ref.shape
    q_half, kv_half = heads // 2, kv_heads // 2
    cols = seq_block * kv_heads
    base = base_ref[0]

    row_id = lax.broadcasted_iota(jnp.int32, (heads, cols), 0)
    col_id = lax.broadcasted_iota(jnp.int32, (heads, cols), 1)
    mine = lax.rem(col_id, kv_heads) == row_id // (heads // kv_heads)
    key_ref[...] = jnp.where(mine, col_id, cols * 4)
    lane_id = lax.broadcasted_iota(jnp.int32, m_ref.shape, 1)
    half_id = lax.broadcasted_iota(jnp.int32, (2 * kv_heads, head_dim), 0) // kv_heads

    def row_of(step):
        piece = step // piece_steps
        return piece * quarter + first_row + (step - piece * piece_steps) * step_rows

    def heads_of(step, count):
        return pl.ds(row_of(step) * count, step_rows * count)

    def both_halves(ref, slot, r, count):
        at = slice(r * count, (r + 1) * count)
        return [ref[slot, 0, at, :], ref[slot, 1, at, :]]

    def loads(step, slot):
        rows = pl.ds(row_of(step), step_rows)
        return (pltpu.make_async_copy(k_hbm.at[rows], kbuf.at[slot], in_sem.at[slot, 0]),
                pltpu.make_async_copy(v_hbm.at[rows], vbuf.at[slot], in_sem.at[slot, 1]),
                pltpu.make_async_copy(q_hbm.at[:, heads_of(step, q_half)], qbuf.at[slot], in_sem.at[slot, 2]),
                pltpu.make_async_copy(kn_hbm.at[:, heads_of(step, kv_half)], knbuf.at[slot], in_sem.at[slot, 3]),
                pltpu.make_async_copy(vn_hbm.at[:, heads_of(step, kv_half)], vnbuf.at[slot], in_sem.at[slot, 4]))

    def stores(step, slot):
        rows = pl.ds(row_of(step), step_rows)
        return (pltpu.make_async_copy(kbuf.at[slot], ko_hbm.at[rows], out_sem.at[slot, 0]),
                pltpu.make_async_copy(vbuf.at[slot], vo_hbm.at[rows], out_sem.at[slot, 1]))

    def o_store(step, slot, d=0):
        at = pl.ds((step - step // piece_steps * piece_steps) * step_rows * heads, step_rows * heads)
        o_hbm = (o0_hbm, o1_hbm, o2_hbm, o3_hbm)[d]
        return pltpu.make_async_copy(obuf.at[slot], o_hbm.at[at], o_sem.at[slot])

    def o_start(step, slot):
        turn = jnp.bitwise_xor(step // piece_steps, base // seq_block)
        for d in range(4):
            @pl.when(turn == d)
            def _():
                o_store(step, slot, d).start()

    for step in range(min(START, n_steps)):
        for copy in loads(step, step):
            copy.start()
    m_ref[...] = jnp.zeros_like(m_ref)
    l_ref[...] = jnp.zeros_like(l_ref)
    scale = head_dim ** -0.5 / SOFT_CAP

    def body(step, carry):
        slot = lax.rem(step, SLOTS)
        oslot = lax.rem(step, 2)
        for copy in loads(step, slot):
            copy.wait()
        issued = jnp.minimum(step + AHEAD, START + 2 * step)
        wanted = jnp.minimum(jnp.minimum(step + 1 + AHEAD, START + 2 * step + 2), n_steps)
        for extra in range(2):
            nxt = issued + extra

            @pl.when(nxt < wanted)
            def _():
                nslot = lax.rem(nxt, SLOTS)

                @pl.when(nxt >= SLOTS)
                def _():
                    for copy in stores(nxt - SLOTS, nslot):
                        copy.wait()

                for copy in loads(nxt, nslot):
                    copy.start()

        for r in range(step_rows):
            local = pos_ref[row_of(step) + r] - base
            inside = (local >= 0) & (local < seq_block)
            at = jnp.clip(local, 0, seq_block - 1)
            pair = pl.ds(pl.multiple_of((at // 2) * (2 * kv_heads), 2 * kv_heads), 2 * kv_heads)
            hit = half_id == jnp.where(inside, lax.rem(at, 2), 2)
            k_row = jnp.concatenate(both_halves(knbuf, slot, r, kv_half) * 2, axis=0).astype(jnp.bfloat16)
            v_row = jnp.concatenate(both_halves(vnbuf, slot, r, kv_half) * 2, axis=0).astype(jnp.bfloat16)
            kbuf[slot, r, pair, :] = jnp.where(hit, k_row, kbuf[slot, r, pair, :])
            vbuf[slot, r, pair, :] = jnp.where(hit, v_row, vbuf[slot, r, pair, :])

        @pl.when(step >= 2)
        def _():
            o_store(step - 2, oslot).wait()

        m_all = m_ref[...]
        l_all = l_ref[...]
        half = cols // 2
        for tick in range(step_rows + LAG_OUT):
            r = tick
            if r < step_rows:
                q_row = jnp.concatenate(both_halves(qbuf, slot, r, q_half), axis=0).astype(jnp.bfloat16)
                raw = lax.dot_general(q_row, kbuf[slot, r], (((1,), (1,)), ((), ())),
                                      preferred_element_type=jnp.float32)
                s_ref[r] = raw
            r = tick - LAG_SOFT
            if 0 <= r < step_rows:
                local = pos_ref[row_of(step) + r] - base
                seen = key_ref[...] < (local + 1) * kv_heads
                soft = jnp.where(seen, jnp.tanh(s_ref[r] * scale), -4.0)
                top = jnp.maximum(jnp.max(soft, axis=-1, keepdims=True), -1.0)
                weight = jnp.exp2((soft - top) * (SOFT_CAP * LOG2E))
                total = jnp.sum(weight, axis=-1, keepdims=True)
                weight = weight.astype(jnp.bfloat16)
                p_ref[r, :heads] = weight[:, :half]
                p_ref[r, heads:] = weight[:, half:]
                here = lane_id == step * step_rows + r
                m_all = jnp.where(here, top * SOFT_CAP, m_all)
                l_all = jnp.where(here, total, l_all)
            r = tick - LAG_OUT
            if 0 <= r < step_rows:
                right = jnp.concatenate([vbuf[slot, r, :half, :], vbuf[slot, r, half:, :]], axis=1)
                both = jnp.dot(p_ref[r], right, preferred_element_type=jnp.float32)
                obuf[oslot, r * heads:(r + 1) * heads, :] = both[:heads, :head_dim] + both[heads:, head_dim:]
        m_ref[...] = m_all
        l_ref[...] = l_all
        o_start(step, oslot)
        for copy in stores(step, slot):
            copy.start()

        return carry

    lax.fori_loop(0, n_steps, body, 0)
    tail = piece_steps * step_rows * heads
    stat_copies = []
    for d, o_hbm in enumerate((o0_hbm, o1_hbm, o2_hbm, o3_hbm)):
        stat_copies.append(pltpu.make_async_copy(m_ref, o_hbm.at[pl.ds(tail, heads)], st_sem.at[d, 0]))
        stat_copies.append(pltpu.make_async_copy(l_ref, o_hbm.at[pl.ds(tail + heads, heads)], st_sem.at[d, 1]))
    for copy in stat_copies:
        copy.start()
    for copy in stat_copies:
        copy.wait()
    for step in range(max(0, n_steps - SLOTS), n_steps):
        for copy in stores(step, step % SLOTS):
            copy.wait()
    for step in range(max(0, n_steps - 2), n_steps):
        o_store(step, step % 2).wait()


def attend(pos, base, q, kn, vn, k_cache, v_cache, prev, first_row, n_rows):
    rows, cols, head_dim = k_cache.shape
    heads = 2 * q.shape[1] // rows
    kv_heads = 2 * kn.shape[1] // rows
    seq_block = cols // kv_heads
    n_steps = n_rows // ROWS_STEP
    hbm = pl.BlockSpec(memory_space=pl.ANY)
    piece = pltpu.HBM((n_rows // 4 * heads + 2 * heads, head_dim), jnp.float32)
    smem = pl.BlockSpec(memory_space=pltpu.SMEM)
    bf = jnp.bfloat16
    aliases = {} if prev is None else {7: 0, 8: 1}
    extra = () if prev is None else tuple(prev)
    return pl.pallas_call(
        functools.partial(attend_kernel, n_steps, rows // 4, first_row, kv_heads, seq_block),
        out_shape=(jax.ShapeDtypeStruct(k_cache.shape, bf), jax.ShapeDtypeStruct(v_cache.shape, bf)) + (piece,) * 4,
        in_specs=[smem, smem, hbm, hbm, hbm, hbm, hbm] + [hbm] * len(extra),
        out_specs=(hbm, hbm) + (pl.BlockSpec(memory_space=pltpu.HBM),) * 4,
        scratch_shapes=[
            pltpu.VMEM((heads, 128), jnp.float32),
            pltpu.VMEM((heads, 128), jnp.float32),
            pltpu.VMEM((SLOTS, ROWS_STEP, cols, head_dim), bf),
            pltpu.VMEM((SLOTS, ROWS_STEP, cols, head_dim), bf),
            pltpu.VMEM((SLOTS, 2, ROWS_STEP * heads // 2, head_dim), jnp.float32),
            pltpu.VMEM((SLOTS, 2, ROWS_STEP * kv_heads // 2, head_dim), jnp.float32),
            pltpu.VMEM((SLOTS, 2, ROWS_STEP * kv_heads // 2, head_dim), jnp.float32),
            pltpu.VMEM((2, ROWS_STEP * heads, head_dim), jnp.float32),
            pltpu.VMEM((heads, cols), jnp.int32),
            pltpu.VMEM((ROWS_STEP, heads, cols), jnp.float32),
            pltpu.VMEM((ROWS_STEP, 2 * heads, cols // 2), bf),
            pltpu.SemaphoreType.DMA((SLOTS, 5)),
            pltpu.SemaphoreType.DMA((SLOTS, 2)),
            pltpu.SemaphoreType.DMA((2,)),
            pltpu.SemaphoreType.DMA((4, 2)),
        ],
        input_output_aliases=aliases,
        compiler_params=pltpu.CompilerParams(vmem_limit_bytes=62 * 1024 * 1024),
        cost_estimate=pl.CostEstimate(flops=n_rows * heads * cols * head_dim * 4,
                                      bytes_accessed=n_rows * cols * head_dim * 8, transcendentals=0),
        name='attend',
    )(pos, base, q, kn, vn, k_cache, v_cache, *extra)


def merge_kernel(chunks, *refs):
    n_in = 4 * len(chunks)
    source = [refs[4 * c:4 * c + 4] for c in range(len(chunks))]
    pieces = [[b.at[d] for d in range(4)] for b in refs[-len(chunks):]]
    refs = refs[:-len(chunks)]
    (wo_hbm, sums, wo, last_in, last_out, osum, lhs, y_out, y_in,
     p_sem, w_sem, o_send, o_recv, y_send, y_recv, g_send, g_recv, d_send, d_recv, f_send, f_recv) = refs[n_in:]
    sp = lax.axis_index('sp')
    tp = lax.axis_index('tp')
    core = lax.rem(sp, 2)
    xpos = sp // 2
    n_chunks, _, chunk = y_out.shape
    heads = lhs.shape[1] // 128
    parts = [c // 4 for c in chunks]
    core_id = 2 * xpos + (1 - core)
    x_id = 2 * (1 - xpos) + core
    core_peer, x_peer, y_peer = {'sp': core_id}, {'sp': x_id}, {'tp': 1 - tp}
    mesh_id = pl.DeviceIdType.MESH

    def remote(src, dst, send, recv, peer):
        return pltpu.make_async_remote_copy(src_ref=src, dst_ref=dst, send_sem=send, recv_sem=recv,
                                            device_id=peer, device_id_type=mesh_id)

    def w_load(n):
        return pltpu.make_async_copy(wo_hbm.at[:, pl.ds(n * chunk, chunk)], wo.at[n], w_sem.at[n])

    local = [[pltpu.make_async_copy(source[c][d], pieces[c][d], p_sem.at[c, d]) for d in range(4)] for c in range(len(chunks))]
    for copy in local[-1]:
        copy.start()
    barrier = pltpu.get_barrier_semaphore()
    for peer in (core_peer, x_peer, y_peer):
        pl.semaphore_signal(barrier, inc=1, device_id=peer, device_id_type=mesh_id)
    pl.semaphore_wait(barrier, 3)

    for copy in local[-1]:
        copy.wait()
    last = [remote(pieces[-1][3], last_in.at[0], o_send.at[0], o_recv.at[0], core_peer),
            remote(pieces[-1][1], last_in.at[1], o_send.at[1], o_recv.at[1], core_peer),
            remote(last_out, last_in.at[2], o_send.at[2], o_recv.at[2], x_peer)]
    last[0].start()
    last[1].start()
    for copy in local[0]:
        copy.start()
    for n in range(3):
        w_load(n).start()

    def shares(blocks, part):
        count = part * heads
        stats = [block[count:count + 2 * heads, :] for block in blocks]
        top = functools.reduce(jnp.maximum, [st[:heads] for st in stats])
        grown = [jnp.exp(st[:heads] - top) for st in stats]
        return top, sum(st[heads:] * g for st, g in zip(stats, grown)), grown

    def mix(blocks, weights, owner, part, out):
        shift = lax.rem(128 - owner * part, 128)
        factors = [pltpu.roll(w, shift, 1) for w in weights]
        for b in range(part):
            at = slice(b * heads, (b + 1) * heads)
            out[at, :] = sum(block[at, :] * f[:, b:b + 1] for block, f in zip(blocks, factors))

    def combine(blocks, part, row0):
        _, total, grown = shares(blocks, part)
        mix(blocks, [g / total for g in grown], sp, part, osum)
        for h in range(heads):
            lhs[row0:row0 + part, h * 128:(h + 1) * 128] = osum[pl.ds(h, part, stride=heads), :].astype(jnp.bfloat16)

    last[0].wait_recv()
    pair = [pieces[-1][2], last_in.at[0]]
    top, total, grown = shares(pair, parts[-1])
    mix(pair, grown, x_id, parts[-1], last_out)
    count = parts[-1] * heads
    last_out[count:count + heads, :] = top
    last_out[count + heads:count + 2 * heads, :] = total
    last[2].start()

    for copy in local[0]:
        copy.wait()
    combine(pieces[0], parts[0], 0)

    sizes = (2, 2, 2, 2, 1)
    order = []
    for c, part in enumerate(parts):
        begin = 0
        for size in sizes:
            order.append((pl.ds(begin, size), pl.ds(sum(parts[:c]), part), range(begin, begin + size)))
            begin += size
    n_pieces = len(order)
    n_first = len(sizes)

    def to_y(t):
        ns, r, _ = order[t]
        return remote(y_out.at[ns, r], y_in.at[ns, r], y_send.at[t], y_recv.at[t], y_peer)

    def gather(t, owner, send, recv, peer):
        ns, r, _ = order[t]
        return remote(sums.at[owner, ns, r], sums.at[owner, ns, r], send.at[t], recv.at[t], peer)

    def to_x(t):
        return gather(t, sp, g_send, g_recv, x_peer)

    def to_core(t):
        return gather(t, sp, d_send, d_recv, core_peer)

    def relay(t):
        return gather(t, x_id, f_send, f_recv, core_peer)

    def project_rows(n, r0, count):
        y_out[n, r0:r0 + count, :] = jnp.dot(lhs[r0:r0 + count, :], wo[n], preferred_element_type=jnp.float32)

    for t in range(n_first):
        for n in order[t][2]:
            w_load(n).wait()
            if n + 3 < n_chunks:
                w_load(n + 3).start()
            project_rows(n, 0, parts[0])
        to_y(t).start()

    for t in range(n_pieces + 3):
        if t == 2:
            for copy in last[1:]:
                copy.wait_recv()
            combine([pieces[-1][0], last_in.at[1], last_in.at[2]], parts[-1], parts[0])
        if 2 <= t < 2 + n_first:
            for n in order[n_first + t - 2][2]:
                project_rows(n, parts[0], parts[-1])
            to_y(n_first + t - 2).start()
        if t < n_pieces:
            ns, r, _ = order[t]
            to_y(t).wait()
            sums[sp, ns, r, :] = y_out[ns, r, :] + y_in[ns, r, :]
            to_x(t).start()
            to_core(t).start()
        if 1 <= t < n_pieces + 1:
            to_x(t - 1).wait_recv()
            relay(t - 1).start()
        if t >= 3:
            to_core(t - 3).wait_recv()
            relay(t - 3).wait_recv()
    for copy in last:
        copy.wait_send()
    for t in range(n_pieces):
        to_x(t).wait_send()
        to_core(t).wait_send()
        relay(t).wait_send()


def merge(chunks, pieces, w_o, n_chunks):
    inner, width = w_o.shape
    heads = inner // 128
    quarter = sum(chunks) // 4
    chunk = width // n_chunks
    hbm = pl.BlockSpec(memory_space=pltpu.HBM)
    f32 = jnp.float32
    dma = pltpu.SemaphoreType.DMA
    flat = [p if 0 < d and c < len(chunks) - 1 else pltpu.with_memory_space_constraint(p, pltpu.HBM)
            for c, piece in enumerate(pieces) for d, p in enumerate(piece)]
    block = pieces[-1][0].shape
    return pl.pallas_call(
        functools.partial(merge_kernel, chunks),
        out_shape=jax.ShapeDtypeStruct((4, n_chunks, quarter, chunk), f32),
        in_specs=[hbm] * (len(flat) + 1),
        out_specs=pl.BlockSpec(memory_space=pltpu.VMEM),
        scratch_shapes=[
            pltpu.VMEM((n_chunks, inner, chunk), jnp.bfloat16),
            pltpu.VMEM((3,) + block, f32),
            pltpu.VMEM(block, f32),
            pltpu.VMEM((max(chunks) // 4 * heads, 128), f32),
            pltpu.VMEM((quarter, inner), jnp.bfloat16),
            pltpu.VMEM((n_chunks, quarter, chunk), f32),
            pltpu.VMEM((n_chunks, quarter, chunk), f32),
            dma((len(chunks), 4)), dma((n_chunks,)), dma((3,)), dma((3,)),
        ] + [dma((10,))] * 8 + [pltpu.VMEM((4,) + piece[0].shape, f32) for piece in pieces],
        compiler_params=pltpu.CompilerParams(vmem_limit_bytes=40 * 1024 * 1024, collective_id=0, has_side_effects=True),
        cost_estimate=pl.CostEstimate(flops=2 * quarter * inner * width, bytes_accessed=2 * inner * width, transcendentals=0),
        name='merge',
    )(*flat, pltpu.with_memory_space_constraint(w_o, pltpu.HBM))


def finish_kernel(sums, xbuf, wpost_ref, out_hbm, gain_ref, obuf, out_sem):
    parts, n_chunks, rows, chunk = sums.shape

    def store(q):
        at = pl.ds(q * rows, rows)
        return pltpu.make_async_copy(obuf.at[at], out_hbm.at[at], out_sem.at[q])

    for j in range(wpost_ref.shape[0]):
        gain_ref[:, j * 128:(j + 1) * 128] = 1.0 + wpost_ref[j:j + 1, :]
    for q in range(parts):
        for k in range(rows // 16):
            at = slice(k * 16, (k + 1) * 16)
            to = slice(q * rows + k * 16, q * rows + (k + 1) * 16)
            square = jnp.zeros((16, chunk), jnp.float32)
            for n in range(n_chunks):
                u = sums[q, n, at, :]
                square = square + u * u
            inv = lax.rsqrt(jnp.sum(square, axis=-1, keepdims=True) * (1.0 / (n_chunks * chunk)) + NORM_EPS)
            for n in range(n_chunks):
                col = slice(n * chunk, (n + 1) * chunk)
                y = xbuf[to, col].astype(jnp.float32) + sums[q, n, at, :] * inv * gain_ref[:, col]
                obuf[to, col] = y.astype(jnp.bfloat16)
        store(q).start()
    for q in range(parts):
        store(q).wait()


def finish(sums, x_in, w_post):
    parts = sums.shape[0]
    hbm = pl.BlockSpec(memory_space=pltpu.HBM)
    dma = pltpu.SemaphoreType.DMA
    return pl.pallas_call(
        finish_kernel,
        out_shape=jax.ShapeDtypeStruct(x_in.shape, x_in.dtype),
        in_specs=[pl.BlockSpec(memory_space=pltpu.VMEM)] * 3,
        out_specs=hbm,
        scratch_shapes=[pltpu.VMEM((1, x_in.shape[1]), jnp.float32), pltpu.VMEM(x_in.shape, x_in.dtype), dma((parts,))],
        compiler_params=pltpu.CompilerParams(vmem_limit_bytes=24 * 1024 * 1024),
        name='finish',
    )(sums, x_in, w_post)


def solution(mesh):
    cache_spec = P('dp', 'sp', 'tp', None)
    sp_size = mesh.shape['sp']

    def local_step(x_in, cur_pos, w_pre, w_q, w_k, w_v, w_o, w_post, k_cache, v_cache):
        row_count, seq_block, kv_local, head_dim = k_cache.shape
        sp_index = lax.axis_index('sp')
        table = rotary_table(sp_size * seq_block, head_dim)
        q_rot, kn2, vn2 = project(cur_pos, x_in, w_pre.reshape(-1, 128), table, w_q, w_k, w_v)
        base = (sp_index * seq_block).astype(jnp.int32).reshape(1)
        kc = k_cache.reshape(row_count, seq_block * kv_local, head_dim)
        vc = v_cache.reshape(row_count, seq_block * kv_local, head_dim)
        chunks = (row_count // 2, row_count // 2)
        prev, first_row, pieces = None, 0, []
        for index, n_rows in enumerate(chunks):
            *prev, p0, p1, p2, p3 = attend(cur_pos, base, q_rot, kn2, vn2, kc, vc, prev, first_row, n_rows)
            first_row += n_rows // 4
            if index < len(chunks) - 1:
                moved = []
                for d, p in ((1, p1), (2, p2), (3, p3)):
                    moved.append(lax.ppermute(p, 'sp', [(i, i ^ d) for i in range(sp_size)]))
                p1, p2, p3 = moved
            pieces.append((p0, p1, p2, p3))
        k_out, v_out = prev
        x_out = finish(merge(chunks, pieces, w_o, 9), x_in, w_post.reshape(-1, 128))
        return x_out, k_out.reshape(k_cache.shape), v_out.reshape(v_cache.shape)

    return jax.shard_map(local_step, mesh=mesh,
                         in_specs=(P('dp', None), P('dp'), P(None), P(None, 'tp'), P(None, 'tp'), P(None, 'tp'), P('tp', None), P(None), cache_spec, cache_spec),
                         out_specs=(P('dp', None), cache_spec, cache_spec), check_vma=False)
```

```python
import functools

import jax
import jax.numpy as jnp
import numpy as np
from jax import lax
from jax.experimental import pallas as pl
from jax.experimental.pallas import tpu as pltpu
from jax.sharding import PartitionSpec as P


SOFT_CAP = 50.0
ROPE_BASE = 10000.0
NORM_EPS = 1e-6
LOG2E = 1.4426950408889634

ROWS_STEP = 8
SLOTS = 9
AHEAD = 5
START = 5
LAG_SOFT = 2
LAG_OUT = 4


def rotary_table(length, head_dim):
    half_dim = head_dim // 2
    inv_freq = np.power(np.float32(ROPE_BASE), -2.0 * np.arange(half_dim, dtype=np.float32) / np.float32(2 * half_dim)).astype(np.float32)
    angles = np.arange(length, dtype=np.float32)[:, None] * inv_freq[None, :]
    cos_tab = np.cos(angles.astype(np.float64))
    sin_tab = np.sin(angles.astype(np.float64))
    return np.concatenate([cos_tab, cos_tab, -sin_tab, sin_tab], axis=-1).astype(np.float32)


def project_kernel(pos_ref, x_hbm, wpre_ref, table_ref, wq_hbm, wk_hbm, wv_hbm, q_ref, k_ref, v_ref,
                   x_ref, gain_ref, cos_ref, sin_ref, weight, normed, q_part, k_part, v_part, x_sem, w_sem, send_sem, recv_sem,
                   out_sem):
    sp = lax.axis_index('sp')
    core = lax.rem(sp, 2)
    peer = {'sp': sp + 1 - 2 * core}
    mesh_id = pl.DeviceIdType.MESH
    rows = x_ref.shape[0]
    block = weight.shape[2]
    per = block // 128
    plan = []
    for w_hbm, part, turn in ((wq_hbm, q_part, True), (wk_hbm, k_part, True), (wv_hbm, v_part, False)):
        mine = w_hbm.shape[1] // 2
        for j in range(mine // block):
            plan.append((w_hbm, part, turn, mine, j, j == mine // block - 1))

    def load(i):
        w_hbm, _, _, mine, j, _ = plan[i]
        col = pl.multiple_of(core * mine + j * block, block)
        return pltpu.make_async_copy(w_hbm.at[:, pl.ds(col, block)], weight.at[i], w_sem.at[i])

    x_loads = [pltpu.make_async_copy(x_hbm.at[pl.ds(k * (rows // 4), rows // 4)], x_ref.at[pl.ds(k * (rows // 4), rows // 4)],
                                     x_sem.at[k]) for k in range(4)]
    for copy in x_loads:
        copy.start()
    load(0).start()
    barrier = pltpu.get_barrier_semaphore()
    pl.semaphore_signal(barrier, inc=1, device_id=peer, device_id_type=mesh_id)
    pl.semaphore_wait(barrier, 1)

    for j in range(wpre_ref.shape[0]):
        gain_ref[:, j * 128:(j + 1) * 128] = 1.0 + wpre_ref[j:j + 1, :]
    gain = gain_ref[...]

    def look_up(k, carry):
        for r in range(8):
            b = k * 8 + r
            row = table_ref[pl.ds(pos_ref[b], 1), :]
            cos_ref[pl.ds(b, 1), :] = row[:, :128]
            sin_ref[pl.ds(b, 1), :] = row[:, 128:]
        return carry

    lax.fori_loop(0, rows // 8, look_up, 0)

    def norm(k, carry):
        at = pl.ds(pl.multiple_of(k * 32, 32), 32)
        x = x_ref[at, :].astype(jnp.float32)
        inv = lax.rsqrt(jnp.mean(x * x, axis=-1, keepdims=True) + NORM_EPS)
        normed[at, :] = (x * inv * gain).astype(jnp.bfloat16)
        return carry

    for k in range(4):
        x_loads[k].wait()
        if k == 1:
            load(1).start()
        lax.fori_loop(k * rows // 128, (k + 1) * rows // 128, norm, 0)

    outs = ((q_part, q_ref), (k_part, k_ref), (v_part, v_ref))
    sends, writes = [], []
    for i, (_, part, turn, mine, j, done) in enumerate(plan):
        load(i).wait()
        if i + 2 < len(plan):
            load(i + 2).start()
        heads = mine // 128
        acc = jnp.dot(normed[...], weight[i], preferred_element_type=jnp.float32)
        for t in range(per):
            value = acc[:, t * 128:(t + 1) * 128]
            if turn:
                value = value * cos_ref[...] + pltpu.roll(value, 64, 1) * sin_ref[...]
            part[pl.ds(j * per + t, rows, stride=heads), :] = value
        if done:
            n = len(sends)
            copy = pltpu.make_async_remote_copy(src_ref=part, dst_ref=outs[n][1].at[core], send_sem=send_sem.at[n],
                                                recv_sem=recv_sem.at[n], device_id=peer, device_id_type=mesh_id)
            copy.start()
            sends.append(copy)
            out = pltpu.make_async_copy(part, outs[n][1].at[core], out_sem.at[n])
            out.start()
            writes.append(out)
    for copy in sends:
        copy.wait()
    for copy in writes:
        copy.wait()


def project(cur_pos, x_in, w_pre, table, w_q, w_k, w_v):
    rows, width = x_in.shape
    block = 512
    q_cols, kv_cols = w_q.shape[1], w_k.shape[1]
    n_blocks = (q_cols + 2 * kv_cols) // 2 // block
    vmem = pl.BlockSpec(memory_space=pltpu.VMEM)
    hbm = pl.BlockSpec(memory_space=pltpu.HBM)
    f32, bf = jnp.float32, jnp.bfloat16
    dma = pltpu.SemaphoreType.DMA
    return pl.pallas_call(
        project_kernel,
        out_shape=(pltpu.HBM((2, rows * q_cols // 256, 128), f32), pltpu.HBM((2, rows * kv_cols // 256, 128), f32),
                   pltpu.HBM((2, rows * kv_cols // 256, 128), f32)),
        in_specs=[pl.BlockSpec(memory_space=pltpu.SMEM), hbm, vmem, vmem] + [hbm] * 3,
        out_specs=(hbm,) * 3,
        scratch_shapes=[
            pltpu.VMEM((rows, width), bf),
            pltpu.VMEM((1, width), f32),
            pltpu.VMEM((rows, 128), f32),
            pltpu.VMEM((rows, 128), f32),
            pltpu.VMEM((n_blocks, width, block), bf),
            pltpu.VMEM((rows, width), bf),
            pltpu.VMEM((rows * q_cols // 256, 128), f32),
            pltpu.VMEM((rows * kv_cols // 256, 128), f32),
            pltpu.VMEM((rows * kv_cols // 256, 128), f32),
            dma((4,)), dma((n_blocks,)), dma((3,)), dma((3,)), dma((3,)),
        ],
        compiler_params=pltpu.CompilerParams(vmem_limit_bytes=62 * 1024 * 1024, collective_id=1, has_side_effects=True),
        cost_estimate=pl.CostEstimate(flops=rows * width * (q_cols + 2 * kv_cols), bytes_accessed=width * (q_cols + 2 * kv_cols), transcendentals=0),
        name='project',
    )(cur_pos, x_in, w_pre, table, w_q, w_k, w_v)


def attend_kernel(n_steps, quarter, first_row, kv_heads, seq_block, pos_ref, base_ref, q_hbm, kn_hbm, vn_hbm, k_hbm, v_hbm,
                  *rest):
    (ko_hbm, vo_hbm, o0_hbm, o1_hbm, o2_hbm, o3_hbm, m_ref, l_ref, kbuf, vbuf, qbuf, knbuf, vnbuf, obuf, key_ref, s_ref, p_ref, in_sem, out_sem, o_sem, st_sem) = rest[-21:]
    step_rows = ROWS_STEP
    piece_steps = n_steps // 4
    heads, head_dim = m_ref.shape
    q_half, kv_half = heads // 2, kv_heads // 2
    cols = seq_block * kv_heads
    base = base_ref[0]

    row_id = lax.broadcasted_iota(jnp.int32, (heads, cols), 0)
    col_id = lax.broadcasted_iota(jnp.int32, (heads, cols), 1)
    mine = lax.rem(col_id, kv_heads) == row_id // (heads // kv_heads)
    key_ref[...] = jnp.where(mine, col_id, cols * 4)
    lane_id = lax.broadcasted_iota(jnp.int32, m_ref.shape, 1)
    half_id = lax.broadcasted_iota(jnp.int32, (2 * kv_heads, head_dim), 0) // kv_heads

    def row_of(step):
        piece = step // piece_steps
        return piece * quarter + first_row + (step - piece * piece_steps) * step_rows

    def heads_of(step, count):
        return pl.ds(row_of(step) * count, step_rows * count)

    def both_halves(ref, slot, r, count):
        at = slice(r * count, (r + 1) * count)
        return [ref[slot, 0, at, :], ref[slot, 1, at, :]]

    def loads(step, slot):
        rows = pl.ds(row_of(step), step_rows)
        return (pltpu.make_async_copy(k_hbm.at[rows], kbuf.at[slot], in_sem.at[slot, 0]),
                pltpu.make_async_copy(v_hbm.at[rows], vbuf.at[slot], in_sem.at[slot, 1]),
                pltpu.make_async_copy(q_hbm.at[:, heads_of(step, q_half)], qbuf.at[slot], in_sem.at[slot, 2]),
                pltpu.make_async_copy(kn_hbm.at[:, heads_of(step, kv_half)], knbuf.at[slot], in_sem.at[slot, 3]),
                pltpu.make_async_copy(vn_hbm.at[:, heads_of(step, kv_half)], vnbuf.at[slot], in_sem.at[slot, 4]))

    def stores(step, slot):
        rows = pl.ds(row_of(step), step_rows)
        return (pltpu.make_async_copy(kbuf.at[slot], ko_hbm.at[rows], out_sem.at[slot, 0]),
                pltpu.make_async_copy(vbuf.at[slot], vo_hbm.at[rows], out_sem.at[slot, 1]))

    def o_store(step, slot, d=0):
        at = pl.ds((step - step // piece_steps * piece_steps) * step_rows * heads, step_rows * heads)
        o_hbm = (o0_hbm, o1_hbm, o2_hbm, o3_hbm)[d]
        return pltpu.make_async_copy(obuf.at[slot], o_hbm.at[at], o_sem.at[slot])

    def o_start(step, slot):
        turn = jnp.bitwise_xor(step // piece_steps, base // seq_block)
        for d in range(4):
            @pl.when(turn == d)
            def _():
                o_store(step, slot, d).start()

    for step in range(min(START, n_steps)):
        for copy in loads(step, step):
            copy.start()
    m_ref[...] = jnp.zeros_like(m_ref)
    l_ref[...] = jnp.zeros_like(l_ref)
    scale = head_dim ** -0.5 / SOFT_CAP

    def body(step, carry):
        slot = lax.rem(step, SLOTS)
        oslot = lax.rem(step, 2)
        for copy in loads(step, slot):
            copy.wait()
        issued = jnp.minimum(step + AHEAD, START + 2 * step)
        wanted = jnp.minimum(jnp.minimum(step + 1 + AHEAD, START + 2 * step + 2), n_steps)
        for extra in range(2):
            nxt = issued + extra

            @pl.when(nxt < wanted)
            def _():
                nslot = lax.rem(nxt, SLOTS)

                @pl.when(nxt >= SLOTS)
                def _():
                    for copy in stores(nxt - SLOTS, nslot):
                        copy.wait()

                for copy in loads(nxt, nslot):
                    copy.start()

        for r in range(step_rows):
            local = pos_ref[row_of(step) + r] - base
            inside = (local >= 0) & (local < seq_block)
            at = jnp.clip(local, 0, seq_block - 1)
            pair = pl.ds(pl.multiple_of((at // 2) * (2 * kv_heads), 2 * kv_heads), 2 * kv_heads)
            hit = half_id == jnp.where(inside, lax.rem(at, 2), 2)
            k_row = jnp.concatenate(both_halves(knbuf, slot, r, kv_half) * 2, axis=0).astype(jnp.bfloat16)
            v_row = jnp.concatenate(both_halves(vnbuf, slot, r, kv_half) * 2, axis=0).astype(jnp.bfloat16)
            kbuf[slot, r, pair, :] = jnp.where(hit, k_row, kbuf[slot, r, pair, :])
            vbuf[slot, r, pair, :] = jnp.where(hit, v_row, vbuf[slot, r, pair, :])

        @pl.when(step >= 2)
        def _():
            o_store(step - 2, oslot).wait()

        m_all = m_ref[...]
        l_all = l_ref[...]
        half = cols // 2
        for tick in range(step_rows + LAG_OUT):
            r = tick
            if r < step_rows:
                q_row = jnp.concatenate(both_halves(qbuf, slot, r, q_half), axis=0).astype(jnp.bfloat16)
                raw = lax.dot_general(q_row, kbuf[slot, r], (((1,), (1,)), ((), ())),
                                      preferred_element_type=jnp.float32)
                s_ref[r] = raw
            r = tick - LAG_SOFT
            if 0 <= r < step_rows:
                local = pos_ref[row_of(step) + r] - base
                seen = key_ref[...] < (local + 1) * kv_heads
                soft = jnp.where(seen, jnp.tanh(s_ref[r] * scale), -4.0)
                top = jnp.maximum(jnp.max(soft, axis=-1, keepdims=True), -1.0)
                weight = jnp.exp2((soft - top) * (SOFT_CAP * LOG2E))
                total = jnp.sum(weight, axis=-1, keepdims=True)
                weight = weight.astype(jnp.bfloat16)
                p_ref[r, :heads] = weight[:, :half]
                p_ref[r, heads:] = weight[:, half:]
                here = lane_id == step * step_rows + r
                m_all = jnp.where(here, top * SOFT_CAP, m_all)
                l_all = jnp.where(here, total, l_all)
            r = tick - LAG_OUT
            if 0 <= r < step_rows:
                right = jnp.concatenate([vbuf[slot, r, :half, :], vbuf[slot, r, half:, :]], axis=1)
                both = jnp.dot(p_ref[r], right, preferred_element_type=jnp.float32)
                obuf[oslot, r * heads:(r + 1) * heads, :] = both[:heads, :head_dim] + both[heads:, head_dim:]
        m_ref[...] = m_all
        l_ref[...] = l_all
        o_start(step, oslot)
        for copy in stores(step, slot):
            copy.start()

        return carry

    lax.fori_loop(0, n_steps, body, 0)
    tail = piece_steps * step_rows * heads
    stat_copies = []
    for d, o_hbm in enumerate((o0_hbm, o1_hbm, o2_hbm, o3_hbm)):
        stat_copies.append(pltpu.make_async_copy(m_ref, o_hbm.at[pl.ds(tail, heads)], st_sem.at[d, 0]))
        stat_copies.append(pltpu.make_async_copy(l_ref, o_hbm.at[pl.ds(tail + heads, heads)], st_sem.at[d, 1]))
    for copy in stat_copies:
        copy.start()
    for copy in stat_copies:
        copy.wait()
    for step in range(max(0, n_steps - SLOTS), n_steps):
        for copy in stores(step, step % SLOTS):
            copy.wait()
    for step in range(max(0, n_steps - 2), n_steps):
        o_store(step, step % 2).wait()


def attend(pos, base, q, kn, vn, k_cache, v_cache, prev, first_row, n_rows):
    rows, cols, head_dim = k_cache.shape
    heads = 2 * q.shape[1] // rows
    kv_heads = 2 * kn.shape[1] // rows
    seq_block = cols // kv_heads
    n_steps = n_rows // ROWS_STEP
    hbm = pl.BlockSpec(memory_space=pl.ANY)
    piece = pltpu.HBM((n_rows // 4 * heads + 2 * heads, head_dim), jnp.float32)
    smem = pl.BlockSpec(memory_space=pltpu.SMEM)
    bf = jnp.bfloat16
    aliases = {} if prev is None else {7: 0, 8: 1}
    extra = () if prev is None else tuple(prev)
    return pl.pallas_call(
        functools.partial(attend_kernel, n_steps, rows // 4, first_row, kv_heads, seq_block),
        out_shape=(jax.ShapeDtypeStruct(k_cache.shape, bf), jax.ShapeDtypeStruct(v_cache.shape, bf)) + (piece,) * 4,
        in_specs=[smem, smem, hbm, hbm, hbm, hbm, hbm] + [hbm] * len(extra),
        out_specs=(hbm, hbm) + (pl.BlockSpec(memory_space=pltpu.HBM),) * 4,
        scratch_shapes=[
            pltpu.VMEM((heads, 128), jnp.float32),
            pltpu.VMEM((heads, 128), jnp.float32),
            pltpu.VMEM((SLOTS, ROWS_STEP, cols, head_dim), bf),
            pltpu.VMEM((SLOTS, ROWS_STEP, cols, head_dim), bf),
            pltpu.VMEM((SLOTS, 2, ROWS_STEP * heads // 2, head_dim), jnp.float32),
            pltpu.VMEM((SLOTS, 2, ROWS_STEP * kv_heads // 2, head_dim), jnp.float32),
            pltpu.VMEM((SLOTS, 2, ROWS_STEP * kv_heads // 2, head_dim), jnp.float32),
            pltpu.VMEM((2, ROWS_STEP * heads, head_dim), jnp.float32),
            pltpu.VMEM((heads, cols), jnp.int32),
            pltpu.VMEM((ROWS_STEP, heads, cols), jnp.float32),
            pltpu.VMEM((ROWS_STEP, 2 * heads, cols // 2), bf),
            pltpu.SemaphoreType.DMA((SLOTS, 5)),
            pltpu.SemaphoreType.DMA((SLOTS, 2)),
            pltpu.SemaphoreType.DMA((2,)),
            pltpu.SemaphoreType.DMA((4, 2)),
        ],
        input_output_aliases=aliases,
        compiler_params=pltpu.CompilerParams(vmem_limit_bytes=62 * 1024 * 1024),
        cost_estimate=pl.CostEstimate(flops=n_rows * heads * cols * head_dim * 4,
                                      bytes_accessed=n_rows * cols * head_dim * 8, transcendentals=0),
        name='attend',
    )(pos, base, q, kn, vn, k_cache, v_cache, *extra)


def merge_kernel(chunks, *refs):
    n_in = 4 * len(chunks)
    source = [refs[4 * c:4 * c + 4] for c in range(len(chunks))]
    pieces = [[b.at[d] for d in range(4)] for b in refs[-len(chunks):]]
    refs = refs[:-len(chunks)]
    (wo_hbm, sums, wo, last_in, last_out, osum, lhs, y_out, y_in,
     p_sem, w_sem, o_send, o_recv, y_send, y_recv, g_send, g_recv, d_send, d_recv, f_send, f_recv) = refs[n_in:]
    sp = lax.axis_index('sp')
    tp = lax.axis_index('tp')
    core = lax.rem(sp, 2)
    xpos = sp // 2
    n_chunks, _, chunk = y_out.shape
    heads = lhs.shape[1] // 128
    parts = [c // 4 for c in chunks]
    core_id = 2 * xpos + (1 - core)
    x_id = 2 * (1 - xpos) + core
    core_peer, x_peer, y_peer = {'sp': core_id}, {'sp': x_id}, {'tp': 1 - tp}
    mesh_id = pl.DeviceIdType.MESH

    def remote(src, dst, send, recv, peer):
        return pltpu.make_async_remote_copy(src_ref=src, dst_ref=dst, send_sem=send, recv_sem=recv,
                                            device_id=peer, device_id_type=mesh_id)

    def w_load(n):
        return pltpu.make_async_copy(wo_hbm.at[:, pl.ds(n * chunk, chunk)], wo.at[n], w_sem.at[n])

    local = [[pltpu.make_async_copy(source[c][d], pieces[c][d], p_sem.at[c, d]) for d in range(4)] for c in range(len(chunks))]
    for copy in local[-1]:
        copy.start()
    barrier = pltpu.get_barrier_semaphore()
    for peer in (core_peer, x_peer, y_peer):
        pl.semaphore_signal(barrier, inc=1, device_id=peer, device_id_type=mesh_id)
    pl.semaphore_wait(barrier, 3)

    for copy in local[-1]:
        copy.wait()
    last = [remote(pieces[-1][3], last_in.at[0], o_send.at[0], o_recv.at[0], core_peer),
            remote(pieces[-1][1], last_in.at[1], o_send.at[1], o_recv.at[1], core_peer),
            remote(last_out, last_in.at[2], o_send.at[2], o_recv.at[2], x_peer)]
    last[0].start()
    last[1].start()
    for copy in local[0]:
        copy.start()
    for n in range(3):
        w_load(n).start()

    def shares(blocks, part):
        count = part * heads
        stats = [block[count:count + 2 * heads, :] for block in blocks]
        top = functools.reduce(jnp.maximum, [st[:heads] for st in stats])
        grown = [jnp.exp(st[:heads] - top) for st in stats]
        return top, sum(st[heads:] * g for st, g in zip(stats, grown)), grown

    def mix(blocks, weights, owner, part, out):
        shift = lax.rem(128 - owner * part, 128)
        factors = [pltpu.roll(w, shift, 1) for w in weights]
        for b in range(part):
            at = slice(b * heads, (b + 1) * heads)
            out[at, :] = sum(block[at, :] * f[:, b:b + 1] for block, f in zip(blocks, factors))

    def combine(blocks, part, row0):
        _, total, grown = shares(blocks, part)
        mix(blocks, [g / total for g in grown], sp, part, osum)
        for h in range(heads):
            lhs[row0:row0 + part, h * 128:(h + 1) * 128] = osum[pl.ds(h, part, stride=heads), :].astype(jnp.bfloat16)

    last[0].wait_recv()
    pair = [pieces[-1][2], last_in.at[0]]
    top, total, grown = shares(pair, parts[-1])
    mix(pair, grown, x_id, parts[-1], last_out)
    count = parts[-1] * heads
    last_out[count:count + heads, :] = top
    last_out[count + heads:count + 2 * heads, :] = total
    last[2].start()

    for copy in local[0]:
        copy.wait()
    combine(pieces[0], parts[0], 0)

    sizes = (2, 2, 2, 2, 1)
    order = []
    for c, part in enumerate(parts):
        begin = 0
        for size in sizes:
            order.append((pl.ds(begin, size), pl.ds(sum(parts[:c]), part), range(begin, begin + size)))
            begin += size
    n_pieces = len(order)
    n_first = len(sizes)

    def to_y(t):
        ns, r, _ = order[t]
        return remote(y_out.at[ns, r], y_in.at[ns, r], y_send.at[t], y_recv.at[t], y_peer)

    def gather(t, owner, send, recv, peer):
        ns, r, _ = order[t]
        return remote(sums.at[owner, ns, r], sums.at[owner, ns, r], send.at[t], recv.at[t], peer)

    def to_x(t):
        return gather(t, sp, g_send, g_recv, x_peer)

    def to_core(t):
        return gather(t, sp, d_send, d_recv, core_peer)

    def relay(t):
        return gather(t, x_id, f_send, f_recv, core_peer)

    def project_rows(n, r0, count):
        y_out[n, r0:r0 + count, :] = jnp.dot(lhs[r0:r0 + count, :], wo[n], preferred_element_type=jnp.float32)

    for t in range(n_first):
        for n in order[t][2]:
            w_load(n).wait()
            if n + 3 < n_chunks:
                w_load(n + 3).start()
            project_rows(n, 0, parts[0])
        to_y(t).start()

    for t in range(n_pieces + 3):
        if t == 2:
            for copy in last[1:]:
                copy.wait_recv()
            combine([pieces[-1][0], last_in.at[1], last_in.at[2]], parts[-1], parts[0])
        if 2 <= t < 2 + n_first:
            for n in order[n_first + t - 2][2]:
                project_rows(n, parts[0], parts[-1])
            to_y(n_first + t - 2).start()
        if t < n_pieces:
            ns, r, _ = order[t]
            to_y(t).wait()
            sums[sp, ns, r, :] = y_out[ns, r, :] + y_in[ns, r, :]
            to_x(t).start()
            to_core(t).start()
        if 1 <= t < n_pieces + 1:
            to_x(t - 1).wait_recv()
            relay(t - 1).start()
        if t >= 3:
            to_core(t - 3).wait_recv()
            relay(t - 3).wait_recv()
    for copy in last:
        copy.wait_send()
    for t in range(n_pieces):
        to_x(t).wait_send()
        to_core(t).wait_send()
        relay(t).wait_send()


def merge(chunks, pieces, w_o, n_chunks):
    inner, width = w_o.shape
    heads = inner // 128
    quarter = sum(chunks) // 4
    chunk = width // n_chunks
    hbm = pl.BlockSpec(memory_space=pltpu.HBM)
    f32 = jnp.float32
    dma = pltpu.SemaphoreType.DMA
    flat = [p if 0 < d and c < len(chunks) - 1 else pltpu.with_memory_space_constraint(p, pltpu.HBM)
            for c, piece in enumerate(pieces) for d, p in enumerate(piece)]
    block = pieces[-1][0].shape
    return pl.pallas_call(
        functools.partial(merge_kernel, chunks),
        out_shape=jax.ShapeDtypeStruct((4, n_chunks, quarter, chunk), f32),
        in_specs=[hbm] * (len(flat) + 1),
        out_specs=pl.BlockSpec(memory_space=pltpu.VMEM),
        scratch_shapes=[
            pltpu.VMEM((n_chunks, inner, chunk), jnp.bfloat16),
            pltpu.VMEM((3,) + block, f32),
            pltpu.VMEM(block, f32),
            pltpu.VMEM((max(chunks) // 4 * heads, 128), f32),
            pltpu.VMEM((quarter, inner), jnp.bfloat16),
            pltpu.VMEM((n_chunks, quarter, chunk), f32),
            pltpu.VMEM((n_chunks, quarter, chunk), f32),
            dma((len(chunks), 4)), dma((n_chunks,)), dma((3,)), dma((3,)),
        ] + [dma((10,))] * 8 + [pltpu.VMEM((4,) + piece[0].shape, f32) for piece in pieces],
        compiler_params=pltpu.CompilerParams(vmem_limit_bytes=40 * 1024 * 1024, collective_id=0, has_side_effects=True),
        cost_estimate=pl.CostEstimate(flops=2 * quarter * inner * width, bytes_accessed=2 * inner * width, transcendentals=0),
        name='merge',
    )(*flat, pltpu.with_memory_space_constraint(w_o, pltpu.HBM))


def finish_kernel(sums, xbuf, wpost_ref, out_hbm, gain_ref, obuf, out_sem):
    parts, n_chunks, rows, chunk = sums.shape

    def store(q):
        at = pl.ds(q * rows, rows)
        return pltpu.make_async_copy(obuf.at[at], out_hbm.at[at], out_sem.at[q])

    for j in range(wpost_ref.shape[0]):
        gain_ref[:, j * 128:(j + 1) * 128] = 1.0 + wpost_ref[j:j + 1, :]
    for q in range(parts):
        for k in range(rows // 16):
            at = slice(k * 16, (k + 1) * 16)
            to = slice(q * rows + k * 16, q * rows + (k + 1) * 16)
            square = jnp.zeros((16, chunk), jnp.float32)
            for n in range(n_chunks):
                u = sums[q, n, at, :]
                square = square + u * u
            inv = lax.rsqrt(jnp.sum(square, axis=-1, keepdims=True) * (1.0 / (n_chunks * chunk)) + NORM_EPS)
            for n in range(n_chunks):
                col = slice(n * chunk, (n + 1) * chunk)
                y = xbuf[to, col].astype(jnp.float32) + sums[q, n, at, :] * inv * gain_ref[:, col]
                obuf[to, col] = y.astype(jnp.bfloat16)
        store(q).start()
    for q in range(parts):
        store(q).wait()


def finish(sums, x_in, w_post):
    parts = sums.shape[0]
    hbm = pl.BlockSpec(memory_space=pltpu.HBM)
    dma = pltpu.SemaphoreType.DMA
    return pl.pallas_call(
        finish_kernel,
        out_shape=jax.ShapeDtypeStruct(x_in.shape, x_in.dtype),
        in_specs=[pl.BlockSpec(memory_space=pltpu.VMEM)] * 3,
        out_specs=hbm,
        scratch_shapes=[pltpu.VMEM((1, x_in.shape[1]), jnp.float32), pltpu.VMEM(x_in.shape, x_in.dtype), dma((parts,))],
        compiler_params=pltpu.CompilerParams(vmem_limit_bytes=24 * 1024 * 1024),
        name='finish',
    )(sums, x_in, w_post)


def solution(mesh):
    cache_spec = P('dp', 'sp', 'tp', None)
    sp_size = mesh.shape['sp']

    def local_step(x_in, cur_pos, w_pre, w_q, w_k, w_v, w_o, w_post, k_cache, v_cache):
        row_count, seq_block, kv_local, head_dim = k_cache.shape
        sp_index = lax.axis_index('sp')
        table = rotary_table(sp_size * seq_block, head_dim)
        q_rot, kn2, vn2 = project(cur_pos, x_in, w_pre.reshape(-1, 128), table, w_q, w_k, w_v)
        base = (sp_index * seq_block).astype(jnp.int32).reshape(1)
        kc = k_cache.reshape(row_count, seq_block * kv_local, head_dim)
        vc = v_cache.reshape(row_count, seq_block * kv_local, head_dim)
        chunks = (row_count // 2, row_count // 2)
        prev, first_row, pieces = None, 0, []
        for index, n_rows in enumerate(chunks):
            *prev, p0, p1, p2, p3 = attend(cur_pos, base, q_rot, kn2, vn2, kc, vc, prev, first_row, n_rows)
            first_row += n_rows // 4
            if index < len(chunks) - 1:
                moved = []
                for d, p in ((1, p1), (2, p2), (3, p3)):
                    moved.append(lax.ppermute(p, 'sp', [(i, i ^ d) for i in range(sp_size)]))
                p1, p2, p3 = moved
            pieces.append((p0, p1, p2, p3))
        k_out, v_out = prev
        x_out = finish(merge(chunks, pieces, w_o, 9), x_in, w_post.reshape(-1, 128))
        return x_out, k_out.reshape(k_cache.shape), v_out.reshape(v_cache.shape)

    return jax.shard_map(local_step, mesh=mesh,
                         in_specs=(P('dp', None), P('dp'), P(None), P(None, 'tp'), P(None, 'tp'), P(None, 'tp'), P('tp', None), P(None), cache_spec, cache_spec),
                         out_specs=(P('dp', None), cache_spec, cache_spec), check_vma=False)
```
